32 devices in a mesh: row: 8 (over z, y), col: 4 (over x, core).
Axes of the slice: x: 2, y: 2, z: 4, core: 2. Of those that a mesh axis runs over, the one named last changes fastest.
Arguments:
- spectra: bfloat16 [600, 32, 512], P(None, 'row', 'col'), may hold values from 0.0099487305 to 1
- wind: float32 [2, 32, 512], P(None, 'row', 'col'), may hold values from -18 to 18
- wave_current: float32 [3, 32, 512], P(None, 'row', 'col'), may hold values from -3 to 3
- wave_wet: int32 [32, 512], P('row', 'col'), may hold values 0 or 1
- interaction: bfloat16 [600, 600], replicated, may hold values from -0.25 to 0.25
- input_rate: float32 [25], replicated, may hold values from 0.002 to 0.03
- eta_gain: float32 [25], replicated, may hold values from -0.5 to 0.5
- stress_map: float32 [2, 600], replicated, may hold values from -0.25 to 0.25
- stokes_map: float32 [6, 600], replicated, may hold values from -0.25 to 0.25
- ocean_vel: float32 [2, 30, 64, 512], P(None, None, 'row', 'col'), may hold values from -3 to 3
- ocean_eta: float32 [64, 512], P('row', 'col'), may hold values from -3 to 3
- ocean_wet: int32 [64, 512], P('row', 'col'), may hold values 0 or 1
- coriolis: float32 [64, 512], P('row', 'col'), may hold values from -1.5 to 1.5
- tau_profile: float32 [30], replicated, may hold values from 0.05 to 1
- stokes_profile: float32 [3, 30], replicated, may hold values from 0.05 to 1
- thickness: float32 [30], replicated, may hold values from 0.02 to 0.1
- mix_inverse: float32 [30, 30], replicated
- fold_index: int32 [512], P('col'), may hold values from 0 to 511, as said below
- wave_send: int32 [8, 4, 3, 64], P('row', 'col'), may hold values from 0 to 511
- ocean_recv: bfloat16 [8, 4, 3, 64, 1024], P('row', 'col'), may hold values from -0.4375 to 0.4375
- ocean_send: int32 [8, 4, 3, 64], P('row', 'col'), may hold values from 0 to 1023
- wave_recv: bfloat16 [8, 4, 3, 64, 512], P('row', 'col'), may hold values from -0.4375 to 0.4375
Outputs:
- spectra_out: bfloat16 [600, 32, 512], P(None, 'row', 'col')
- ocean_vel_out: float32 [2, 30, 64, 512], P(None, None, 'row', 'col')
- ocean_eta_out: float32 [64, 512], P('row', 'col')
- current_out: float32 [3, 32, 512], P(None, 'row', 'col')
The draws below stay inside these ranges and needn't reach their ends.
Inputs may be any that keep to these rules, and one draw needn't show every extreme that they name: `wave_send`: entries name cells of the sending wave tile numbered y * 128 + x. `ocean_send`: entries name cells of the sending ocean tile numbered y * 128 + x. `fold_index`: each entry names a column of the whole top line; columns of any block may be named from any block.
All inputs are finite; a program needn't handle non-finite values. No bound on the sum of `wave_wet` or of `ocean_wet` on one device may be relied on, other than what follows from the above.
Results may differ from the reference program's by a relative error of at most 0.006.
Values may be sent and summed in bfloat16 or wider, within the bound.
No kernel may reach another device: no remote copies, remote signals or barrier semaphores. Data moves between devices by JAX's collectives and lax.ppermute only.
A program may use at most 64 MiB of HBM per device.

```python
import math
import jax
import jax.numpy as jnp
from jax import lax

NDIR = 24
NFREQ = 25
LEV = 30
NBAND = 3
WXD = 128
WYD = 4
OX = 128
OY = 8
SLOT = 64
STEPS = 2
SPEC = 600
WY = 32
WX = 512
OYG = 64
OXG = 512
N_ROW = 8
N_COL = 4


def draw_mix_inverse(key, part):
    noise_key = jax.random.fold_in(key, 11)
    noise = jax.random.normal(noise_key, (LEV, LEV), jnp.float32)
    return 0.7 * jnp.eye(LEV, dtype=jnp.float32) + 0.3 * noise / jnp.sqrt(jnp.float32(LEV))


def draw_fold_index(key, part):
    total = OX * N_COL
    spread = jax.random.randint(jax.random.fold_in(key, 5), (N_COL, OX), 0, total, jnp.int32)
    within = jax.random.randint(jax.random.fold_in(key, 7), (N_COL,), 0, OX, jnp.int32)
    far_block = (jnp.arange(N_COL, dtype=jnp.int32) + N_COL // 2) % N_COL
    first = far_block * OX + within
    spread = spread.at[:, 0].set(first)
    return spread.reshape(-1).astype(jnp.int32)


def plant(result, own_key, smallest, high):
    longest = result.shape.index(max(result.shape))
    spots = []
    for shift in (0, 1):
        where = [jax.random.randint(jax.random.fold_in(own_key, axis), (), 0, length) for axis, length in enumerate(result.shape)]
        where[longest] = (where[longest] + shift) % result.shape[longest]
        spots.append(tuple(where))
    return result.at[spots[0]].set(smallest).at[spots[1]].set(high)


def block_scale(stream_key, dims, pieces, least, high):
    loudness, own = 1.0, jax.random.fold_in(stream_key, 6)
    for position, parts in pieces:
        steps = jnp.exp(jax.random.uniform(jax.random.fold_in(own, position), (parts,), jnp.float32, least / len(pieces), high / len(pieces)))
        loudness = loudness * jnp.repeat(steps, dims[position] // parts).reshape([-1 if axis == position else 1 for axis in range(len(dims))])
    return loudness


def bell_draw(own_key, dims, scale, reach, shards=(), kind=jnp.bfloat16):
    loudness = block_scale(own_key, dims, shards, -0.22, 0.18) if shards else 1.0
    drawn = jax.random.normal(own_key, dims, jnp.float32) * scale * loudness
    return jnp.minimum(jnp.maximum(drawn, -reach), reach).astype(kind)


def setup_inputs(seed: int = 0) -> dict:
    splits = jax.random.split(jax.random.key(seed), 23)
    spectra = jnp.clip(jnp.exp(math.log(1.0) - 4.61031033 * jax.random.uniform(splits[0], (SPEC, WY, WX), jnp.float32) ** block_scale(splits[0], (SPEC, WY, WX), ((1, 8), (2, 4)), -0.2, 0.2)), 0.0099487305, 1.0).astype(jnp.bfloat16)
    wind = bell_draw(splits[1], (2, WY, WX), 3.0, 18.0, ((1, 8), (2, 4)), jnp.float32)
    wave_current = bell_draw(splits[2], (3, WY, WX), 0.5, 3.0, ((1, 8), (2, 4)), jnp.float32)
    wave_wet = plant((jax.random.randint(splits[3], (WY, WX), 0, 4) < 3).astype(jnp.int32), jax.random.fold_in(splits[3], 1), 0, 1)
    interaction = bell_draw(splits[4], (SPEC, SPEC), SPEC ** -0.5, 0.25)
    input_rate = jnp.clip(jnp.exp(jax.random.uniform(splits[5], (NFREQ,), jnp.float32, math.log(0.002), math.log(0.03))), 0.002, 0.03)
    eta_gain = jnp.clip(jax.random.uniform(splits[6], (NFREQ,), jnp.float32, -0.5, 0.5), -0.5, 0.5)
    stress_map = bell_draw(splits[7], (2, SPEC), SPEC ** -0.5, 0.25, (), jnp.float32)
    stokes_map = bell_draw(splits[8], (2 * NBAND, SPEC), SPEC ** -0.5, 0.25, (), jnp.float32)
    ocean_vel = bell_draw(splits[9], (2, LEV, OYG, OXG), 0.5, 3.0, ((2, 8), (3, 4)), jnp.float32)
    ocean_eta = bell_draw(splits[10], (OYG, OXG), 0.5, 3.0, ((0, 8), (1, 4)), jnp.float32)
    ocean_wet = plant((jax.random.randint(splits[11], (OYG, OXG), 0, 3) < 2).astype(jnp.int32), jax.random.fold_in(splits[11], 1), 0, 1)
    coriolis = jnp.clip(jax.random.uniform(splits[12], (OYG, OXG), jnp.float32, -1.5, 1.5) * block_scale(splits[12], (OYG, OXG), ((0, 8), (1, 4)), -0.4, 0.0), -1.5, 1.5)
    tau_profile = jnp.clip(jnp.exp(jax.random.uniform(splits[13], (LEV,), jnp.float32, math.log(0.05), math.log(1.0))), 0.05, 1.0)
    stokes_profile = jnp.clip(jnp.exp(jax.random.uniform(splits[14], (NBAND, LEV), jnp.float32, math.log(0.05), math.log(1.0))), 0.05, 1.0)
    thickness = jnp.clip(jnp.exp(jax.random.uniform(splits[15], (LEV,), jnp.float32, math.log(0.02), math.log(0.1))), 0.02, 0.1)
    mix_inverse = draw_mix_inverse(jax.random.fold_in(splits[22], 71), 0)
    fold_index = draw_fold_index(jax.random.fold_in(splits[22], 71), 0)
    wave_send = plant(jax.random.randint(splits[18], (N_ROW, N_COL, 3, SLOT), 0, WYD * WXD), jax.random.fold_in(splits[18], 1), 0, (WYD * WXD) - 1).astype(jnp.int32)
    ocean_recv = bell_draw(splits[19], (N_ROW, N_COL, 3, SLOT, OY * OX), (3 * SLOT) ** -0.5, 0.4375, ((0, 8), (1, 4)))
    ocean_send = plant(jax.random.randint(splits[20], (N_ROW, N_COL, 3, SLOT), 0, OY * OX), jax.random.fold_in(splits[20], 1), 0, (OY * OX) - 1).astype(jnp.int32)
    wave_recv = bell_draw(splits[21], (N_ROW, N_COL, 3, SLOT, WYD * WXD), (3 * SLOT) ** -0.5, 0.4375, ((0, 8), (1, 4)))
    return dict(spectra=spectra, wind=wind, wave_current=wave_current, wave_wet=wave_wet, interaction=interaction, input_rate=input_rate, eta_gain=eta_gain, stress_map=stress_map, stokes_map=stokes_map, ocean_vel=ocean_vel, ocean_eta=ocean_eta, ocean_wet=ocean_wet, coriolis=coriolis, tau_profile=tau_profile, stokes_profile=stokes_profile, thickness=thickness, mix_inverse=mix_inverse, fold_index=fold_index, wave_send=wave_send, ocean_recv=ocean_recv, ocean_send=ocean_send, wave_recv=wave_recv)


viscous = 0.2
surface_rate = 0.5
highest = lax.Precision.HIGHEST


def wave_cells(energy, wind_cells, current, wet_cells, interaction, input_rate, eta_gain, stress_map, stokes_map):
    spectrum_len = energy.shape[0]
    heading = ((jnp.arange(spectrum_len) % NDIR).astype(jnp.float32) + 0.5) * (2.0 * math.pi / NDIR)
    cosine = jnp.cos(heading)[:, None]
    sine_dir = jnp.sin(heading)[:, None]
    relative = (wind_cells[0] - current[0]) * cosine + (wind_cells[1] - current[1]) * sine_dir
    growth = jnp.repeat(input_rate, NDIR)[:, None] * jax.nn.softplus(relative)
    energy_wide = energy.astype(jnp.float32)
    transfer_term = jnp.dot(interaction, energy, preferred_element_type=jnp.float32)
    level_term = jnp.repeat(eta_gain, NDIR)[:, None] * current[2]
    updated = (wet_cells.astype(jnp.float32) * (energy_wide + (growth + level_term) * energy_wide + transfer_term)).astype(jnp.bfloat16)
    stress = jnp.dot(stress_map, growth * energy_wide, precision=highest)
    stokes = jnp.dot(stokes_map, updated.astype(jnp.float32), precision=highest)
    return updated, jnp.concatenate([stress, stokes], 0).astype(jnp.bfloat16)


def ocean_force(velocity, forcing, ocean_wet, coriolis, tau_profile, stokes_profile):
    wet_mask = ocean_wet.astype(jnp.float32)
    along_u = tau_profile[:, None, None] * forcing[0]
    along_v = tau_profile[:, None, None] * forcing[1]
    for band_index in range(NBAND):
        profile = stokes_profile[band_index][:, None, None]
        along_u = along_u + coriolis * profile * forcing[3 + 2 * band_index]
        along_v = along_v - coriolis * profile * forcing[2 + 2 * band_index]
    return wet_mask * (velocity + jnp.stack([along_u, along_v]))


def ocean_finish(forced, padded, elevation, ocean_wet, thickness, mix_inverse):
    wet_mask = ocean_wet.astype(jnp.float32)
    laplacian = padded[:, :, 2:, 1:-1] + padded[:, :, :-2, 1:-1] + padded[:, :, 1:-1, 2:] + padded[:, :, 1:-1, :-2] - 4.0 * forced
    smoothed = wet_mask * (forced + viscous * laplacian)
    transport = jnp.einsum('l,clyx->cyx', thickness, padded, precision=highest)
    divergence = 0.5 * (transport[0, 1:-1, 2:] - transport[0, 1:-1, :-2]) + 0.5 * (transport[1, 2:, 1:-1] - transport[1, :-2, 1:-1])
    eta_next = wet_mask * (elevation - surface_rate * divergence)
    vel_next = jnp.einsum('lm,cmyx->clyx', mix_inverse, smoothed, precision=highest)
    return vel_next, eta_next


def tile_view(grid_data, tile_rows, tile_cols):
    fields = grid_data.shape[0]
    shaped = grid_data.reshape(fields, N_ROW, tile_rows, N_COL, tile_cols)
    return shaped.transpose(1, 3, 0, 2, 4).reshape(N_ROW, N_COL, fields, tile_rows * tile_cols)


def grid_view(tile_data, tile_rows, tile_cols):
    fields = tile_data.shape[2]
    shaped = tile_data.reshape(N_ROW, N_COL, fields, tile_rows, tile_cols)
    return shaped.transpose(2, 0, 3, 1, 4).reshape(fields, N_ROW * tile_rows, N_COL * tile_cols)


def pick_slots(tile_data, indices):
    return jnp.moveaxis(jnp.take(tile_data, indices, axis=1), 1, 0)


def remap_tiles(tiles, send_rows, weights):
    slot_rows = jax.vmap(jax.vmap(pick_slots))(tiles, send_rows)
    zero_band = jnp.zeros_like(slot_rows[:1, :, 0])
    from_north = jnp.concatenate([slot_rows[1:, :, 0], zero_band], 0)
    from_south = jnp.concatenate([zero_band, slot_rows[:-1, :, 2]], 0)
    received = jnp.stack([from_north, slot_rows[:, :, 1], from_south], axis=2)

    def band_sum(items):
        return jnp.einsum('cjfs,cjsn->cfn', items[0].astype(jnp.float32), items[1].astype(jnp.float32))

    return lax.map(band_sum, (received, weights))


def pad_grid(forced, fold_index):
    north_row = -jnp.take(forced[:, :, -1, :], fold_index, axis=2)[:, :, None, :]
    south_row = jnp.zeros_like(north_row)
    middle = jnp.concatenate([south_row, forced, north_row], axis=2)
    return jnp.concatenate([middle[..., -1:], middle, middle[..., :1]], axis=3)


def reference(spectra, wind, wave_current, wave_wet, interaction, input_rate, eta_gain, stress_map, stokes_map, ocean_vel, ocean_eta, ocean_wet, coriolis, tau_profile, stokes_profile, thickness, mix_inverse, fold_index, wave_send, ocean_recv, ocean_send, wave_recv):
    energy = tile_view(spectra, WYD, WXD)
    wind_tiles = tile_view(wind, WYD, WXD)
    current = tile_view(wave_current, WYD, WXD)
    wet_tiles = tile_view(wave_wet[None], WYD, WXD)[:, :, 0]
    velocity = ocean_vel
    elevation = ocean_eta
    tile_step = jax.vmap(wave_cells, in_axes=(0, 0, 0, 0, None, None, None, None, None))

    def band_step(items):
        return tile_step(items[0], items[1], items[2], items[3], interaction, input_rate, eta_gain, stress_map, stokes_map)

    for step_index in range(STEPS):
        energy, fields = lax.map(band_step, (energy, wind_tiles, current, wet_tiles))
        forcing = grid_view(remap_tiles(fields, wave_send, ocean_recv), OY, OX)
        forced = ocean_force(velocity, forcing, ocean_wet, coriolis, tau_profile, stokes_profile)
        velocity, elevation = ocean_finish(forced, pad_grid(forced, fold_index), elevation, ocean_wet, thickness, mix_inverse)
        back = jnp.stack([velocity[0, 0], velocity[1, 0], elevation]).astype(jnp.bfloat16)
        current = remap_tiles(tile_view(back, OY, OX), ocean_send, wave_recv)
    return grid_view(energy, WYD, WXD), velocity, elevation, grid_view(current, WYD, WXD)
```

```python
import functools
import math

import jax
import jax.numpy as jnp
import numpy as np
from jax import lax
from jax.experimental import pallas as pl
from jax.experimental.pallas import tpu as pltpu
from jax.sharding import PartitionSpec as P

NDIR = 24
NBAND = 3
STEPS = 2
viscous = 0.2
surface_rate = 0.5

f32, bf16 = jnp.float32, jnp.bfloat16
VMEM = pl.BlockSpec(memory_space=pltpu.VMEM)
SMEM = pl.BlockSpec(memory_space=pltpu.SMEM)


def call(kernel, outs, specs, scratch=(), name=None):
    out_shape = tuple(jax.ShapeDtypeStruct(s, d) for s, d in outs)
    return pl.pallas_call(
        kernel,
        out_shape=out_shape,
        in_specs=list(specs),
        out_specs=tuple(VMEM for _ in outs),
        scratch_shapes=list(scratch),
        name=name,
    )


def dot(a, b):
    return jnp.dot(a, b, preferred_element_type=f32)


def split2(w):
    high = w.astype(bf16)
    low = (w - high.astype(f32)).astype(bf16)
    return high, low


def is_even(index):
    return lax.rem(index, 2) == 0


def stress_rows(smap, rate_ref, nfreq):
    spec = smap.shape[1]
    col = lax.broadcasted_iota(jnp.int32, (1, spec), 1)
    band = jnp.zeros((1, spec), jnp.int32)
    rate = jnp.full((1, spec), rate_ref[0], f32)
    for f in range(1, nfreq):
        past = col >= NDIR * f
        band = band + jnp.where(past, 1, 0)
        rate = jnp.where(past, rate_ref[f], rate)
    direction = col - NDIR * band
    row = lax.broadcasted_iota(jnp.int32, (NDIR, spec), 0)
    keep = row == direction
    weights = [jnp.where(keep, smap[i : i + 1] * rate, 0.0) for i in range(2)]
    weights = jnp.concatenate(weights, axis=0)
    high, low = split2(weights)
    return jnp.concatenate([high.astype(f32), low.astype(f32)], axis=0).astype(bf16)


def transfer(inter, smap, rate_ref, eb, t_ref, q_ref, nfreq):
    t_ref[...] = dot(inter, eb)
    q = dot(stress_rows(smap, rate_ref, nfreq), eb)
    half = 2 * NDIR
    q_ref[...] = q[:half] + q[half:]


def wave_finish(
    e_of, t_ref, q_ref, wind_ref, current_of, wet_ref, rate_ref, gain_ref, kmap, trig_ref, upd_ref, nfreq
):
    rows, lanes = wet_ref.shape
    cosine, sine = trig_ref[:NDIR], trig_ref[NDIR:]
    stress = []
    for y in range(rows):
        cells = slice(y * lanes, (y + 1) * lanes)
        dx = wind_ref[0, y : y + 1, :] - current_of(0, y)
        dy = wind_ref[1, y : y + 1, :] - current_of(1, y)
        level = current_of(2, y)
        wet = wet_ref[y : y + 1, :].astype(f32)
        relative = dx * cosine + dy * sine
        soft = jnp.maximum(relative, 0.0) + jnp.log1p(jnp.exp(-jnp.abs(relative)))
        stress.append(
            [
                jnp.sum(soft * q_ref[i * NDIR : (i + 1) * NDIR, cells], axis=0, keepdims=True)
                for i in range(2)
            ]
        )
        rate = jnp.concatenate(
            [rate_ref[f] * soft + gain_ref[f] * level for f in range(nfreq)], axis=0
        )
        e = e_of(y)
        upd_ref[:, cells] = (wet * (e + rate * e + t_ref[:, cells])).astype(bf16)
    high, low = split2(kmap)
    pair = jnp.concatenate([high.astype(f32), low.astype(f32)], axis=0).astype(bf16)
    stokes = dot(pair, upd_ref[...])
    bands = 2 * NBAND
    stokes = stokes[:bands] + stokes[bands:]
    stress = jnp.concatenate(
        [jnp.concatenate([stress[y][i] for y in range(rows)], axis=1) for i in range(2)], axis=0
    )
    return jnp.concatenate([stress, stokes], axis=0)


def pick(fields, send, outs):
    to_even, to_odd, own = outs
    slot = send.shape[1]
    index = jnp.concatenate([send[j : j + 1] for j in range(3)], axis=1)
    cell = lax.broadcasted_iota(jnp.int32, (fields.shape[1], 3 * slot), 0)
    hot = jnp.where(cell == index, 1.0, 0.0).astype(bf16)
    slots = dot(fields.astype(bf16), hot)
    even = is_even(lax.axis_index("row"))
    south, north = slots[:, :slot], slots[:, 2 * slot :]
    to_even[...] = jnp.where(even, north, south).astype(bf16)
    to_odd[...] = jnp.where(even, south, north).astype(bf16)
    own[...] = slots[:, slot : 2 * slot].astype(bf16)


def gather_slots(got_even, got_odd, own, rows):
    row = lax.axis_index("row")
    even = is_even(row)
    a, b = got_even[...].astype(f32), got_odd[...].astype(f32)
    north = jnp.where(row == rows - 1, 0.0, jnp.where(even, a, b))
    south = jnp.where(row == 0, 0.0, jnp.where(even, b, a))
    return jnp.concatenate([north, own[...].astype(f32), south], axis=1).astype(bf16)


def k_wave_first(
    nfreq,
    spec_ref, wind_ref, cur_ref, wet_ref, inter_ref, rate_ref, gain_ref, smap_ref, kmap_ref, trig_ref, send_ref,
    upd_ref, to_even, to_odd, own,
    ef, eb, t, q,
):
    rows, lanes = wet_ref.shape
    spec = inter_ref.shape[0]
    ef[...] = spec_ref[...].astype(f32)
    for y in range(rows):
        eb[:, y * lanes : (y + 1) * lanes] = ef[pl.ds(y, spec, stride=rows), :].astype(bf16)
    transfer(inter_ref[...], smap_ref[...], rate_ref, eb[...], t, q, nfreq)
    fields = wave_finish(
        lambda y: ef[pl.ds(y, spec, stride=rows), :],
        t, q, wind_ref,
        lambda i, y: cur_ref[i, y : y + 1, :],
        wet_ref, rate_ref, gain_ref, kmap_ref[...], trig_ref, upd_ref, nfreq,
    )
    pick(fields, send_ref[...], (to_even, to_odd, own))


def k_transfer(nfreq, upd_ref, inter_ref, smap_ref, rate_ref, t_ref, q_ref):
    transfer(inter_ref[...], smap_ref[...], rate_ref, upd_ref[...], t_ref, q_ref, nfreq)


def k_wave_next(
    nfreq, n_row,
    got_even, got_odd, got_own, recv_ref, old_ref, t_ref, q_ref, wind_ref, wet_ref, rate_ref, gain_ref, kmap_ref, trig_ref, send_ref,
    upd_ref, to_even, to_odd, own,
    cur,
):
    lanes = wet_ref.shape[1]
    slots = gather_slots(got_even, got_odd, got_own, n_row)
    cur[...] = dot(slots, recv_ref[...])
    fields = wave_finish(
        lambda y: old_ref[:, y * lanes : (y + 1) * lanes].astype(f32),
        t_ref, q_ref, wind_ref,
        lambda i, y: cur[i : i + 1, y * lanes : (y + 1) * lanes],
        wet_ref, rate_ref, gain_ref, kmap_ref[...], trig_ref, upd_ref, nfreq,
    )
    pick(fields, send_ref[...], (to_even, to_odd, own))


def k_spectra_out(rows, upd_ref, out_ref, wide):
    spec = upd_ref.shape[0]
    lanes = out_ref.shape[1]
    for y in range(rows):
        wide[pl.ds(y, spec, stride=rows), :] = upd_ref[:, y * lanes : (y + 1) * lanes].astype(f32)
    out_ref[...] = wide[...].astype(bf16)


def k_current_out(n_row, got_even, got_odd, own, recv_ref, out_ref):
    rows, lanes = out_ref.shape[1:]
    cur = dot(gather_slots(got_even, got_odd, own, n_row), recv_ref[...])
    for i in range(3):
        for y in range(rows):
            out_ref[i, y : y + 1, :] = cur[i : i + 1, y * lanes : (y + 1) * lanes]


def k_force(
    n_row, lev, pad,
    got_even, got_odd, own, recv_ref, vel_ref, wet_ref, cor_ref, tau_ref, prof_ref,
    forced_ref, row_even, row_odd, col_even, col_odd,
    fs,
):
    oy, ox = wet_ref.shape
    planes = 2 * lev
    forcing = dot(gather_slots(got_even, got_odd, own, n_row), recv_ref[...])
    nf = forcing.shape[0]
    for y in range(oy):
        fs[y * nf : (y + 1) * nf, :] = forcing[:, y * ox : (y + 1) * ox]
    field = [fs[pl.ds(i, oy, stride=nf), :] for i in range(nf)]
    wet = wet_ref[...].astype(f32)
    cor = cor_ref[...]
    along = [cor * field[i] for i in range(2, nf)]
    lane = lax.broadcasted_iota(jnp.int32, (oy, ox), 1)
    east = jnp.zeros((oy, ox), f32)
    west = jnp.zeros((oy, ox), f32)
    for i in range(planes):
        c, l = divmod(i, lev)
        accel = tau_ref[l] * field[c]
        for b in range(NBAND):
            term = prof_ref[b, l] * along[2 * b + 1 - c]
            accel = accel + term if c == 0 else accel - term
        value = wet * (vel_ref[i * oy : (i + 1) * oy, :] + accel)
        forced_ref[i * oy : (i + 1) * oy, :] = value
        here = lane == i
        west = jnp.where(here, pltpu.roll(value, i, 1) if i else value, west)
        east = jnp.where(here, pltpu.roll(value, (i + 1) % ox, 1), east)
    bottom = forced_ref[pl.ds(0, planes, stride=oy), :]
    top = forced_ref[pl.ds(oy - 1, planes, stride=oy), :]
    even = is_even(lax.axis_index("row"))
    row_even[...] = jnp.where(even, top, bottom).astype(bf16)
    row_odd[...] = jnp.where(even, bottom, top).astype(bf16)
    even = is_even(lax.axis_index("col"))
    col_even[:planes, :] = top.astype(bf16)
    col_odd[:planes, :] = top.astype(bf16)
    filler = jnp.zeros((16 - oy, ox), f32)
    col_even[pad:, :] = jnp.concatenate([jnp.where(even, east, west), filler], 0).astype(bf16)
    col_odd[pad:, :] = jnp.concatenate([jnp.where(even, west, east), filler], 0).astype(bf16)


def k_smooth(
    n_row, n_col, lev, pad, whole,
    forced_ref, got_row_even, got_row_odd, got_col_even, got_col_odd, line_ref, fold_ref, eta_ref, wet_ref, thick_ref, mix_ref, send_ref,
    smooth_ref, eta_out, to_even, to_odd, own,
    north, south, bs,
):
    oy, ox = wet_ref.shape
    planes = 2 * lev
    row, col = lax.axis_index("row"), lax.axis_index("col")
    even = is_even(row)
    a, b = got_row_even[...].astype(f32), got_row_odd[...].astype(f32)
    if whole:
        pieces = [(line_ref[t * planes : (t + 1) * planes, :], t) for t in range(n_col)]
    else:
        top = forced_ref[pl.ds(oy - 1, planes, stride=oy), :].astype(bf16)
        pair_even = jnp.where(is_even(col), col + 1, col - 1)
        pair_odd = lax.rem(jnp.where(is_even(col), col - 1, col + 1) + n_col, n_col)
        pieces = [
            (top, col),
            (got_col_even[:planes, :], pair_even),
            (got_col_odd[:planes, :], pair_odd),
            (got_row_odd[...], lax.rem(col + n_col // 2, n_col)),
        ]
    cell = lax.broadcasted_iota(jnp.int32, (ox, ox), 0)
    across = None
    for piece, tile in pieces:
        hot = jnp.where(cell == fold_ref[...] - tile * ox, 1.0, 0.0).astype(bf16)
        part = dot(piece, hot)
        across = part if across is None else across + part
    north[...] = jnp.where(row == n_row - 1, -across, jnp.where(even, a, b))
    south[...] = jnp.where(row == 0, 0.0, jnp.where(even, b, a))
    even = is_even(col)
    a = got_col_even[pad:, :].astype(f32)[:oy]
    b = got_col_odd[pad:, :].astype(f32)[:oy]
    east_col = jnp.where(even, a, b)
    west_col = jnp.where(even, b, a)
    wet = wet_ref[...].astype(f32)
    lane = lax.broadcasted_iota(jnp.int32, (oy, ox), 1)
    line = lax.broadcasted_iota(jnp.int32, (oy, ox), 0)
    is_top, is_bottom = line == oy - 1, line == 0
    is_east, is_west = lane == ox - 1, lane == 0
    across_u = jnp.zeros((oy, ox), f32)
    across_v = jnp.zeros((oy, ox), f32)
    surface = []
    for i in range(planes):
        c, l = divmod(i, lev)
        here = forced_ref[i * oy : (i + 1) * oy, :]
        up = jnp.where(is_top, north[i : i + 1, :], pltpu.roll(here, oy - 1, 0))
        down = jnp.where(is_bottom, south[i : i + 1, :], pltpu.roll(here, 1, 0))
        right = jnp.where(is_east, pltpu.roll(east_col, (ox - 1 - i) % ox, 1), pltpu.roll(here, ox - 1, 1))
        left = jnp.where(is_west, pltpu.roll(west_col, (ox - i) % ox, 1), pltpu.roll(here, 1, 1))
        smooth = wet * (here + viscous * (up + down + right + left - 4.0 * here))
        smooth_ref[i * oy : (i + 1) * oy, :] = smooth
        if l == 0:
            surface.append(mix_ref[0, 0] * smooth)
        else:
            surface[c] = surface[c] + mix_ref[0, l] * smooth
        if c == 0:
            across_u = across_u + thick_ref[l] * (right - left)
        else:
            across_v = across_v + thick_ref[l] * (up - down)
    eta = wet * (eta_ref[...] - surface_rate * (0.5 * across_u + 0.5 * across_v))
    eta_out[...] = eta
    bs[: oy, :] = surface[0]
    bs[oy : 2 * oy, :] = surface[1]
    bs[2 * oy : 3 * oy, :] = eta
    bs[3 * oy :, :] = jnp.zeros((5 * oy, ox), f32)
    back = jnp.concatenate([bs[pl.ds(y, 8, stride=oy), :] for y in range(oy)], axis=1)
    pick(back, send_ref[...], (to_even, to_odd, own))


def k_mix(lev, oy, smooth_ref, mix_ref, vel_ref):
    group = 6
    for first in range(0, lev, group):
        levels = range(first, min(first + group, lev))
        total = {}
        for m in range(lev):
            u = smooth_ref[m * oy : (m + 1) * oy, :]
            v = smooth_ref[(lev + m) * oy : (lev + m + 1) * oy, :]
            for l in levels:
                w = mix_ref[l, m]
                total[l, 0] = w * u if m == 0 else total[l, 0] + w * u
                total[l, 1] = w * v if m == 0 else total[l, 1] + w * v
        for l in levels:
            vel_ref[l * oy : (l + 1) * oy, :] = total[l, 0]
            vel_ref[(lev + l) * oy : (lev + l + 1) * oy, :] = total[l, 1]


def pairings(n_row, n_col):
    def place(r, c):
        return r * n_col + c

    row_even = [(place(r, c), place(r ^ 1, c)) for r in range(n_row) for c in range(n_col)]
    row_odd = []
    for r in range(n_row):
        other = r + 1 if r % 2 else r - 1
        for c in range(n_col):
            if 0 <= other < n_row:
                row_odd.append((place(r, c), place(other, c)))
            else:
                row_odd.append((place(r, c), place(r, (c + n_col // 2) % n_col)))
    col_even = [(c, c ^ 1) for c in range(n_col)]
    col_odd = [(c, (c + 1 if c % 2 else c - 1) % n_col) for c in range(n_col)]
    return row_even, row_odd, col_even, col_odd


def shards(
    n_row,
    n_col,
    spectra,
    wind,
    wave_current,
    wave_wet,
    interaction,
    input_rate,
    eta_gain,
    stress_map,
    stokes_map,
    ocean_vel,
    ocean_eta,
    ocean_wet,
    coriolis,
    tau_profile,
    stokes_profile,
    thickness,
    mix_inverse,
    fold_index,
    wave_send,
    ocean_recv,
    ocean_send,
    wave_recv,
):
    spec, rows, lanes = spectra.shape
    cells = rows * lanes
    oy, ox = ocean_eta.shape
    lev = ocean_vel.shape[1]
    planes = 2 * lev
    nfreq = input_rate.shape[0]
    slot = wave_send.shape[-1]
    pad = -(-planes // 16) * 16
    heading = ((np.arange(NDIR)).astype(np.float32) + 0.5) * np.float32(2.0 * math.pi / NDIR)
    trig = np.concatenate([np.cos(heading), np.sin(heading)]).astype(np.float32)
    trig = jnp.asarray(np.repeat(trig[:, None], lanes, axis=1))
    pairs = pairings(n_row, n_col)
    both = ("row", "col")
    ocean_w = ocean_recv.reshape(3 * slot, oy * ox)
    wave_w = wave_recv.reshape(3 * slot, cells)
    wsend, osend = wave_send.reshape(3, slot), ocean_send.reshape(3, slot)
    fold = fold_index.reshape(1, ox)
    velocity = ocean_vel.reshape(planes * oy, ox)
    eta = ocean_eta
    whole = n_col != 4

    def trade_rows(to_even, to_odd):
        return lax.ppermute(to_odd, both, pairs[1]), lax.ppermute(to_even, both, pairs[0])

    slots_out = [((8, slot), bf16)] * 3
    wave_outs = [((spec, cells), bf16)] + slots_out
    for step in range(STEPS):
        if step == 0:
            updated, to_even, to_odd, own = call(
                functools.partial(k_wave_first, nfreq),
                wave_outs,
                [VMEM] * 5 + [SMEM] * 2 + [VMEM] * 4,
                [
                    pltpu.VMEM((spec * rows, lanes), f32),
                    pltpu.VMEM((spec, cells), bf16),
                    pltpu.VMEM((spec, cells), f32),
                    pltpu.VMEM((2 * NDIR, cells), f32),
                ],
                "wave_first",
            )(
                spectra.reshape(spec * rows, lanes), wind, wave_current, wave_wet, interaction,
                input_rate, eta_gain, stress_map, stokes_map, trig, wsend,
            )
        else:
            updated, to_even, to_odd, own = call(
                functools.partial(k_wave_next, nfreq, n_row),
                wave_outs,
                [VMEM] * 9 + [SMEM] * 2 + [VMEM] * 3,
                [pltpu.VMEM((8, cells), f32)],
                "wave_next",
            )(
                got_even, got_odd, own, wave_w, updated, moved, q, wind, wave_wet,
                input_rate, eta_gain, stokes_map, trig, wsend,
            )
        got_odd, got_even = trade_rows(to_even, to_odd)
        if step + 1 < STEPS:
            moved, q = call(
                functools.partial(k_transfer, nfreq),
                [((spec, cells), f32), ((2 * NDIR, cells), f32)],
                [VMEM] * 3 + [SMEM],
                name="transfer",
            )(updated, interaction, stress_map, input_rate)
        else:
            (spectra_out,) = call(
                functools.partial(k_spectra_out, rows),
                [((spec * rows, lanes), bf16)],
                [VMEM],
                [pltpu.VMEM((spec * rows, lanes), f32)],
                "spectra_out",
            )(updated)
        forced, row_even, row_odd, col_even, col_odd = call(
            functools.partial(k_force, n_row, lev, pad),
            [((planes * oy, ox), f32)] + [((planes, ox), bf16)] * 2 + [((pad + 16, ox), bf16)] * 2,
            [VMEM] * 7 + [SMEM] * 2,
            [pltpu.VMEM((8 * oy, ox), f32)],
            "force",
        )(got_even, got_odd, own, ocean_w, velocity, ocean_wet, coriolis, tau_profile, stokes_profile)
        got_row_odd, got_row_even = trade_rows(row_even, row_odd)
        got_col_odd = lax.ppermute(col_odd, "col", pairs[3])
        got_col_even = lax.ppermute(col_even, "col", pairs[2])
        if whole:
            top_line = lax.all_gather(col_even[:planes], "col", axis=0, tiled=True)
        else:
            top_line = fold
        smooth, eta, to_even, to_odd, own = call(
            functools.partial(k_smooth, n_row, n_col, lev, pad, whole),
            [((planes * oy, ox), f32), ((oy, ox), f32)] + slots_out,
            [VMEM] * 9 + [SMEM] * 2 + [VMEM],
            [
                pltpu.VMEM((planes, ox), f32),
                pltpu.VMEM((planes, ox), f32),
                pltpu.VMEM((8 * oy, ox), f32),
            ],
            "smooth",
        )(
            forced, got_row_even, got_row_odd, got_col_even, got_col_odd, top_line, fold, eta, ocean_wet,
            thickness, mix_inverse, osend,
        )
        got_odd, got_even = trade_rows(to_even, to_odd)
        (velocity,) = call(
            functools.partial(k_mix, lev, oy), [((planes * oy, ox), f32)], [VMEM, SMEM], name="mix"
        )(smooth, mix_inverse)
    (current,) = call(
        functools.partial(k_current_out, n_row), [((3, rows, lanes), f32)], [VMEM] * 4, name="current_out"
    )(got_even, got_odd, own, wave_w)
    return (
        spectra_out.reshape(spec, rows, lanes),
        velocity.reshape(2, lev, oy, ox),
        eta,
        current,
    )


def solution(mesh):
    n_row, n_col = mesh.shape["row"], mesh.shape["col"]
    in_specs = (
        P(None, "row", "col"),
        P(None, "row", "col"),
        P(None, "row", "col"),
        P("row", "col"),
        P(),
        P(),
        P(),
        P(),
        P(),
        P(None, None, "row", "col"),
        P("row", "col"),
        P("row", "col"),
        P("row", "col"),
        P(),
        P(),
        P(),
        P(),
        P("col"),
        P("row", "col", None, None),
        P("row", "col", None, None, None),
        P("row", "col", None, None),
        P("row", "col", None, None, None),
    )
    out_specs = (
        P(None, "row", "col"),
        P(None, None, "row", "col"),
        P("row", "col"),
        P(None, "row", "col"),
    )
    body = functools.partial(shards, n_row, n_col)
    return jax.shard_map(body, mesh=mesh, in_specs=in_specs, out_specs=out_specs, check_vma=False)
```

```python
import functools
import math

import jax
import jax.numpy as jnp
from jax import lax
from jax.experimental import pallas as pl
from jax.experimental.pallas import tpu as pltpu
from jax.sharding import PartitionSpec as P


NDIR = 24
NBAND = 3
STEPS = 2
viscous = 0.2
surface_rate = 0.5

f32, bf16 = jnp.float32, jnp.bfloat16
VMEM = pl.BlockSpec(memory_space=pltpu.VMEM)
SMEM = pl.BlockSpec(memory_space=pltpu.SMEM)
HBM = pl.BlockSpec(memory_space=pltpu.HBM)


def call(kernel, outs, specs, scratch=()):
    out_shape = tuple(jax.ShapeDtypeStruct(s, d) for s, d in outs)
    return pl.pallas_call(
        kernel,
        out_shape=out_shape,
        in_specs=list(specs),
        out_specs=tuple(VMEM for _ in outs),
        scratch_shapes=list(scratch),
        compiler_params=pltpu.CompilerParams(vmem_limit_bytes=12 << 20),
    )


def dot(a, b):
    return jnp.dot(a, b, preferred_element_type=f32)


def split2(w):
    high = w.astype(bf16)
    low = (w - high.astype(f32)).astype(bf16)
    return high, low


def is_even(index):
    return lax.rem(index, 2) == 0


def stress_rows(smap, rate_ref, nfreq):
    spec = smap.shape[1]
    col = lax.broadcasted_iota(jnp.int32, (1, spec), 1)
    band = jnp.zeros((1, spec), jnp.int32)
    rate = jnp.full((1, spec), rate_ref[0], f32)
    for f in range(1, nfreq):
        past = col >= NDIR * f
        band = band + jnp.where(past, 1, 0)
        rate = jnp.where(past, rate_ref[f], rate)
    direction = col - NDIR * band
    row = lax.broadcasted_iota(jnp.int32, (NDIR, spec), 0)
    keep = row == direction
    weights = [jnp.where(keep, smap[i : i + 1] * rate, 0.0) for i in range(2)]
    weights = jnp.concatenate(weights, axis=0)
    high, low = split2(weights)
    return jnp.concatenate([high.astype(f32), low.astype(f32)], axis=0).astype(bf16)


def transfer(inter, smap, rate_ref, eb, t_ref, q_ref, nfreq):
    t_ref[...] = dot(inter, eb)
    q = dot(stress_rows(smap, rate_ref, nfreq), eb)
    half = 2 * NDIR
    q_ref[...] = q[:half] + q[half:]


def wave_finish(
    e_of, t_ref, q_ref, wind_ref, current_of, wet_ref, rate_ref, gain_ref, kmap, upd_ref, nfreq
):
    rows, lanes = wet_ref.shape
    heading = lax.broadcasted_iota(jnp.int32, (NDIR, lanes), 0).astype(f32)
    heading = (heading + 0.5) * (2.0 * math.pi / NDIR)
    cosine, sine = jnp.cos(heading), jnp.sin(heading)
    stress = []
    for y in range(rows):
        cells = slice(y * lanes, (y + 1) * lanes)
        dx = wind_ref[0, y : y + 1, :] - current_of(0, y)
        dy = wind_ref[1, y : y + 1, :] - current_of(1, y)
        level = current_of(2, y)
        wet = wet_ref[y : y + 1, :].astype(f32)
        relative = dx * cosine + dy * sine
        soft = jnp.maximum(relative, 0.0) + jnp.log1p(jnp.exp(-jnp.abs(relative)))
        stress.append(
            [
                jnp.sum(soft * q_ref[i * NDIR : (i + 1) * NDIR, cells], axis=0, keepdims=True)
                for i in range(2)
            ]
        )
        rate = jnp.concatenate(
            [rate_ref[f] * soft + gain_ref[f] * level for f in range(nfreq)], axis=0
        )
        e = e_of(y)
        upd_ref[:, cells] = (wet * (e + rate * e + t_ref[:, cells])).astype(bf16)
    high, low = split2(kmap)
    pair = jnp.concatenate([high.astype(f32), low.astype(f32)], axis=0).astype(bf16)
    stokes = dot(pair, upd_ref[...])
    bands = 2 * NBAND
    stokes = stokes[:bands] + stokes[bands:]
    stress = jnp.concatenate(
        [jnp.concatenate([stress[y][i] for y in range(rows)], axis=1) for i in range(2)], axis=0
    )
    return jnp.concatenate([stress, stokes], axis=0)


def pick(fields, send, outs):
    to_even, to_odd, own = outs
    slot = send.shape[2]
    index = jnp.concatenate([send[j] for j in range(3)], axis=1)
    cell = lax.broadcasted_iota(jnp.int32, (fields.shape[1], 3 * slot), 0)
    hot = jnp.where(cell == index, 1.0, 0.0).astype(bf16)
    slots = dot(fields.astype(bf16), hot)
    even = is_even(lax.axis_index("row"))
    south, north = slots[:, :slot], slots[:, 2 * slot :]
    to_even[...] = jnp.where(even, north, south).astype(bf16)
    to_odd[...] = jnp.where(even, south, north).astype(bf16)
    own[...] = slots[:, slot : 2 * slot].astype(bf16)


def gather_slots(got_even, got_odd, own, rows):
    row = lax.axis_index("row")
    even = is_even(row)
    a, b = got_even[...].astype(f32), got_odd[...].astype(f32)
    north = jnp.where(row == rows - 1, 0.0, jnp.where(even, a, b))
    south = jnp.where(row == 0, 0.0, jnp.where(even, b, a))
    return jnp.concatenate([north, own[...].astype(f32), south], axis=1).astype(bf16)


def k_wave_first(
    nfreq,
    spec_hbm, inter_hbm, smap_hbm, rate_hbm, wind_hbm, cur_hbm, wet_hbm, gain_hbm, kmap_hbm, send_hbm,
    upd_ref, to_even, to_odd, own,
    spec_ref, inter_ref, smap_ref, rate_ref, wind_ref, cur_ref, wet_ref, gain_ref, kmap_ref, send_ref,
    ef, eb, t, q, sems,
):
    sources = (spec_hbm, inter_hbm, smap_hbm, rate_hbm, wind_hbm, cur_hbm, wet_hbm, gain_hbm, kmap_hbm, send_hbm)
    held = (spec_ref, inter_ref, smap_ref, rate_ref, wind_ref, cur_ref, wet_ref, gain_ref, kmap_ref, send_ref)
    copies = [pltpu.make_async_copy(a, b, sems.at[i]) for i, (a, b) in enumerate(zip(sources, held))]
    for copy in copies:
        copy.start()
    rows, lanes = wet_ref.shape
    spec = inter_ref.shape[0]
    copies[0].wait()
    ef[...] = spec_ref[...].astype(f32)
    for y in range(rows):
        eb[:, y * lanes : (y + 1) * lanes] = ef[pl.ds(y, spec, stride=rows), :].astype(bf16)
    for copy in copies[1:]:
        copy.wait()
    transfer(inter_ref[...], smap_ref[...], rate_ref, eb[...], t, q, nfreq)
    fields = wave_finish(
        lambda y: ef[pl.ds(y, spec, stride=rows), :],
        t, q, wind_ref,
        lambda i, y: cur_ref[i, y : y + 1, :],
        wet_ref, rate_ref, gain_ref, kmap_ref[...], upd_ref, nfreq,
    )
    pick(fields, send_ref, (to_even, to_odd, own))


def k_transfer(nfreq, upd_ref, inter_ref, smap_ref, rate_ref, t_ref, q_ref):
    transfer(inter_ref[...], smap_ref[...], rate_ref, upd_ref[...], t_ref, q_ref, nfreq)


def k_wave_next(
    nfreq, n_row,
    got_even, got_odd, got_own, recv_ref, old_ref, t_ref, q_ref, wind_ref, wet_ref, rate_ref, gain_ref, kmap_ref, send_ref,
    upd_ref, to_even, to_odd, own,
    cur,
):
    lanes = wet_ref.shape[1]
    slots = gather_slots(got_even, got_odd, got_own, n_row)
    cur[...] = dot(slots, recv_ref[...])
    fields = wave_finish(
        lambda y: old_ref[:, y * lanes : (y + 1) * lanes].astype(f32),
        t_ref, q_ref, wind_ref,
        lambda i, y: cur[i : i + 1, y * lanes : (y + 1) * lanes],
        wet_ref, rate_ref, gain_ref, kmap_ref[...], upd_ref, nfreq,
    )
    pick(fields, send_ref, (to_even, to_odd, own))


def k_spectra_out(rows, upd_ref, out_ref, wide):
    spec = upd_ref.shape[0]
    lanes = out_ref.shape[1]
    for y in range(rows):
        wide[pl.ds(y, spec, stride=rows), :] = upd_ref[:, y * lanes : (y + 1) * lanes].astype(f32)
    out_ref[...] = wide[...].astype(bf16)


def k_current_out(n_row, got_even, got_odd, own, recv_ref, out_ref):
    rows, lanes = out_ref.shape[1:]
    cur = dot(gather_slots(got_even, got_odd, own, n_row), recv_ref[...])
    for i in range(3):
        for y in range(rows):
            out_ref[i, y : y + 1, :] = cur[i : i + 1, y * lanes : (y + 1) * lanes]


def k_force(
    n_row, lev, pad,
    got_even, got_odd, own, recv_ref, vel_ref, wet_ref, cor_ref, tau_ref, prof_ref,
    forced_ref, row_even, row_odd, col_even, col_odd,
    fs,
):
    oy, ox = wet_ref.shape
    planes = 2 * lev
    forcing = dot(gather_slots(got_even, got_odd, own, n_row), recv_ref[...])
    nf = forcing.shape[0]
    for y in range(oy):
        fs[y * nf : (y + 1) * nf, :] = forcing[:, y * ox : (y + 1) * ox]
    field = [fs[pl.ds(i, oy, stride=nf), :] for i in range(nf)]
    wet = wet_ref[...].astype(f32)
    cor = cor_ref[...]
    along = [cor * field[i] for i in range(2, nf)]
    lane = lax.broadcasted_iota(jnp.int32, (oy, ox), 1)
    east = jnp.zeros((oy, ox), f32)
    west = jnp.zeros((oy, ox), f32)
    for i in range(planes):
        c, l = divmod(i, lev)
        accel = tau_ref[l] * field[c]
        for b in range(NBAND):
            term = prof_ref[b, l] * along[2 * b + 1 - c]
            accel = accel + term if c == 0 else accel - term
        value = wet * (vel_ref[i * oy : (i + 1) * oy, :] + accel)
        forced_ref[i * oy : (i + 1) * oy, :] = value
        here = lane == i
        west = jnp.where(here, pltpu.roll(value, i, 1) if i else value, west)
        east = jnp.where(here, pltpu.roll(value, (i + 1) % ox, 1), east)
    bottom = forced_ref[pl.ds(0, planes, stride=oy), :]
    top = forced_ref[pl.ds(oy - 1, planes, stride=oy), :]
    even = is_even(lax.axis_index("row"))
    row_even[...] = jnp.where(even, top, bottom).astype(bf16)
    row_odd[...] = jnp.where(even, bottom, top).astype(bf16)
    even = is_even(lax.axis_index("col"))
    col_even[:planes, :] = top.astype(bf16)
    col_odd[:planes, :] = top.astype(bf16)
    filler = jnp.zeros((16 - oy, ox), f32)
    col_even[pad:, :] = jnp.concatenate([jnp.where(even, east, west), filler], 0).astype(bf16)
    col_odd[pad:, :] = jnp.concatenate([jnp.where(even, west, east), filler], 0).astype(bf16)


def k_smooth(
    n_row, n_col, lev, pad, whole,
    forced_ref, got_row_even, got_row_odd, got_col_even, got_col_odd, line_ref, fold_ref, eta_ref, wet_ref, thick_ref, mix_ref, send_ref,
    smooth_ref, eta_out, to_even, to_odd, own,
    north, south, bs,
):
    oy, ox = wet_ref.shape
    planes = 2 * lev
    row, col = lax.axis_index("row"), lax.axis_index("col")
    even = is_even(row)
    a, b = got_row_even[...].astype(f32), got_row_odd[...].astype(f32)
    if whole:
        pieces = [(line_ref[t * planes : (t + 1) * planes, :], t) for t in range(n_col)]
    else:
        top = forced_ref[pl.ds(oy - 1, planes, stride=oy), :].astype(bf16)
        pair_even = jnp.where(is_even(col), col + 1, col - 1)
        pair_odd = lax.rem(jnp.where(is_even(col), col - 1, col + 1) + n_col, n_col)
        pieces = [
            (top, col),
            (got_col_even[:planes, :], pair_even),
            (got_col_odd[:planes, :], pair_odd),
            (got_row_odd[...], lax.rem(col + n_col // 2, n_col)),
        ]
    cell = lax.broadcasted_iota(jnp.int32, (ox, ox), 0)
    across = None
    for piece, tile in pieces:
        hot = jnp.where(cell == fold_ref[...] - tile * ox, 1.0, 0.0).astype(bf16)
        part = dot(piece, hot)
        across = part if across is None else across + part
    north[...] = jnp.where(row == n_row - 1, -across, jnp.where(even, a, b))
    south[...] = jnp.where(row == 0, 0.0, jnp.where(even, b, a))
    even = is_even(col)
    a = got_col_even[pad:, :].astype(f32)[:oy]
    b = got_col_odd[pad:, :].astype(f32)[:oy]
    east_col = jnp.where(even, a, b)
    west_col = jnp.where(even, b, a)
    wet = wet_ref[...].astype(f32)
    lane = lax.broadcasted_iota(jnp.int32, (oy, ox), 1)
    line = lax.broadcasted_iota(jnp.int32, (oy, ox), 0)
    is_top, is_bottom = line == oy - 1, line == 0
    is_east, is_west = lane == ox - 1, lane == 0
    across_u = jnp.zeros((oy, ox), f32)
    across_v = jnp.zeros((oy, ox), f32)
    surface = []
    for i in range(planes):
        c, l = divmod(i, lev)
        here = forced_ref[i * oy : (i + 1) * oy, :]
        up = jnp.where(is_top, north[i : i + 1, :], pltpu.roll(here, oy - 1, 0))
        down = jnp.where(is_bottom, south[i : i + 1, :], pltpu.roll(here, 1, 0))
        right = jnp.where(is_east, pltpu.roll(east_col, (ox - 1 - i) % ox, 1), pltpu.roll(here, ox - 1, 1))
        left = jnp.where(is_west, pltpu.roll(west_col, (ox - i) % ox, 1), pltpu.roll(here, 1, 1))
        smooth = wet * (here + viscous * (up + down + right + left - 4.0 * here))
        smooth_ref[i * oy : (i + 1) * oy, :] = smooth
        if l == 0:
            surface.append(mix_ref[0, 0] * smooth)
        else:
            surface[c] = surface[c] + mix_ref[0, l] * smooth
        if c == 0:
            across_u = across_u + thick_ref[l] * (right - left)
        else:
            across_v = across_v + thick_ref[l] * (up - down)
    eta = wet * (eta_ref[...] - surface_rate * (0.5 * across_u + 0.5 * across_v))
    eta_out[...] = eta
    bs[: oy, :] = surface[0]
    bs[oy : 2 * oy, :] = surface[1]
    bs[2 * oy : 3 * oy, :] = eta
    bs[3 * oy :, :] = jnp.zeros((5 * oy, ox), f32)
    back = jnp.concatenate([bs[pl.ds(y, 8, stride=oy), :] for y in range(oy)], axis=1)
    pick(back, send_ref, (to_even, to_odd, own))


def k_mix(lev, oy, smooth_ref, mix_ref, vel_ref):
    group = 6
    for first in range(0, lev, group):
        levels = range(first, min(first + group, lev))
        total = {}
        for m in range(lev):
            u = smooth_ref[m * oy : (m + 1) * oy, :]
            v = smooth_ref[(lev + m) * oy : (lev + m + 1) * oy, :]
            for l in levels:
                w = mix_ref[l, m]
                total[l, 0] = w * u if m == 0 else total[l, 0] + w * u
                total[l, 1] = w * v if m == 0 else total[l, 1] + w * v
        for l in levels:
            vel_ref[l * oy : (l + 1) * oy, :] = total[l, 0]
            vel_ref[(lev + l) * oy : (lev + l + 1) * oy, :] = total[l, 1]


def pairings(n_row, n_col):
    def place(r, c):
        return r * n_col + c

    row_even = [(place(r, c), place(r ^ 1, c)) for r in range(n_row) for c in range(n_col)]
    row_odd = []
    for r in range(n_row):
        other = r + 1 if r % 2 else r - 1
        for c in range(n_col):
            if 0 <= other < n_row:
                row_odd.append((place(r, c), place(other, c)))
            else:
                row_odd.append((place(r, c), place(r, (c + n_col // 2) % n_col)))
    col_even = [(c, c ^ 1) for c in range(n_col)]
    col_odd = [(c, (c + 1 if c % 2 else c - 1) % n_col) for c in range(n_col)]
    return dict(row_even=row_even, row_odd=row_odd, col_even=col_even, col_odd=col_odd)


def shards(
    n_row,
    n_col,
    spectra,
    wind,
    wave_current,
    wave_wet,
    interaction,
    input_rate,
    eta_gain,
    stress_map,
    stokes_map,
    ocean_vel,
    ocean_eta,
    ocean_wet,
    coriolis,
    tau_profile,
    stokes_profile,
    thickness,
    mix_inverse,
    fold_index,
    wave_send,
    ocean_recv,
    ocean_send,
    wave_recv,
):
    spec, rows, lanes = spectra.shape
    cells = rows * lanes
    oy, ox = ocean_eta.shape
    lev = ocean_vel.shape[1]
    planes = 2 * lev
    nfreq = input_rate.shape[0]
    slot = wave_send.shape[-1]
    pad = -(-planes // 16) * 16
    pairs = pairings(n_row, n_col)
    both = ("row", "col")
    ocean_w = ocean_recv.reshape(3 * slot, oy * ox)
    wave_w = wave_recv.reshape(3 * slot, cells)
    wsend, osend = wave_send.reshape(3, 1, slot), ocean_send.reshape(3, 1, slot)
    fold = fold_index.reshape(1, ox)
    velocity = ocean_vel.reshape(planes * oy, ox)
    eta = ocean_eta
    whole = n_col != 4

    def trade(label, array):
        axis = both if label.startswith("row") else "col"
        return lax.ppermute(array, axis, pairs[label])

    slots_out = [((8, slot), bf16)] * 3
    wave_outs = [((spec, cells), bf16)] + slots_out
    for step in range(STEPS):
        if step == 0:
            inputs = (
                spectra.reshape(spec * rows, lanes), interaction, stress_map, input_rate, wind, wave_current,
                wave_wet, eta_gain, stokes_map, wsend,
            )
            held = [(pltpu.SMEM if x.ndim == 1 else pltpu.VMEM)(x.shape, x.dtype) for x in inputs]
            updated, to_even, to_odd, own = call(
                functools.partial(k_wave_first, nfreq),
                wave_outs,
                [HBM] * len(inputs),
                held
                + [
                    pltpu.VMEM((spec * rows, lanes), f32),
                    pltpu.VMEM((spec, cells), bf16),
                    pltpu.VMEM((spec, cells), f32),
                    pltpu.VMEM((2 * NDIR, cells), f32),
                    pltpu.SemaphoreType.DMA((len(inputs),)),
                ],
            )(*(pltpu.with_memory_space_constraint(x, pltpu.HBM) for x in inputs))
        else:
            updated, to_even, to_odd, own = call(
                functools.partial(k_wave_next, nfreq, n_row),
                wave_outs,
                [VMEM] * 9 + [SMEM] * 2 + [VMEM] * 2,
                [pltpu.VMEM((8, cells), f32)],
            )(
                got_even, got_odd, own, wave_w, updated, moved, q, wind, wave_wet,
                input_rate, eta_gain, stokes_map, wsend,
            )
        got_odd, got_even = trade("row_odd", to_odd), trade("row_even", to_even)
        if step + 1 < STEPS:
            moved, q = call(
                functools.partial(k_transfer, nfreq),
                [((spec, cells), f32), ((2 * NDIR, cells), f32)],
                [VMEM] * 3 + [SMEM],
            )(updated, interaction, stress_map, input_rate)
        forced, row_even, row_odd, col_even, col_odd = call(
            functools.partial(k_force, n_row, lev, pad),
            [((planes * oy, ox), f32)] + [((planes, ox), bf16)] * 2 + [((pad + 16, ox), bf16)] * 2,
            [VMEM] * 7 + [SMEM] * 2,
            [pltpu.VMEM((8 * oy, ox), f32)],
        )(got_even, got_odd, own, ocean_w, velocity, ocean_wet, coriolis, tau_profile, stokes_profile)
        got_row_odd, got_row_even = trade("row_odd", row_odd), trade("row_even", row_even)
        got_col_odd, got_col_even = trade("col_odd", col_odd), trade("col_even", col_even)
        if step + 1 == STEPS:
            (spectra_out,) = call(
                functools.partial(k_spectra_out, rows),
                [((spec * rows, lanes), bf16)],
                [VMEM],
                [pltpu.VMEM((spec * rows, lanes), f32)],
            )(updated)
        if whole:
            top_line = lax.all_gather(col_even[:planes], "col", axis=0, tiled=True)
        else:
            top_line = fold
        smooth, eta, to_even, to_odd, own = call(
            functools.partial(k_smooth, n_row, n_col, lev, pad, whole),
            [((planes * oy, ox), f32), ((oy, ox), f32)] + slots_out,
            [VMEM] * 9 + [SMEM] * 2 + [VMEM],
            [
                pltpu.VMEM((planes, ox), f32),
                pltpu.VMEM((planes, ox), f32),
                pltpu.VMEM((8 * oy, ox), f32),
            ],
        )(
            forced, got_row_even, got_row_odd, got_col_even, got_col_odd, top_line, fold, eta, ocean_wet,
            thickness, mix_inverse, osend,
        )
        got_odd, got_even = trade("row_odd", to_odd), trade("row_even", to_even)
        (velocity,) = call(
            functools.partial(k_mix, lev, oy), [((planes * oy, ox), f32)], [VMEM, SMEM]
        )(smooth, mix_inverse)
    (current,) = call(
        functools.partial(k_current_out, n_row), [((3, rows, lanes), f32)], [VMEM] * 4
    )(got_even, got_odd, own, wave_w)
    return (
        spectra_out.reshape(spec, rows, lanes),
        velocity.reshape(2, lev, oy, ox),
        eta,
        current,
    )


def solution(mesh):
    n_row, n_col = mesh.shape["row"], mesh.shape["col"]
    in_specs = (
        P(None, "row", "col"),
        P(None, "row", "col"),
        P(None, "row", "col"),
        P("row", "col"),
        P(),
        P(),
        P(),
        P(),
        P(),
        P(None, None, "row", "col"),
        P("row", "col"),
        P("row", "col"),
        P("row", "col"),
        P(),
        P(),
        P(),
        P(),
        P("col"),
        P("row", "col", None, None),
        P("row", "col", None, None, None),
        P("row", "col", None, None),
        P("row", "col", None, None, None),
    )
    out_specs = (
        P(None, "row", "col"),
        P(None, None, "row", "col"),
        P("row", "col"),
        P(None, "row", "col"),
    )
    body = functools.partial(shards, n_row, n_col)
    return jax.shard_map(body, mesh=mesh, in_specs=in_specs, out_specs=out_specs, check_vma=False)
```

```python
import functools
import math

import jax
import jax.numpy as jnp
from jax import lax
from jax.experimental import pallas as pl
from jax.experimental.pallas import tpu as pltpu
from jax.sharding import PartitionSpec as P


NDIR = 24
NBAND = 3
STEPS = 2
viscous = 0.2
surface_rate = 0.5

f32, bf16 = jnp.float32, jnp.bfloat16
VMEM = pl.BlockSpec(memory_space=pltpu.VMEM)
SMEM = pl.BlockSpec(memory_space=pltpu.SMEM)
HBM = pl.BlockSpec(memory_space=pltpu.HBM)


def call(kernel, outs, specs, scratch=()):
    out_shape = tuple(jax.ShapeDtypeStruct(s, d) for s, d in outs)
    return pl.pallas_call(
        kernel,
        out_shape=out_shape,
        in_specs=list(specs),
        out_specs=tuple(VMEM for _ in outs),
        scratch_shapes=list(scratch),
        compiler_params=pltpu.CompilerParams(vmem_limit_bytes=12 << 20),
    )


def dot(a, b):
    return jnp.dot(a, b, preferred_element_type=f32)


def split2(w):
    high = w.astype(bf16)
    low = (w - high.astype(f32)).astype(bf16)
    return high, low


def is_even(index):
    return lax.rem(index, 2) == 0


def stress_rows(smap, rate_ref, nfreq):
    spec = smap.shape[1]
    col = lax.broadcasted_iota(jnp.int32, (1, spec), 1)
    band = jnp.zeros((1, spec), jnp.int32)
    rate = jnp.full((1, spec), rate_ref[0], f32)
    for f in range(1, nfreq):
        past = col >= NDIR * f
        band = band + jnp.where(past, 1, 0)
        rate = jnp.where(past, rate_ref[f], rate)
    direction = col - NDIR * band
    row = lax.broadcasted_iota(jnp.int32, (NDIR, spec), 0)
    keep = row == direction
    weights = [jnp.where(keep, smap[i : i + 1] * rate, 0.0) for i in range(2)]
    weights = jnp.concatenate(weights, axis=0)
    high, low = split2(weights)
    return jnp.concatenate([high.astype(f32), low.astype(f32)], axis=0).astype(bf16)


def transfer(inter, weights, eb, t_ref, q_ref):
    t_ref[...] = dot(inter, eb)
    q = dot(weights, eb)
    half = 2 * NDIR
    q_ref[...] = q[:half] + q[half:]


def wave_finish(
    e_of, t_ref, q_ref, wind_ref, current_of, wet_ref, rate_of, gain_of, kmap, upd_ref, nfreq
):
    rows, lanes = wet_ref.shape
    heading = lax.broadcasted_iota(jnp.int32, (NDIR, lanes), 0).astype(f32)
    heading = (heading + 0.5) * (2.0 * math.pi / NDIR)
    cosine, sine = jnp.cos(heading), jnp.sin(heading)
    stress = []
    for y in range(rows):
        cells = slice(y * lanes, (y + 1) * lanes)
        dx = wind_ref[0, y : y + 1, :] - current_of(0, y)
        dy = wind_ref[1, y : y + 1, :] - current_of(1, y)
        level = current_of(2, y)
        wet = wet_ref[y : y + 1, :].astype(f32)
        relative = dx * cosine + dy * sine
        soft = jnp.maximum(relative, 0.0) + jnp.log1p(jnp.exp(-jnp.abs(relative)))
        stress.append(
            [
                jnp.sum(soft * q_ref[i * NDIR : (i + 1) * NDIR, cells], axis=0, keepdims=True)
                for i in range(2)
            ]
        )
        rate = jnp.concatenate(
            [rate_of(f) * soft + gain_of(f) * level for f in range(nfreq)], axis=0
        )
        e = e_of(y)
        upd_ref[:, cells] = (wet * (e + rate * e + t_ref[:, cells])).astype(bf16)
    high, low = split2(kmap)
    pair = jnp.concatenate([high.astype(f32), low.astype(f32)], axis=0).astype(bf16)
    stokes = dot(pair, upd_ref[...])
    bands = 2 * NBAND
    stokes = stokes[:bands] + stokes[bands:]
    stress = jnp.concatenate(
        [jnp.concatenate([stress[y][i] for y in range(rows)], axis=1) for i in range(2)], axis=0
    )
    return jnp.concatenate([stress, stokes], axis=0)


def pick(fields, send, outs):
    to_even, to_odd, own = outs
    slot = send.shape[2]
    index = jnp.concatenate([send[j] for j in range(3)], axis=1)
    cell = lax.broadcasted_iota(jnp.int32, (fields.shape[1], 3 * slot), 0)
    hot = jnp.where(cell == index, 1.0, 0.0).astype(bf16)
    slots = dot(fields.astype(bf16), hot)
    even = is_even(lax.axis_index("row"))
    south, north = slots[:, :slot], slots[:, 2 * slot :]
    to_even[...] = jnp.where(even, north, south).astype(bf16)
    to_odd[...] = jnp.where(even, south, north).astype(bf16)
    own[...] = slots[:, slot : 2 * slot].astype(bf16)


def gather_slots(got_even, got_odd, own, rows):
    row = lax.axis_index("row")
    even = is_even(row)
    a, b = got_even[...].astype(f32), got_odd[...].astype(f32)
    north = jnp.where(row == rows - 1, 0.0, jnp.where(even, a, b))
    south = jnp.where(row == 0, 0.0, jnp.where(even, b, a))
    return jnp.concatenate([north, own[...].astype(f32), south], axis=1).astype(bf16)


def k_wave_first(
    nfreq,
    spec_hbm, inter_hbm, smap_hbm, rate_hbm, wind_hbm, cur_hbm, wet_hbm, gain_hbm, kmap_hbm, send_hbm,
    upd_ref, to_even, to_odd, own, weight_ref,
    spec_ref, inter_ref, smap_ref, rate_ref, wind_ref, cur_ref, wet_ref, gain_ref, kmap_ref, send_ref,
    ef, eb, t, q, sems,
):
    sources = (spec_hbm, inter_hbm, smap_hbm, rate_hbm, wind_hbm, cur_hbm, wet_hbm, gain_hbm, kmap_hbm, send_hbm)
    held = (spec_ref, inter_ref, smap_ref, rate_ref, wind_ref, cur_ref, wet_ref, gain_ref, kmap_ref, send_ref)
    copies = [pltpu.make_async_copy(a, b, sems.at[i]) for i, (a, b) in enumerate(zip(sources, held))]
    for copy in copies:
        copy.start()
    rows, lanes = wet_ref.shape
    spec = inter_ref.shape[0]
    copies[0].wait()
    ef[...] = spec_ref[...].astype(f32)
    for y in range(rows):
        eb[:, y * lanes : (y + 1) * lanes] = ef[pl.ds(y, spec, stride=rows), :].astype(bf16)
    for copy in copies[1:]:
        copy.wait()
    weight_ref[...] = stress_rows(smap_ref[...], rate_ref, nfreq)
    transfer(inter_ref[...], weight_ref[...], eb[...], t, q)
    fields = wave_finish(
        lambda y: ef[pl.ds(y, spec, stride=rows), :],
        t, q, wind_ref,
        lambda i, y: cur_ref[i, y : y + 1, :],
        wet_ref, lambda f: rate_ref[f], lambda f: gain_ref[f], kmap_ref[...], upd_ref, nfreq,
    )
    pick(fields, send_ref, (to_even, to_odd, own))


def k_transfer(upd_ref, inter_ref, weight_ref, t_ref, q_ref):
    transfer(inter_ref[...], weight_ref[...], upd_ref[...], t_ref, q_ref)


def k_wave_next(
    nfreq, n_row,
    got_even, got_odd, got_own, recv_ref, old_ref, t_ref, q_ref, wind_ref, wet_ref, coef_ref, kmap_ref, send_ref,
    upd_ref, to_even, to_odd, own,
    cur,
):
    lanes = wet_ref.shape[1]
    slots = gather_slots(got_even, got_odd, got_own, n_row)
    cur[...] = dot(slots, recv_ref[...])
    fields = wave_finish(
        lambda y: old_ref[:, y * lanes : (y + 1) * lanes].astype(f32),
        t_ref, q_ref, wind_ref,
        lambda i, y: cur[i : i + 1, y * lanes : (y + 1) * lanes],
        wet_ref, row_of(coef_ref, RATE), row_of(coef_ref, GAIN), kmap_ref[...], upd_ref, nfreq,
    )
    pick(fields, send_ref, (to_even, to_odd, own))


def k_spectra_out(rows, upd_ref, out_ref, wide):
    spec = upd_ref.shape[0]
    lanes = out_ref.shape[1]
    for y in range(rows):
        wide[pl.ds(y, spec, stride=rows), :] = upd_ref[:, y * lanes : (y + 1) * lanes].astype(f32)
    out_ref[...] = wide[...].astype(bf16)


def k_current_out(n_row, got_even, got_odd, own, recv_ref, out_ref):
    rows, lanes = out_ref.shape[1:]
    cur = dot(gather_slots(got_even, got_odd, own, n_row), recv_ref[...])
    for i in range(3):
        for y in range(rows):
            out_ref[i, y : y + 1, :] = cur[i : i + 1, y * lanes : (y + 1) * lanes]


TAU, PROF, THICK, SURF, RATE, GAIN = 0, 1, 1 + NBAND, 2 + NBAND, 3 + NBAND, 4 + NBAND


def row_of(coef_ref, which):
    return lambda l: coef_ref[which * 32 + l : which * 32 + l + 1, :]


def column(vector, first, count):
    row = lax.broadcasted_iota(jnp.int32, (count, vector.shape[1]), 0)
    lane = lax.broadcasted_iota(jnp.int32, (count, vector.shape[1]), 1)
    picked = jnp.sum(jnp.where(row - first == lane, vector, 0.0), axis=1, keepdims=True)
    return jnp.broadcast_to(picked, (count, 128))


def spread(vector, first):
    lev = vector.shape[1]
    parts = [vector, jnp.zeros((1, 128 - lev - first), f32)]
    if first:
        parts = [jnp.zeros((1, first), f32)] + parts
    return jnp.concatenate(parts, axis=1)


def k_prepare(lev, tau_ref, prof_ref, thick_ref, mix_ref, rate_ref, gain_ref, coef_ref, side_ref, lane_ref):
    surf = mix_ref[0:1, :]
    vectors = [tau_ref[...]] + [prof_ref[b : b + 1, :] for b in range(NBAND)]
    vectors += [thick_ref[...], surf, rate_ref[...], gain_ref[...]]
    for i, vector in enumerate(vectors):
        coef_ref[i * 32 : (i + 1) * 32, :] = column(vector, 0, 32)
    side_ref[0] = column(surf, 0, 2 * lev)
    side_ref[1] = column(surf, lev, 2 * lev)
    side_ref[2] = column(thick_ref[...], lev, 2 * lev)
    lane_ref[0:1, :] = spread(surf, 0)
    lane_ref[1:2, :] = spread(surf, lev)
    lane_ref[2:3, :] = spread(thick_ref[...], 0)


def k_force(
    n_row, lev, pad,
    got_even, got_odd, own, recv_ref, vel_ref, wet_ref, cor_ref, coef_ref,
    forced_ref, row_even, row_odd, col_even, col_odd,
    fs,
):
    oy, ox = wet_ref.shape
    planes = 2 * lev
    forcing = dot(gather_slots(got_even, got_odd, own, n_row), recv_ref[...])
    nf = forcing.shape[0]
    for y in range(oy):
        fs[y * nf : (y + 1) * nf, :] = forcing[:, y * ox : (y + 1) * ox]
    field = [fs[pl.ds(i, oy, stride=nf), :] for i in range(nf)]
    wet = wet_ref[...].astype(f32)
    cor = cor_ref[...]
    along = [cor * field[i] for i in range(2, nf)]
    tau = row_of(coef_ref, TAU)
    prof = [row_of(coef_ref, PROF + b) for b in range(NBAND)]
    lane = lax.broadcasted_iota(jnp.int32, (oy, ox), 1)
    east = jnp.zeros((oy, ox), f32)
    west = jnp.zeros((oy, ox), f32)
    for i in range(planes):
        c, l = divmod(i, lev)
        accel = tau(l) * field[c]
        for b in range(NBAND):
            term = prof[b](l) * along[2 * b + 1 - c]
            accel = accel + term if c == 0 else accel - term
        value = wet * (vel_ref[i * oy : (i + 1) * oy, :] + accel)
        forced_ref[i * oy : (i + 1) * oy, :] = value
        here = lane == i
        west = jnp.where(here, pltpu.roll(value, i, 1) if i else value, west)
        east = jnp.where(here, pltpu.roll(value, (i + 1) % ox, 1), east)
    bottom = forced_ref[pl.ds(0, planes, stride=oy), :]
    top = forced_ref[pl.ds(oy - 1, planes, stride=oy), :]
    even = is_even(lax.axis_index("row"))
    row_even[...] = jnp.where(even, top, bottom).astype(bf16)
    row_odd[...] = jnp.where(even, bottom, top).astype(bf16)
    even = is_even(lax.axis_index("col"))
    col_even[:planes, :] = top.astype(bf16)
    col_odd[:planes, :] = top.astype(bf16)
    filler = jnp.zeros((16 - oy, ox), f32)
    col_even[pad:, :] = jnp.concatenate([jnp.where(even, east, west), filler], 0).astype(bf16)
    col_odd[pad:, :] = jnp.concatenate([jnp.where(even, west, east), filler], 0).astype(bf16)


def borders(oy, ox):
    lane = lax.broadcasted_iota(jnp.int32, (oy, ox), 1)
    line = lax.broadcasted_iota(jnp.int32, (oy, ox), 0)
    return line == oy - 1, line == 0, lane == ox - 1, lane == 0


def k_interior(lev, forced_ref, eta_ref, wet_ref, coef_ref, part_ref, sums_ref):
    oy, ox = wet_ref.shape
    wet = wet_ref[...].astype(f32)
    is_top, is_bottom, is_east, is_west = borders(oy, ox)
    thick, surf = row_of(coef_ref, THICK), row_of(coef_ref, SURF)
    across = jnp.zeros((oy, ox), f32)
    surface = [jnp.zeros((oy, ox), f32), jnp.zeros((oy, ox), f32)]
    for i in range(2 * lev):
        c, l = divmod(i, lev)
        here = forced_ref[i * oy : (i + 1) * oy, :]
        up = jnp.where(is_top, 0.0, pltpu.roll(here, oy - 1, 0))
        down = jnp.where(is_bottom, 0.0, pltpu.roll(here, 1, 0))
        right = jnp.where(is_east, 0.0, pltpu.roll(here, ox - 1, 1))
        left = jnp.where(is_west, 0.0, pltpu.roll(here, 1, 1))
        part = wet * (here + viscous * (up + down + right + left - 4.0 * here))
        part_ref[i * oy : (i + 1) * oy, :] = part
        surface[c] = surface[c] + surf(l) * part
        across = across + thick(l) * (right - left if c == 0 else up - down)
    sums_ref[:oy, :] = surface[0]
    sums_ref[oy : 2 * oy, :] = surface[1]
    sums_ref[2 * oy :, :] = wet * (eta_ref[...] - surface_rate * 0.5 * across)


def k_back(
    n_row, n_col, pad, whole,
    got_row_even, got_row_odd, got_col_even, got_col_odd, sent_col, line_ref, fold_ref, sums_ref, wet_ref, side_ref, lane_ref, send_ref,
    eta_out, to_even, to_odd, own, north_ref, south_ref, ends_ref,
    bs,
):
    oy, ox = wet_ref.shape
    planes = got_row_even.shape[0]
    row, col = lax.axis_index("row"), lax.axis_index("col")
    even = is_even(row)
    a, b = got_row_even[...].astype(f32), got_row_odd[...].astype(f32)
    if whole:
        pieces = [(line_ref[t * planes : (t + 1) * planes, :], t) for t in range(n_col)]
    else:
        pair_even = jnp.where(is_even(col), col + 1, col - 1)
        pair_odd = lax.rem(jnp.where(is_even(col), col - 1, col + 1) + n_col, n_col)
        pieces = [
            (sent_col[:planes, :], col),
            (got_col_even[:planes, :], pair_even),
            (got_col_odd[:planes, :], pair_odd),
            (got_row_odd[...], lax.rem(col + n_col // 2, n_col)),
        ]
    cell = lax.broadcasted_iota(jnp.int32, (ox, ox), 0)
    across = None
    for piece, tile in pieces:
        hot = jnp.where(cell == fold_ref[...] - tile * ox, 1.0, 0.0).astype(bf16)
        part = dot(piece, hot)
        across = part if across is None else across + part
    north = jnp.where(row == n_row - 1, -across, jnp.where(even, a, b))
    south = jnp.where(row == 0, 0.0, jnp.where(even, b, a))
    even = is_even(col)
    a = got_col_even[pad:, :].astype(f32)[:oy]
    b = got_col_odd[pad:, :].astype(f32)[:oy]
    east, west = jnp.where(even, a, b), jnp.where(even, b, a)
    north_ref[...] = north
    south_ref[...] = south
    ends_ref[:oy, :] = east
    ends_ref[oy:, :] = west
    wet = wet_ref[...].astype(f32)
    is_top, is_bottom, is_east, is_west = borders(oy, ox)

    def over_rows(x, i):
        return jnp.sum(x * side_ref[i], axis=0, keepdims=True)

    def over_lanes(x, i):
        return jnp.sum(x * lane_ref[i : i + 1, :], axis=1, keepdims=True)

    for c in range(2):
        edge = jnp.where(is_top, over_rows(north, c), 0.0) + jnp.where(is_bottom, over_rows(south, c), 0.0)
        edge = edge + jnp.where(is_east, over_lanes(east, c), 0.0)
        edge = edge + jnp.where(is_west, over_lanes(west, c), 0.0)
        bs[c * oy : (c + 1) * oy, :] = sums_ref[c * oy : (c + 1) * oy, :] + viscous * wet * edge
    flow = jnp.where(is_east, over_lanes(east, 2), 0.0) - jnp.where(is_west, over_lanes(west, 2), 0.0)
    flow = flow + jnp.where(is_top, over_rows(north, 2), 0.0) - jnp.where(is_bottom, over_rows(south, 2), 0.0)
    eta = sums_ref[2 * oy :, :] - surface_rate * 0.5 * wet * flow
    eta_out[...] = eta
    bs[2 * oy : 3 * oy, :] = eta
    bs[3 * oy :, :] = jnp.zeros((5 * oy, ox), f32)
    back = jnp.concatenate([bs[pl.ds(y, 8, stride=oy), :] for y in range(oy)], axis=1)
    pick(back, send_ref, (to_even, to_odd, own))


def k_mix(lev, part_ref, north_ref, south_ref, ends_ref, wet_ref, mix_ref, eta_ref, vel_ref, eta_out, smooth, wide):
    oy, ox = wet_ref.shape
    planes = 2 * lev
    eta_out[...] = eta_ref[...]
    wet = viscous * wet_ref[...].astype(f32)
    is_top, is_bottom, is_east, is_west = borders(oy, ox)
    east, west = ends_ref[:oy, :], ends_ref[oy:, :]
    for i in range(planes):
        edge = jnp.where(is_top, north_ref[i : i + 1, :], 0.0)
        edge = edge + jnp.where(is_bottom, south_ref[i : i + 1, :], 0.0)
        edge = edge + jnp.where(is_east, pltpu.roll(east, (ox - 1 - i) % ox, 1), 0.0)
        edge = edge + jnp.where(is_west, pltpu.roll(west, (ox - i) % ox, 1), 0.0)
        smooth[i * oy : (i + 1) * oy, :] = part_ref[i * oy : (i + 1) * oy, :] + wet * edge
    step = wide.shape[0] // 3
    blocks = [(c, y) for c in range(2) for y in range(oy)]
    for n, (c, y) in enumerate(blocks):
        column_block = smooth[pl.ds(c * lev * oy + y, lev, stride=oy), :]
        column_block = jnp.concatenate([column_block, jnp.zeros((step - lev, ox), f32)], axis=0)
        high, low = split2(column_block)
        cells = slice(n * ox, (n + 1) * ox)
        wide[:step, cells] = high
        wide[step : 2 * step, cells] = low
        wide[2 * step :, cells] = high
    high, low = split2(mix_ref[...])
    filler = jnp.zeros((lev, step - lev), f32)
    high, low = high.astype(f32), low.astype(f32)
    left = jnp.concatenate([high, filler, high, filler, low, filler], axis=1).astype(bf16)
    mixed = dot(left, wide[...])
    for n, (c, y) in enumerate(blocks):
        vel_ref[pl.ds(c * lev * oy + y, lev, stride=oy), :] = mixed[:, n * ox : (n + 1) * ox]


def pairings(n_row, n_col):
    def place(r, c):
        return r * n_col + c

    row_even = [(place(r, c), place(r ^ 1, c)) for r in range(n_row) for c in range(n_col)]
    row_odd = []
    for r in range(n_row):
        other = r + 1 if r % 2 else r - 1
        for c in range(n_col):
            if 0 <= other < n_row:
                row_odd.append((place(r, c), place(other, c)))
            else:
                row_odd.append((place(r, c), place(r, (c + n_col // 2) % n_col)))
    col_even = [(c, c ^ 1) for c in range(n_col)]
    col_odd = [(c, (c + 1 if c % 2 else c - 1) % n_col) for c in range(n_col)]
    return dict(row_even=row_even, row_odd=row_odd, col_even=col_even, col_odd=col_odd)


def shards(
    n_row,
    n_col,
    spectra,
    wind,
    wave_current,
    wave_wet,
    interaction,
    input_rate,
    eta_gain,
    stress_map,
    stokes_map,
    ocean_vel,
    ocean_eta,
    ocean_wet,
    coriolis,
    tau_profile,
    stokes_profile,
    thickness,
    mix_inverse,
    fold_index,
    wave_send,
    ocean_recv,
    ocean_send,
    wave_recv,
):
    spec, rows, lanes = spectra.shape
    cells = rows * lanes
    oy, ox = ocean_eta.shape
    lev = ocean_vel.shape[1]
    planes = 2 * lev
    nfreq = input_rate.shape[0]
    slot = wave_send.shape[-1]
    pad = -(-planes // 16) * 16
    pairs = pairings(n_row, n_col)
    both = ("row", "col")
    ocean_w = ocean_recv.reshape(3 * slot, oy * ox)
    wave_w = wave_recv.reshape(3 * slot, cells)
    wsend, osend = wave_send.reshape(3, 1, slot), ocean_send.reshape(3, 1, slot)
    fold = fold_index.reshape(1, ox)
    velocity = ocean_vel.reshape(planes * oy, ox)
    eta = ocean_eta
    whole = n_col != 4

    def trade(label, array):
        axis = both if label.startswith("row") else "col"
        return lax.ppermute(array, axis, pairs[label])

    slots_out = [((8, slot), bf16)] * 3
    wave_outs = [((spec, cells), bf16)] + slots_out
    full = (planes * oy, ox)
    for step in range(STEPS):
        last = step + 1 == STEPS
        if step == 0:
            inputs = (
                spectra.reshape(spec * rows, lanes), interaction, stress_map, input_rate, wind, wave_current,
                wave_wet, eta_gain, stokes_map, wsend,
            )
            held = [(pltpu.SMEM if x.ndim == 1 else pltpu.VMEM)(x.shape, x.dtype) for x in inputs]
            updated, to_even, to_odd, own, weights = call(
                functools.partial(k_wave_first, nfreq),
                wave_outs + [((4 * NDIR, spec), bf16)],
                [HBM] * len(inputs),
                held
                + [
                    pltpu.VMEM((spec * rows, lanes), f32),
                    pltpu.VMEM((spec, cells), bf16),
                    pltpu.VMEM((spec, cells), f32),
                    pltpu.VMEM((2 * NDIR, cells), f32),
                    pltpu.SemaphoreType.DMA((len(inputs),)),
                ],
            )(*(pltpu.with_memory_space_constraint(x, pltpu.HBM) for x in inputs))
        else:
            updated, to_even, to_odd, own = call(
                functools.partial(k_wave_next, nfreq, n_row), wave_outs, [VMEM] * 12, [pltpu.VMEM((8, cells), f32)]
            )(
                got_even, got_odd, own, wave_w, updated, moved, q, wind, wave_wet,
                coef, stokes_map, wsend,
            )
        got_odd, got_even = trade("row_odd", to_odd), trade("row_even", to_even)
        if step == 0:
            coef, side, lane_rows = call(
                functools.partial(k_prepare, lev),
                [((8 * 32, 128), f32), ((3, planes, 128), f32), ((8, 128), f32)],
                [VMEM] * 6,
            )(
                tau_profile.reshape(1, lev), stokes_profile, thickness.reshape(1, lev), mix_inverse,
                input_rate.reshape(1, nfreq), eta_gain.reshape(1, nfreq),
            )
        if last:
            (spectra_out,) = call(
                functools.partial(k_spectra_out, rows),
                [((spec * rows, lanes), bf16)],
                [VMEM],
                [pltpu.VMEM((spec * rows, lanes), f32)],
            )(updated)
        forced, row_even, row_odd, col_even, col_odd = call(
            functools.partial(k_force, n_row, lev, pad),
            [(full, f32)] + [((planes, ox), bf16)] * 2 + [((pad + 16, ox), bf16)] * 2,
            [VMEM] * 8,
            [pltpu.VMEM((8 * oy, ox), f32)],
        )(got_even, got_odd, own, ocean_w, velocity, ocean_wet, coriolis, coef)
        got_row_odd, got_row_even = trade("row_odd", row_odd), trade("row_even", row_even)
        got_col_odd, got_col_even = trade("col_odd", col_odd), trade("col_even", col_even)
        part, sums = call(
            functools.partial(k_interior, lev), [(full, f32), ((3 * oy, ox), f32)], [VMEM] * 4
        )(forced, eta, ocean_wet, coef)
        if whole:
            top_line = lax.all_gather(col_even[:planes], "col", axis=0, tiled=True)
        else:
            top_line = fold
        eta, to_even, to_odd, own, north, south, ends = call(
            functools.partial(k_back, n_row, n_col, pad, whole),
            [((oy, ox), f32)] + slots_out + [((planes, ox), f32)] * 2 + [((2 * oy, ox), f32)],
            [VMEM] * 12,
            [pltpu.VMEM((8 * oy, ox), f32)],
        )(
            got_row_even, got_row_odd, got_col_even, got_col_odd, col_even, top_line, fold, sums, ocean_wet,
            side, lane_rows, osend,
        )
        got_odd, got_even = trade("row_odd", to_odd), trade("row_even", to_even)
        if not last:
            moved, q = call(
                k_transfer, [((spec, cells), f32), ((2 * NDIR, cells), f32)], [VMEM] * 3
            )(updated, interaction, weights)
        velocity, eta = call(
            functools.partial(k_mix, lev),
            [(full, f32), ((oy, ox), f32)],
            [VMEM] * 7,
            [pltpu.VMEM(full, f32), pltpu.VMEM((96, 2 * oy * ox), bf16)],
        )(part, north, south, ends, ocean_wet, mix_inverse, eta)
    (current,) = call(
        functools.partial(k_current_out, n_row), [((3, rows, lanes), f32)], [VMEM] * 4
    )(got_even, got_odd, own, wave_w)
    return (
        spectra_out.reshape(spec, rows, lanes),
        velocity.reshape(2, lev, oy, ox),
        eta,
        current,
    )


def solution(mesh):
    n_row, n_col = mesh.shape["row"], mesh.shape["col"]
    in_specs = (
        P(None, "row", "col"),
        P(None, "row", "col"),
        P(None, "row", "col"),
        P("row", "col"),
        P(),
        P(),
        P(),
        P(),
        P(),
        P(None, None, "row", "col"),
        P("row", "col"),
        P("row", "col"),
        P("row", "col"),
        P(),
        P(),
        P(),
        P(),
        P("col"),
        P("row", "col", None, None),
        P("row", "col", None, None, None),
        P("row", "col", None, None),
        P("row", "col", None, None, None),
    )
    out_specs = (
        P(None, "row", "col"),
        P(None, None, "row", "col"),
        P("row", "col"),
        P(None, "row", "col"),
    )
    body = functools.partial(shards, n_row, n_col)
    return jax.shard_map(body, mesh=mesh, in_specs=in_specs, out_specs=out_specs, check_vma=False)
```

```python
import functools
import math

import jax
import jax.numpy as jnp
from jax import lax
from jax.experimental import pallas as pl
from jax.experimental.pallas import tpu as pltpu
from jax.sharding import PartitionSpec as P


NDIR = 24
NBAND = 3
STEPS = 2
viscous = 0.2
surface_rate = 0.5

f32, bf16 = jnp.float32, jnp.bfloat16
VMEM = pl.BlockSpec(memory_space=pltpu.VMEM)
SMEM = pl.BlockSpec(memory_space=pltpu.SMEM)
HBM = pl.BlockSpec(memory_space=pltpu.HBM)


def call(kernel, outs, specs, scratch=()):
    out_shape = tuple(jax.ShapeDtypeStruct(s, d) for s, d in outs)
    return pl.pallas_call(
        kernel,
        out_shape=out_shape,
        in_specs=list(specs),
        out_specs=tuple(VMEM for _ in outs),
        scratch_shapes=list(scratch),
        compiler_params=pltpu.CompilerParams(vmem_limit_bytes=12 << 20),
    )


def dot(a, b):
    return jnp.dot(a, b, preferred_element_type=f32)


def split2(w):
    high = w.astype(bf16)
    low = (w - high.astype(f32)).astype(bf16)
    return high, low


def is_even(index):
    return lax.rem(index, 2) == 0


GROUP = 8


def field_weights(smap, kmap, rate_ref, gain_ref, nfreq):
    spec = smap.shape[1]
    col = lax.broadcasted_iota(jnp.int32, (1, spec), 1)
    band = jnp.zeros((1, spec), jnp.int32)
    rate = jnp.full((1, spec), rate_ref[0], f32)
    gain = jnp.full((1, spec), gain_ref[0], f32)
    for f in range(1, nfreq):
        past = col >= NDIR * f
        band = band + jnp.where(past, 1, 0)
        rate = jnp.where(past, rate_ref[f], rate)
        gain = jnp.where(past, gain_ref[f], gain)
    keep = lax.broadcasted_iota(jnp.int32, (NDIR, spec), 0) == col - NDIR * band
    maps = [smap[i : i + 1] for i in range(2)] + [kmap[i : i + 1] for i in range(2 * NBAND)]
    rows = jnp.concatenate([jnp.where(keep, m * rate, 0.0) for m in maps], axis=0)
    return rows, jnp.concatenate([jnp.zeros((2, spec), f32), kmap], axis=0), gain


def rest_weights(stokes, gain, inter):
    high, low = split2(stokes)
    moved = dot(jnp.concatenate([high.astype(f32), low.astype(f32)], axis=0).astype(bf16), inter)
    return jnp.concatenate([stokes * gain, stokes + moved[:GROUP] + moved[GROUP:]], axis=0)


def joined(parts):
    direct = GROUP * NDIR
    rest = parts[direct : direct + 2 * GROUP] + parts[direct + 2 * GROUP :]
    return jnp.concatenate([parts[:direct], rest], axis=0)


def soft_growth(dx, dy):
    heading = lax.broadcasted_iota(jnp.int32, (NDIR, dx.shape[1]), 0).astype(f32)
    heading = (heading + 0.5) * (2.0 * math.pi / NDIR)
    relative = dx * jnp.cos(heading) + dy * jnp.sin(heading)
    return jnp.maximum(relative, 0.0) + jnp.log1p(jnp.exp(-jnp.abs(relative)))


def fields_of(soft, level, wet, parts):
    sums = [
        jnp.sum(soft * parts[i * NDIR : (i + 1) * NDIR], axis=0, keepdims=True) for i in range(GROUP)
    ]
    rest = GROUP * NDIR
    total = jnp.concatenate(sums, axis=0) + level * parts[rest : rest + GROUP] + parts[rest + GROUP :]
    row = lax.broadcasted_iota(jnp.int32, total.shape, 0)
    return jnp.where(row < 2, total, wet * total)


def flat(ref, *first):
    rows = ref.shape[-2]
    return jnp.concatenate([ref[(*first, slice(y, y + 1), slice(None))] for y in range(rows)], axis=1)


def update(old_of, moved_of, soft_ref, wet_ref, coef_ref, nfreq, store):
    rows, lanes = wet_ref.shape
    rate, gain = row_of(coef_ref, RATE), row_of(coef_ref, GAIN)
    for y in range(rows):
        cells = slice(y * lanes, (y + 1) * lanes)
        soft, level = soft_ref[:NDIR, cells], soft_ref[NDIR : NDIR + 1, cells]
        wet = wet_ref[y : y + 1, :].astype(f32)
        growth = jnp.concatenate([rate(f) * soft + gain(f) * level for f in range(nfreq)], axis=0)
        old = old_of(cells)
        store(y, cells, wet * (old + growth * old + moved_of(cells)))


def pick(fields, send, outs):
    to_even, to_odd, own = outs
    slot = send.shape[2]
    index = jnp.concatenate([send[j] for j in range(3)], axis=1)
    cell = lax.broadcasted_iota(jnp.int32, (fields.shape[1], 3 * slot), 0)
    hot = jnp.where(cell == index, 1.0, 0.0).astype(bf16)
    slots = dot(fields.astype(bf16), hot)
    even = is_even(lax.axis_index("row"))
    south, north = slots[:, :slot], slots[:, 2 * slot :]
    to_even[...] = jnp.where(even, north, south).astype(bf16)
    to_odd[...] = jnp.where(even, south, north).astype(bf16)
    own[...] = slots[:, slot : 2 * slot].astype(bf16)


def gather_slots(got_even, got_odd, own, rows):
    row = lax.axis_index("row")
    even = is_even(row)
    a, b = got_even[...].astype(f32), got_odd[...].astype(f32)
    north = jnp.where(row == rows - 1, 0.0, jnp.where(even, a, b))
    south = jnp.where(row == 0, 0.0, jnp.where(even, b, a))
    return jnp.concatenate([north, own[...].astype(f32), south], axis=1).astype(bf16)


def k_wave_first(
    nfreq,
    smap_hbm, kmap_hbm, rate_hbm, gain_hbm, wind_hbm, cur_hbm, wet_hbm, send_hbm, spec_hbm, inter_hbm,
    to_even, to_odd, own, old_ref, soft_ref, weight_ref,
    smap_ref, kmap_ref, rate_ref, gain_ref, wind_ref, cur_ref, wet_ref, send_ref, spec_ref, inter_ref,
    wide, sems,
):
    rows, lanes = wet_ref.shape
    spec = inter_ref.shape[0]
    cut = spec // 32 * 16
    small = (
        (smap_hbm, smap_ref), (kmap_hbm, kmap_ref), (rate_hbm, rate_ref), (gain_hbm, gain_ref),
        (wind_hbm, wind_ref), (cur_hbm, cur_ref), (wet_hbm, wet_ref), (send_hbm, send_ref),
    )
    large = []
    for first, size in ((0, cut), (cut, spec - cut)):
        part = pl.ds(first * rows, size * rows)
        large.append((spec_hbm.at[part], spec_ref.at[part]))
    for first, size in ((0, cut), (cut, spec - cut)):
        part = pl.ds(first, size)
        large.append((inter_hbm.at[part], inter_ref.at[part]))
    copies = [pltpu.make_async_copy(a, b, sems.at[i]) for i, (a, b) in enumerate((*small, *large))]
    for copy in copies:
        copy.start()
    for copy in copies[: len(small)]:
        copy.wait()
    level = flat(cur_ref, 2)
    soft = soft_growth(flat(wind_ref, 0) - flat(cur_ref, 0), flat(wind_ref, 1) - flat(cur_ref, 1))
    soft_ref[:NDIR, :] = soft
    soft_ref[NDIR:, :] = jnp.concatenate([level] * (soft_ref.shape[0] - NDIR), axis=0)
    direct = GROUP * NDIR
    weights, stokes, gain = field_weights(smap_ref[...], kmap_ref[...], rate_ref, gain_ref, nfreq)
    weight_ref[:direct, :] = weights.astype(bf16)
    for n, (first, size) in enumerate(((0, cut), (cut, spec - cut))):
        copies[len(small) + n].wait()
        part = slice(first * rows, (first + size) * rows)
        wide[part, :] = spec_ref[part, :].astype(f32)
        for y in range(rows):
            taken = wide[pl.ds(first * rows + y, size, stride=rows), :]
            old_ref[first : first + size, y * lanes : (y + 1) * lanes] = taken.astype(bf16)
    for copy in copies[len(small) + 2 :]:
        copy.wait()
    half = direct + 2 * GROUP
    rest = rest_weights(stokes, gain, inter_ref[...])
    weight_ref[direct:half, :], weight_ref[half:, :] = split2(rest)
    parts = joined(dot(weight_ref[...], old_ref[...]))
    fields = fields_of(soft, level, flat(wet_ref).astype(f32), parts)
    pick(fields, send_ref, (to_even, to_odd, own))


def k_update(nfreq, old_ref, inter_ref, soft_ref, wet_ref, coef_ref, new_ref, moved):
    moved[...] = dot(inter_ref[...], old_ref[...])

    def store(y, cells, value):
        new_ref[:, cells] = value.astype(bf16)

    update(
        lambda cells: old_ref[:, cells].astype(f32), lambda cells: moved[:, cells],
        soft_ref, wet_ref, coef_ref, nfreq, store,
    )


def k_transfer(old_ref, inter_ref, weight_ref, moved_ref, parts_ref):
    parts_ref[...] = joined(dot(weight_ref[...], old_ref[...]))
    moved_ref[...] = dot(inter_ref[...], old_ref[...])


def k_wave_next(
    n_row,
    got_even, got_odd, got_own, recv_ref, parts_ref, wind_ref, wet_ref, send_ref,
    to_even, to_odd, own, soft_ref,
    cur_ref,
):
    cur_ref[...] = dot(gather_slots(got_even, got_odd, got_own, n_row), recv_ref[...])
    level = cur_ref[2:3, :]
    soft = soft_growth(flat(wind_ref, 0) - cur_ref[0:1, :], flat(wind_ref, 1) - cur_ref[1:2, :])
    soft_ref[:NDIR, :] = soft
    soft_ref[NDIR:, :] = jnp.concatenate([level] * (soft_ref.shape[0] - NDIR), axis=0)
    fields = fields_of(soft, level, flat(wet_ref).astype(f32), parts_ref[...])
    pick(fields, send_ref, (to_even, to_odd, own))


def k_update_last(nfreq, old_ref, moved_ref, soft_ref, wet_ref, coef_ref, out_ref, wide):
    rows, spec = wet_ref.shape[0], old_ref.shape[0]

    def store(y, cells, value):
        wide[pl.ds(y, spec, stride=rows), :] = value

    update(
        lambda cells: old_ref[:, cells].astype(f32), lambda cells: moved_ref[:, cells],
        soft_ref, wet_ref, coef_ref, nfreq, store,
    )
    out_ref[...] = wide[...].astype(bf16)


def k_current_out(n_row, got_even, got_odd, own, recv_ref, out_ref):
    rows, lanes = out_ref.shape[1:]
    cur = dot(gather_slots(got_even, got_odd, own, n_row), recv_ref[...])
    for i in range(3):
        for y in range(rows):
            out_ref[i, y : y + 1, :] = cur[i : i + 1, y * lanes : (y + 1) * lanes]


TAU, PROF, THICK, SURF, RATE, GAIN = 0, 1, 1 + NBAND, 2 + NBAND, 3 + NBAND, 4 + NBAND


def row_of(coef_ref, which):
    return lambda l: coef_ref[which * 32 + l : which * 32 + l + 1, :]


def column(vector, first, count):
    row = lax.broadcasted_iota(jnp.int32, (count, vector.shape[1]), 0)
    lane = lax.broadcasted_iota(jnp.int32, (count, vector.shape[1]), 1)
    picked = jnp.sum(jnp.where(row - first == lane, vector, 0.0), axis=1, keepdims=True)
    return jnp.broadcast_to(picked, (count, 128))


def spread(vector, first):
    lev = vector.shape[1]
    parts = [vector, jnp.zeros((1, 128 - lev - first), f32)]
    if first:
        parts = [jnp.zeros((1, first), f32)] + parts
    return jnp.concatenate(parts, axis=1)


def k_prepare(lev, tau_ref, prof_ref, thick_ref, mix_ref, rate_ref, gain_ref, coef_ref, side_ref, lane_ref):
    surf = mix_ref[0:1, :]
    vectors = [tau_ref[...]] + [prof_ref[b : b + 1, :] for b in range(NBAND)]
    vectors += [thick_ref[...], surf, rate_ref[...], gain_ref[...]]
    for i, vector in enumerate(vectors):
        coef_ref[i * 32 : (i + 1) * 32, :] = column(vector, 0, 32)
    side_ref[0] = column(surf, 0, 2 * lev)
    side_ref[1] = column(surf, lev, 2 * lev)
    side_ref[2] = column(thick_ref[...], lev, 2 * lev)
    lane_ref[0:1, :] = spread(surf, 0)
    lane_ref[1:2, :] = spread(surf, lev)
    lane_ref[2:3, :] = spread(thick_ref[...], 0)


def k_force(
    n_row, lev, pad,
    got_even, got_odd, own, recv_ref, vel_ref, wet_ref, cor_ref, coef_ref,
    forced_ref, row_even, row_odd, col_even, col_odd,
    fs,
):
    oy, ox = wet_ref.shape
    planes = 2 * lev
    forcing = dot(gather_slots(got_even, got_odd, own, n_row), recv_ref[...])
    nf = forcing.shape[0]
    for y in range(oy):
        fs[y * nf : (y + 1) * nf, :] = forcing[:, y * ox : (y + 1) * ox]
    field = [fs[pl.ds(i, oy, stride=nf), :] for i in range(nf)]
    wet = wet_ref[...].astype(f32)
    cor = cor_ref[...]
    along = [cor * field[i] for i in range(2, nf)]
    tau = row_of(coef_ref, TAU)
    prof = [row_of(coef_ref, PROF + b) for b in range(NBAND)]
    lane = lax.broadcasted_iota(jnp.int32, (oy, ox), 1)
    east = jnp.zeros((oy, ox), f32)
    west = jnp.zeros((oy, ox), f32)
    for i in range(planes):
        c, l = divmod(i, lev)
        accel = tau(l) * field[c]
        for b in range(NBAND):
            term = prof[b](l) * along[2 * b + 1 - c]
            accel = accel + term if c == 0 else accel - term
        value = wet * (vel_ref[i * oy : (i + 1) * oy, :] + accel)
        forced_ref[i * oy : (i + 1) * oy, :] = value
        here = lane == i
        west = jnp.where(here, pltpu.roll(value, i, 1) if i else value, west)
        east = jnp.where(here, pltpu.roll(value, (i + 1) % ox, 1), east)
    bottom = forced_ref[pl.ds(0, planes, stride=oy), :]
    top = forced_ref[pl.ds(oy - 1, planes, stride=oy), :]
    even = is_even(lax.axis_index("row"))
    row_even[...] = jnp.where(even, top, bottom).astype(bf16)
    row_odd[...] = jnp.where(even, bottom, top).astype(bf16)
    even = is_even(lax.axis_index("col"))
    col_even[:planes, :] = top.astype(bf16)
    col_odd[:planes, :] = top.astype(bf16)
    filler = jnp.zeros((16 - oy, ox), f32)
    col_even[pad:, :] = jnp.concatenate([jnp.where(even, east, west), filler], 0).astype(bf16)
    col_odd[pad:, :] = jnp.concatenate([jnp.where(even, west, east), filler], 0).astype(bf16)


def borders(oy, ox):
    lane = lax.broadcasted_iota(jnp.int32, (oy, ox), 1)
    line = lax.broadcasted_iota(jnp.int32, (oy, ox), 0)
    return line == oy - 1, line == 0, lane == ox - 1, lane == 0


def k_interior(lev, forced_ref, eta_ref, wet_ref, coef_ref, part_ref, sums_ref):
    oy, ox = wet_ref.shape
    wet = wet_ref[...].astype(f32)
    is_top, is_bottom, is_east, is_west = borders(oy, ox)
    thick, surf = row_of(coef_ref, THICK), row_of(coef_ref, SURF)
    across = jnp.zeros((oy, ox), f32)
    surface = [jnp.zeros((oy, ox), f32), jnp.zeros((oy, ox), f32)]
    for i in range(2 * lev):
        c, l = divmod(i, lev)
        here = forced_ref[i * oy : (i + 1) * oy, :]
        up = jnp.where(is_top, 0.0, pltpu.roll(here, oy - 1, 0))
        down = jnp.where(is_bottom, 0.0, pltpu.roll(here, 1, 0))
        right = jnp.where(is_east, 0.0, pltpu.roll(here, ox - 1, 1))
        left = jnp.where(is_west, 0.0, pltpu.roll(here, 1, 1))
        part = wet * (here + viscous * (up + down + right + left - 4.0 * here))
        part_ref[i * oy : (i + 1) * oy, :] = part
        surface[c] = surface[c] + surf(l) * part
        across = across + thick(l) * (right - left if c == 0 else up - down)
    sums_ref[:oy, :] = surface[0]
    sums_ref[oy : 2 * oy, :] = surface[1]
    sums_ref[2 * oy :, :] = wet * (eta_ref[...] - surface_rate * 0.5 * across)


def k_back(
    n_row, n_col, pad, whole,
    got_row_even, got_row_odd, got_col_even, got_col_odd, sent_col, line_ref, fold_ref, sums_ref, wet_ref, side_ref, lane_ref, send_ref,
    eta_out, to_even, to_odd, own, north_ref, south_ref, ends_ref,
    bs,
):
    oy, ox = wet_ref.shape
    planes = got_row_even.shape[0]
    row, col = lax.axis_index("row"), lax.axis_index("col")
    even = is_even(row)
    a, b = got_row_even[...].astype(f32), got_row_odd[...].astype(f32)
    north_ref[...] = jnp.where(even, a, b)

    @pl.when(row == n_row - 1)
    def _():
        if whole:
            pieces = [(line_ref[t * planes : (t + 1) * planes, :], t) for t in range(n_col)]
        else:
            pair_even = jnp.where(is_even(col), col + 1, col - 1)
            pair_odd = lax.rem(jnp.where(is_even(col), col - 1, col + 1) + n_col, n_col)
            pieces = [
                (sent_col[:planes, :], col),
                (got_col_even[:planes, :], pair_even),
                (got_col_odd[:planes, :], pair_odd),
                (got_row_odd[...], lax.rem(col + n_col // 2, n_col)),
            ]
        cell = lax.broadcasted_iota(jnp.int32, (ox, ox), 0)
        across = None
        for piece, tile in pieces:
            hot = jnp.where(cell == fold_ref[...] - tile * ox, 1.0, 0.0).astype(bf16)
            part = dot(piece, hot)
            across = part if across is None else across + part
        north_ref[...] = -across

    north = north_ref[...]
    south = jnp.where(row == 0, 0.0, jnp.where(even, b, a))
    even = is_even(col)
    a = got_col_even[pad:, :].astype(f32)[:oy]
    b = got_col_odd[pad:, :].astype(f32)[:oy]
    east, west = jnp.where(even, a, b), jnp.where(even, b, a)
    south_ref[...] = south
    ends_ref[:oy, :] = east
    ends_ref[oy:, :] = west
    wet = wet_ref[...].astype(f32)
    is_top, is_bottom, is_east, is_west = borders(oy, ox)

    def over_rows(x, i):
        return jnp.sum(x * side_ref[i], axis=0, keepdims=True)

    def over_lanes(x, i):
        return jnp.sum(x * lane_ref[i : i + 1, :], axis=1, keepdims=True)

    for c in range(2):
        edge = jnp.where(is_top, over_rows(north, c), 0.0) + jnp.where(is_bottom, over_rows(south, c), 0.0)
        edge = edge + jnp.where(is_east, over_lanes(east, c), 0.0)
        edge = edge + jnp.where(is_west, over_lanes(west, c), 0.0)
        bs[c * oy : (c + 1) * oy, :] = sums_ref[c * oy : (c + 1) * oy, :] + viscous * wet * edge
    flow = jnp.where(is_east, over_lanes(east, 2), 0.0) - jnp.where(is_west, over_lanes(west, 2), 0.0)
    flow = flow + jnp.where(is_top, over_rows(north, 2), 0.0) - jnp.where(is_bottom, over_rows(south, 2), 0.0)
    eta = sums_ref[2 * oy :, :] - surface_rate * 0.5 * wet * flow
    eta_out[...] = eta
    bs[2 * oy : 3 * oy, :] = eta
    bs[3 * oy :, :] = jnp.zeros((5 * oy, ox), f32)
    back = jnp.concatenate([bs[pl.ds(y, 8, stride=oy), :] for y in range(oy)], axis=1)
    pick(back, send_ref, (to_even, to_odd, own))


def k_mix(lev, part_ref, north_ref, south_ref, ends_ref, wet_ref, mix_ref, eta_ref, vel_ref, eta_out, smooth, wide):
    oy, ox = wet_ref.shape
    planes = 2 * lev
    eta_out[...] = eta_ref[...]
    wet = viscous * wet_ref[...].astype(f32)
    is_top, is_bottom, is_east, is_west = borders(oy, ox)
    east, west = ends_ref[:oy, :], ends_ref[oy:, :]
    for i in range(planes):
        edge = jnp.where(is_top, north_ref[i : i + 1, :], 0.0)
        edge = edge + jnp.where(is_bottom, south_ref[i : i + 1, :], 0.0)
        edge = edge + jnp.where(is_east, pltpu.roll(east, (ox - 1 - i) % ox, 1), 0.0)
        edge = edge + jnp.where(is_west, pltpu.roll(west, (ox - i) % ox, 1), 0.0)
        smooth[i * oy : (i + 1) * oy, :] = part_ref[i * oy : (i + 1) * oy, :] + wet * edge
    step = wide.shape[0] // 3
    blocks = [(c, y) for c in range(2) for y in range(oy)]
    for n, (c, y) in enumerate(blocks):
        column_block = smooth[pl.ds(c * lev * oy + y, lev, stride=oy), :]
        column_block = jnp.concatenate([column_block, jnp.zeros((step - lev, ox), f32)], axis=0)
        high, low = split2(column_block)
        cells = slice(n * ox, (n + 1) * ox)
        wide[:step, cells] = high
        wide[step : 2 * step, cells] = low
        wide[2 * step :, cells] = high
    high, low = split2(mix_ref[...])
    filler = jnp.zeros((lev, step - lev), f32)
    high, low = high.astype(f32), low.astype(f32)
    left = jnp.concatenate([high, filler, high, filler, low, filler], axis=1).astype(bf16)
    mixed = dot(left, wide[...])
    for n, (c, y) in enumerate(blocks):
        vel_ref[pl.ds(c * lev * oy + y, lev, stride=oy), :] = mixed[:, n * ox : (n + 1) * ox]


def pairings(n_row, n_col):
    def place(r, c):
        return r * n_col + c

    row_even = [(place(r, c), place(r ^ 1, c)) for r in range(n_row) for c in range(n_col)]
    row_odd = []
    for r in range(n_row):
        other = r + 1 if r % 2 else r - 1
        for c in range(n_col):
            if 0 <= other < n_row:
                row_odd.append((place(r, c), place(other, c)))
            else:
                row_odd.append((place(r, c), place(r, (c + n_col // 2) % n_col)))
    col_even = [(c, c ^ 1) for c in range(n_col)]
    col_odd = [(c, (c + 1 if c % 2 else c - 1) % n_col) for c in range(n_col)]
    return dict(row_even=row_even, row_odd=row_odd, col_even=col_even, col_odd=col_odd)


def shards(
    n_row,
    n_col,
    spectra,
    wind,
    wave_current,
    wave_wet,
    interaction,
    input_rate,
    eta_gain,
    stress_map,
    stokes_map,
    ocean_vel,
    ocean_eta,
    ocean_wet,
    coriolis,
    tau_profile,
    stokes_profile,
    thickness,
    mix_inverse,
    fold_index,
    wave_send,
    ocean_recv,
    ocean_send,
    wave_recv,
):
    spec, rows, lanes = spectra.shape
    cells = rows * lanes
    oy, ox = ocean_eta.shape
    lev = ocean_vel.shape[1]
    planes = 2 * lev
    nfreq = input_rate.shape[0]
    slot = wave_send.shape[-1]
    pad = -(-planes // 16) * 16
    pairs = pairings(n_row, n_col)
    both = ("row", "col")
    ocean_w = ocean_recv.reshape(3 * slot, oy * ox)
    wave_w = wave_recv.reshape(3 * slot, cells)
    wsend, osend = wave_send.reshape(3, 1, slot), ocean_send.reshape(3, 1, slot)
    fold = fold_index.reshape(1, ox)
    velocity = ocean_vel.reshape(planes * oy, ox)
    eta = ocean_eta
    whole = n_col != 4

    def trade(label, array):
        axis = both if label.startswith("row") else "col"
        return lax.ppermute(array, axis, pairs[label])

    slots_out = [((8, slot), bf16)] * 3
    soft_out = ((32, cells), f32)
    half = GROUP * (NDIR + 2)
    full = (planes * oy, ox)
    for step in range(STEPS):
        last = step + 1 == STEPS
        if step == 0:
            inputs = (
                stress_map, stokes_map, input_rate, eta_gain, wind, wave_current, wave_wet, wsend,
                spectra.reshape(spec * rows, lanes), interaction,
            )
            held = [(pltpu.SMEM if x.ndim == 1 else pltpu.VMEM)(x.shape, x.dtype) for x in inputs]
            to_even, to_odd, own, energy, soft, weights = call(
                functools.partial(k_wave_first, nfreq),
                slots_out + [((spec, cells), bf16), soft_out, ((half + 2 * GROUP, spec), bf16)],
                [HBM] * len(inputs),
                held + [pltpu.VMEM((spec * rows, lanes), f32), pltpu.SemaphoreType.DMA((len(inputs) + 2,))],
            )(*(pltpu.with_memory_space_constraint(x, pltpu.HBM) for x in inputs))
        else:
            to_even, to_odd, own, soft = call(
                functools.partial(k_wave_next, n_row), slots_out + [soft_out], [VMEM] * 8, [pltpu.VMEM((8, cells), f32)]
            )(got_even, got_odd, own, wave_w, parts, wind, wave_wet, wsend)
        got_odd, got_even = trade("row_odd", to_odd), trade("row_even", to_even)
        if step == 0:
            coef, side, lane_rows = call(
                functools.partial(k_prepare, lev),
                [((8 * 32, 128), f32), ((3, planes, 128), f32), ((8, 128), f32)],
                [VMEM] * 6,
            )(
                tau_profile.reshape(1, lev), stokes_profile, thickness.reshape(1, lev), mix_inverse,
                input_rate.reshape(1, nfreq), eta_gain.reshape(1, nfreq),
            )
        if last:
            (spectra_out,) = call(
                functools.partial(k_update_last, nfreq),
                [((spec * rows, lanes), bf16)],
                [VMEM] * 5,
                [pltpu.VMEM((spec * rows, lanes), f32)],
            )(energy, moved, soft, wave_wet, coef)
        else:
            (energy,) = call(
                functools.partial(k_update, nfreq),
                [((spec, cells), bf16)],
                [VMEM] * 5,
                [pltpu.VMEM((spec, cells), f32)],
            )(energy, interaction, soft, wave_wet, coef)
        forced, row_even, row_odd, col_even, col_odd = call(
            functools.partial(k_force, n_row, lev, pad),
            [(full, f32)] + [((planes, ox), bf16)] * 2 + [((pad + 16, ox), bf16)] * 2,
            [VMEM] * 8,
            [pltpu.VMEM((8 * oy, ox), f32)],
        )(got_even, got_odd, own, ocean_w, velocity, ocean_wet, coriolis, coef)
        got_row_odd, got_row_even = trade("row_odd", row_odd), trade("row_even", row_even)
        got_col_odd, got_col_even = trade("col_odd", col_odd), trade("col_even", col_even)
        part, sums = call(
            functools.partial(k_interior, lev), [(full, f32), ((3 * oy, ox), f32)], [VMEM] * 4
        )(forced, eta, ocean_wet, coef)
        if whole:
            top_line = lax.all_gather(col_even[:planes], "col", axis=0, tiled=True)
        else:
            top_line = fold
        eta, to_even, to_odd, own, north, south, ends = call(
            functools.partial(k_back, n_row, n_col, pad, whole),
            [((oy, ox), f32)] + slots_out + [((planes, ox), f32)] * 2 + [((2 * oy, ox), f32)],
            [VMEM] * 12,
            [pltpu.VMEM((8 * oy, ox), f32)],
        )(
            got_row_even, got_row_odd, got_col_even, got_col_odd, col_even, top_line, fold, sums, ocean_wet,
            side, lane_rows, osend,
        )
        got_odd, got_even = trade("row_odd", to_odd), trade("row_even", to_even)
        if not last:
            moved, parts = call(
                k_transfer, [((spec, cells), f32), ((half, cells), f32)], [VMEM] * 3
            )(energy, interaction, weights)
        velocity, eta = call(
            functools.partial(k_mix, lev),
            [(full, f32), ((oy, ox), f32)],
            [VMEM] * 7,
            [pltpu.VMEM(full, f32), pltpu.VMEM((96, 2 * oy * ox), bf16)],
        )(part, north, south, ends, ocean_wet, mix_inverse, eta)
    (current,) = call(
        functools.partial(k_current_out, n_row), [((3, rows, lanes), f32)], [VMEM] * 4
    )(got_even, got_odd, own, wave_w)
    return (
        spectra_out.reshape(spec, rows, lanes),
        velocity.reshape(2, lev, oy, ox),
        eta,
        current,
    )


def solution(mesh):
    n_row, n_col = mesh.shape["row"], mesh.shape["col"]
    in_specs = (
        P(None, "row", "col"),
        P(None, "row", "col"),
        P(None, "row", "col"),
        P("row", "col"),
        P(),
        P(),
        P(),
        P(),
        P(),
        P(None, None, "row", "col"),
        P("row", "col"),
        P("row", "col"),
        P("row", "col"),
        P(),
        P(),
        P(),
        P(),
        P("col"),
        P("row", "col", None, None),
        P("row", "col", None, None, None),
        P("row", "col", None, None),
        P("row", "col", None, None, None),
    )
    out_specs = (
        P(None, "row", "col"),
        P(None, None, "row", "col"),
        P("row", "col"),
        P(None, "row", "col"),
    )
    body = functools.partial(shards, n_row, n_col)
    return jax.shard_map(body, mesh=mesh, in_specs=in_specs, out_specs=out_specs, check_vma=False)
```

```python
import functools
import math

import jax
import jax.numpy as jnp
from jax import lax
from jax.experimental import pallas as pl
from jax.experimental.pallas import tpu as pltpu
from jax.sharding import PartitionSpec as P


NDIR = 24
NBAND = 3
viscous = 0.2
surface_rate = 0.5

f32, bf16 = jnp.float32, jnp.bfloat16
VMEM = pl.BlockSpec(memory_space=pltpu.VMEM)
SMEM = pl.BlockSpec(memory_space=pltpu.SMEM)
HBM = pl.BlockSpec(memory_space=pltpu.HBM)


def call(kernel, outs, specs, scratch=(), out_spec=VMEM):
    out_shape = tuple(jax.ShapeDtypeStruct(s, d) for s, d in outs)
    return pl.pallas_call(
        kernel,
        out_shape=out_shape,
        in_specs=list(specs),
        out_specs=tuple(out_spec for _ in outs),
        scratch_shapes=list(scratch),
        compiler_params=pltpu.CompilerParams(vmem_limit_bytes=12 << 20),
    )


def dot(a, b):
    return jnp.dot(a, b, preferred_element_type=f32)


def split2(w):
    high = w.astype(bf16)
    low = (w - high.astype(f32)).astype(bf16)
    return high, low


def is_even(index):
    return lax.rem(index, 2) == 0


GROUP = 8


def field_weights(smap, kmap, rate_ref, gain_ref, nfreq):
    spec = smap.shape[1]
    col = lax.broadcasted_iota(jnp.int32, (1, spec), 1)
    band = jnp.zeros((1, spec), jnp.int32)
    rate = jnp.full((1, spec), rate_ref[0], f32)
    gain = jnp.full((1, spec), gain_ref[0], f32)
    for f in range(1, nfreq):
        past = col >= NDIR * f
        band = band + jnp.where(past, 1, 0)
        rate = jnp.where(past, rate_ref[f], rate)
        gain = jnp.where(past, gain_ref[f], gain)
    keep = lax.broadcasted_iota(jnp.int32, (NDIR, spec), 0) == col - NDIR * band
    maps = [smap[i : i + 1] for i in range(2)] + [kmap[i : i + 1] for i in range(2 * NBAND)]
    rows = jnp.concatenate([jnp.where(keep, m * rate, 0.0) for m in maps], axis=0)
    return rows, jnp.concatenate([jnp.zeros((2, spec), f32), kmap], axis=0), gain


def rest_weights(stokes, gain, inter):
    high, low = split2(stokes)
    moved = dot(jnp.concatenate([high.astype(f32), low.astype(f32)], axis=0).astype(bf16), inter)
    return jnp.concatenate([stokes * gain, stokes + moved[:GROUP] + moved[GROUP:]], axis=0)


def joined(parts):
    direct = GROUP * NDIR
    rest = parts[direct : direct + 2 * GROUP] + parts[direct + 2 * GROUP :]
    return jnp.concatenate([parts[:direct], rest], axis=0)


def soft_growth(dx, dy):
    heading = lax.broadcasted_iota(jnp.int32, (NDIR, dx.shape[1]), 0).astype(f32)
    heading = (heading + 0.5) * (2.0 * math.pi / NDIR)
    relative = dx * jnp.cos(heading) + dy * jnp.sin(heading)
    return jnp.maximum(relative, 0.0) + jnp.log1p(jnp.exp(-jnp.abs(relative)))


def fields_of(soft, level, wet, parts):
    sums = [
        jnp.sum(soft * parts[i * NDIR : (i + 1) * NDIR], axis=0, keepdims=True) for i in range(GROUP)
    ]
    rest = GROUP * NDIR
    total = jnp.concatenate(sums, axis=0) + level * parts[rest : rest + GROUP] + parts[rest + GROUP :]
    row = lax.broadcasted_iota(jnp.int32, total.shape, 0)
    return jnp.where(row < 2, total, wet * total)


def flat(ref, *first):
    rows = ref.shape[-2]
    return jnp.concatenate([ref[(*first, slice(y, y + 1), slice(None))] for y in range(rows)], axis=1)


def update(old_of, moved_of, soft_ref, wet_ref, coef_ref, nfreq, store):
    rows, lanes = wet_ref.shape
    rate, gain = row_of(coef_ref, RATE), row_of(coef_ref, GAIN)
    for y in range(rows):
        cells = slice(y * lanes, (y + 1) * lanes)
        soft, level = soft_ref[:NDIR, cells], soft_ref[NDIR : NDIR + 1, cells]
        wet = wet_ref[y : y + 1, :].astype(f32)
        growth = jnp.concatenate([rate(f) * soft + gain(f) * level for f in range(nfreq)], axis=0)
        old = old_of(cells)
        store(y, cells, wet * (old + growth * old + moved_of(cells)))


def picked(fields, send):
    index = jnp.concatenate([send[j] for j in range(3)], axis=1)
    cell = lax.broadcasted_iota(jnp.int32, (fields.shape[1], index.shape[1]), 0)
    return dot(fields.astype(bf16), jnp.where(cell == index, 1.0, 0.0).astype(bf16))


def pick(fields, send, outs):
    to_even, to_odd, own = outs
    slot = send.shape[2]
    slots = picked(fields, send)
    even = is_even(lax.axis_index("row"))
    south, north = slots[:, :slot], slots[:, 2 * slot :]
    to_even[...] = jnp.where(even, north, south).astype(bf16)
    to_odd[...] = jnp.where(even, south, north).astype(bf16)
    own[...] = slots[:, slot : 2 * slot].astype(bf16)


def in_first_half(row):
    return lax.rem(row, 4) < 2


def pick_far(fields, send, outs):
    to_even, to_odd, own, far_even, far_odd = outs
    slot = send.shape[2]
    slots = picked(fields, send)
    row = lax.axis_index("row")
    even, first = is_even(row), in_first_half(row)
    south, here, north = slots[:, :slot], slots[:, slot : 2 * slot], slots[:, 2 * slot :]
    to_even[...] = jnp.concatenate([jnp.where(even, north, south), here], axis=1).astype(bf16)
    to_odd[...] = jnp.concatenate([jnp.where(even, south, north), here], axis=1).astype(bf16)
    own[...] = slots.astype(bf16)
    far_even[...] = jnp.where(first, north, south).astype(bf16)
    far_odd[...] = jnp.where(first, south, north).astype(bf16)


def gather_slots(got_even, got_odd, own, rows):
    row = lax.axis_index("row")
    even = is_even(row)
    a, b = got_even[...].astype(f32), got_odd[...].astype(f32)
    north = jnp.where(row == rows - 1, 0.0, jnp.where(even, a, b))
    south = jnp.where(row == 0, 0.0, jnp.where(even, b, a))
    return jnp.concatenate([north, own[...].astype(f32), south], axis=1).astype(bf16)


def k_wave_first(
    nfreq,
    smap_hbm, kmap_hbm, rate_hbm, gain_hbm, wind_hbm, cur_hbm, wet_hbm, send_hbm, spec_hbm, inter_hbm,
    to_even, to_odd, own, old_ref, soft_ref, weight_ref,
    smap_ref, kmap_ref, rate_ref, gain_ref, wind_ref, cur_ref, wet_ref, send_ref, spec_ref, inter_ref,
    wide, sems,
):
    rows, lanes = wet_ref.shape
    spec = inter_ref.shape[0]
    cut = spec // 32 * 16
    small = (
        (smap_hbm, smap_ref), (kmap_hbm, kmap_ref), (rate_hbm, rate_ref), (gain_hbm, gain_ref),
        (wind_hbm, wind_ref), (cur_hbm, cur_ref), (wet_hbm, wet_ref), (send_hbm, send_ref),
    )
    large = []
    for first, size in ((0, cut), (cut, spec - cut)):
        part = pl.ds(first * rows, size * rows)
        large.append((spec_hbm.at[part], spec_ref.at[part]))
    for first, size in ((0, cut), (cut, spec - cut)):
        part = pl.ds(first, size)
        large.append((inter_hbm.at[part], inter_ref.at[part]))
    copies = [pltpu.make_async_copy(a, b, sems.at[i]) for i, (a, b) in enumerate((*small, *large))]
    for copy in copies:
        copy.start()
    for copy in copies[: len(small)]:
        copy.wait()
    level = flat(cur_ref, 2)
    soft = soft_growth(flat(wind_ref, 0) - flat(cur_ref, 0), flat(wind_ref, 1) - flat(cur_ref, 1))
    soft_ref[:NDIR, :] = soft
    soft_ref[NDIR:, :] = jnp.concatenate([level] * (soft_ref.shape[0] - NDIR), axis=0)
    direct = GROUP * NDIR
    weights, stokes, gain = field_weights(smap_ref[...], kmap_ref[...], rate_ref, gain_ref, nfreq)
    weight_ref[:direct, :] = weights.astype(bf16)
    for n, (first, size) in enumerate(((0, cut), (cut, spec - cut))):
        copies[len(small) + n].wait()
        part = slice(first * rows, (first + size) * rows)
        wide[part, :] = spec_ref[part, :].astype(f32)
        for y in range(rows):
            taken = wide[pl.ds(first * rows + y, size, stride=rows), :]
            old_ref[first : first + size, y * lanes : (y + 1) * lanes] = taken.astype(bf16)
    for copy in copies[len(small) + 2 :]:
        copy.wait()
    half = direct + 2 * GROUP
    rest = rest_weights(stokes, gain, inter_ref[...])
    weight_ref[direct:half, :], weight_ref[half:, :] = split2(rest)
    parts = joined(dot(weight_ref[...], old_ref[...]))
    fields = fields_of(soft, level, flat(wet_ref).astype(f32), parts)
    pick(fields, send_ref, (to_even, to_odd, own))


def k_update(nfreq, old_ref, inter_ref, soft_ref, wet_ref, coef_ref, new_ref, moved):
    moved[...] = dot(inter_ref[...], old_ref[...])

    def store(y, cells, value):
        new_ref[:, cells] = value.astype(bf16)

    update(
        lambda cells: old_ref[:, cells].astype(f32), lambda cells: moved[:, cells],
        soft_ref, wet_ref, coef_ref, nfreq, store,
    )


def k_pack(energy_ref, weight_ref, recv_ref, wind_ref, wet_ref, send_ref, south_ref, own_ref, north_ref):
    parts = joined(dot(weight_ref[...], energy_ref[...]))
    slot = send_ref.shape[2]
    rows = parts.shape[0]
    extra = []
    for i in range(2):
        high, low = split2(flat(wind_ref, i))
        extra += [high.astype(f32), low.astype(f32)]
    extra.append(flat(wet_ref).astype(f32))
    extra.append(jnp.zeros((rows - recv_ref.shape[0] - len(extra), parts.shape[1]), f32))
    extra = jnp.concatenate(extra, axis=0).astype(bf16)
    stack = jnp.concatenate([parts.astype(bf16), recv_ref[...], extra], axis=0)
    cells = picked(stack, send_ref)
    for j, ref in enumerate((south_ref, own_ref, north_ref)):
        lanes = slice(j * slot, (j + 1) * slot)
        ref[...] = jnp.concatenate([cells[:rows, lanes], cells[rows:, lanes]], axis=1).astype(bf16)


def k_transfer(old_ref, inter_ref, moved_ref):
    moved_ref[...] = dot(inter_ref[...], old_ref[...])


def k_wave_next(
    n_row, pad,
    got_even, got_odd, far_even, far_odd, own_ref, row_even, row_odd, pack_ref,
    slots_ref, mine_ref,
):
    slot = far_even.shape[1]
    row = lax.axis_index("row")
    even, first = is_even(row), in_first_half(row)
    a, b = got_even[...].astype(f32), got_odd[...].astype(f32)
    north = jnp.where(row == n_row - 1, 0.0, jnp.where(even, a, b))
    south = jnp.where(row == 0, 0.0, jnp.where(even, b, a))
    a, b = far_even[...].astype(f32), far_odd[...].astype(f32)
    far_north = jnp.where(row >= n_row - 2, 0.0, jnp.where(first, a, b))
    far_south = jnp.where(row < 2, 0.0, jnp.where(first, b, a))
    own = own_ref[...].astype(f32)
    down, here, up = own[:, :slot], own[:, slot : 2 * slot], own[:, 2 * slot :]
    mine = jnp.concatenate([north[:, :slot], here, south[:, :slot]], axis=1).astype(bf16)
    mine_ref[...] = mine
    slots = [
        jnp.concatenate([far_north, north[:, slot:], up], axis=1).astype(bf16),
        mine,
        jnp.concatenate([down, south[:, slot:], far_south], axis=1).astype(bf16),
    ]
    a, b = row_even[pad:, :].astype(f32), row_odd[pad:, :].astype(f32)
    packs = [jnp.where(even, a, b), pack_ref[...].astype(f32), jnp.where(even, b, a)]
    recv = 3 * slot
    current = jnp.concatenate(
        [dot(x, p[:recv, slot:].astype(bf16)) for x, p in zip(slots, packs)], axis=1
    )
    extra = jnp.concatenate([p[recv : recv + 8, slot:] for p in packs], axis=1)
    parts = jnp.concatenate([p[:, :slot] for p in packs], axis=1)
    soft = soft_growth(
        extra[0:1] + extra[1:2] - current[0:1], extra[2:3] + extra[3:4] - current[1:2]
    )
    fields = fields_of(soft, current[2:3], extra[4:5], parts)
    lane = lax.broadcasted_iota(jnp.int32, fields.shape, 1)
    fields = jnp.where((row == n_row - 1) & (lane < slot), 0.0, fields)
    fields = jnp.where((row == 0) & (lane >= 2 * slot), 0.0, fields)
    slots_ref[...] = fields.astype(bf16)


def k_update_last(
    nfreq, old_ref, moved_ref, mine_ref, recv_ref, wind_ref, wet_ref, coef_ref, out_ref, cur, soft_ref, wide
):
    rows, spec = wet_ref.shape[0], old_ref.shape[0]
    cur[...] = dot(mine_ref[...], recv_ref[...])
    soft_ref[:NDIR, :] = soft_growth(
        flat(wind_ref, 0) - cur[0:1, :], flat(wind_ref, 1) - cur[1:2, :]
    )
    soft_ref[NDIR:, :] = jnp.concatenate([cur[2:3, :]] * (soft_ref.shape[0] - NDIR), axis=0)

    def store(y, cells, value):
        wide[pl.ds(y, spec, stride=rows), :] = value

    update(
        lambda cells: old_ref[:, cells].astype(f32), lambda cells: moved_ref[:, cells],
        soft_ref, wet_ref, coef_ref, nfreq, store,
    )
    out_ref[...] = wide[...].astype(bf16)


def k_last(
    lev,
    spectra_ref, eta_ref, part_ref, north_ref, south_ref, ends_ref, sea_ref, mix_ref,
    spectra_out, eta_out, vel_out,
    vel_ref, smooth, pieces, sems,
):
    copies = [
        pltpu.make_async_copy(spectra_ref, spectra_out, sems.at[0]),
        pltpu.make_async_copy(eta_ref, eta_out, sems.at[1]),
        pltpu.make_async_copy(vel_ref, vel_out, sems.at[2]),
    ]
    copies[0].start()
    copies[1].start()
    k_mix(lev, part_ref, north_ref, south_ref, ends_ref, sea_ref, mix_ref, vel_ref, smooth, pieces)
    copies[2].start()
    for copy in copies:
        copy.wait()


def k_current_out(n_row, got_even, got_odd, own, recv_ref, out_ref):
    rows, lanes = out_ref.shape[1:]
    cur = dot(gather_slots(got_even, got_odd, own, n_row), recv_ref[...])
    for i in range(3):
        for y in range(rows):
            out_ref[i, y : y + 1, :] = cur[i : i + 1, y * lanes : (y + 1) * lanes]


TAU, PROF, THICK, SURF, RATE, GAIN = 0, 1, 1 + NBAND, 2 + NBAND, 3 + NBAND, 4 + NBAND


def row_of(coef_ref, which):
    return lambda l: coef_ref[which * 32 + l : which * 32 + l + 1, :]


def column(vector, first, count):
    row = lax.broadcasted_iota(jnp.int32, (count, vector.shape[1]), 0)
    lane = lax.broadcasted_iota(jnp.int32, (count, vector.shape[1]), 1)
    picked = jnp.sum(jnp.where(row - first == lane, vector, 0.0), axis=1, keepdims=True)
    return jnp.broadcast_to(picked, (count, 128))


def spread(vector, first):
    lev = vector.shape[1]
    parts = [vector, jnp.zeros((1, 128 - lev - first), f32)]
    if first:
        parts = [jnp.zeros((1, first), f32)] + parts
    return jnp.concatenate(parts, axis=1)


def k_prepare(lev, tau_ref, prof_ref, thick_ref, mix_ref, rate_ref, gain_ref, coef_ref, side_ref, lane_ref):
    surf = mix_ref[0:1, :]
    vectors = [tau_ref[...]] + [prof_ref[b : b + 1, :] for b in range(NBAND)]
    vectors += [thick_ref[...], surf, rate_ref[...], gain_ref[...]]
    for i, vector in enumerate(vectors):
        coef_ref[i * 32 : (i + 1) * 32, :] = column(vector, 0, 32)
    side_ref[0] = column(surf, 0, 2 * lev)
    side_ref[1] = column(surf, lev, 2 * lev)
    side_ref[2] = column(thick_ref[...], lev, 2 * lev)
    lane_ref[0:1, :] = spread(surf, 0)
    lane_ref[1:2, :] = spread(surf, lev)
    lane_ref[2:3, :] = spread(thick_ref[...], 0)


def k_force(
    n_row, lev, pad, first,
    *refs,
):
    if first:
        got_even, got_odd, own, pack_south, pack_north, *refs = refs
        slots = gather_slots(got_even, got_odd, own, n_row)
    else:
        slot_ref, *refs = refs
        slots = slot_ref[...]
    recv_ref, vel_ref, wet_ref, cor_ref, coef_ref, forced_ref, row_even, row_odd, col_even, col_odd, fs = refs
    oy, ox = wet_ref.shape
    planes = 2 * lev
    forcing = dot(slots, recv_ref[...])
    nf = forcing.shape[0]
    for y in range(oy):
        fs[y * nf : (y + 1) * nf, :] = forcing[:, y * ox : (y + 1) * ox]
    field = [fs[pl.ds(i, oy, stride=nf), :] for i in range(nf)]
    wet = wet_ref[...].astype(f32)
    cor = cor_ref[...]
    along = [cor * field[i] for i in range(2, nf)]
    tau = row_of(coef_ref, TAU)
    prof = [row_of(coef_ref, PROF + b) for b in range(NBAND)]
    lane = lax.broadcasted_iota(jnp.int32, (oy, ox), 1)
    east = jnp.zeros((oy, ox), f32)
    west = jnp.zeros((oy, ox), f32)
    for i in range(planes):
        c, l = divmod(i, lev)
        accel = tau(l) * field[c]
        for b in range(NBAND):
            term = prof[b](l) * along[2 * b + 1 - c]
            accel = accel + term if c == 0 else accel - term
        value = wet * (vel_ref[i * oy : (i + 1) * oy, :] + accel)
        forced_ref[i * oy : (i + 1) * oy, :] = value
        here = lane == i
        west = jnp.where(here, pltpu.roll(value, i, 1) if i else value, west)
        east = jnp.where(here, pltpu.roll(value, (i + 1) % ox, 1), east)
    bottom = forced_ref[pl.ds(0, planes, stride=oy), :]
    top = forced_ref[pl.ds(oy - 1, planes, stride=oy), :]
    even = is_even(lax.axis_index("row"))
    row_even[:planes, :] = jnp.where(even, top, bottom).astype(bf16)
    row_odd[:planes, :] = jnp.where(even, bottom, top).astype(bf16)
    if first:
        a, b = pack_south[...].astype(f32), pack_north[...].astype(f32)
        row_even[pad:, :] = jnp.where(even, b, a).astype(bf16)
        row_odd[pad:, :] = jnp.where(even, a, b).astype(bf16)
    even = is_even(lax.axis_index("col"))
    col_even[:planes, :] = top.astype(bf16)
    col_odd[:planes, :] = top.astype(bf16)
    filler = jnp.zeros((16 - oy, ox), f32)
    col_even[pad:, :] = jnp.concatenate([jnp.where(even, east, west), filler], 0).astype(bf16)
    col_odd[pad:, :] = jnp.concatenate([jnp.where(even, west, east), filler], 0).astype(bf16)


def borders(oy, ox):
    lane = lax.broadcasted_iota(jnp.int32, (oy, ox), 1)
    line = lax.broadcasted_iota(jnp.int32, (oy, ox), 0)
    return line == oy - 1, line == 0, lane == ox - 1, lane == 0


def k_interior(lev, forced_ref, eta_ref, wet_ref, coef_ref, part_ref, sums_ref):
    oy, ox = wet_ref.shape
    wet = wet_ref[...].astype(f32)
    is_top, is_bottom, is_east, is_west = borders(oy, ox)
    thick, surf = row_of(coef_ref, THICK), row_of(coef_ref, SURF)
    across = jnp.zeros((oy, ox), f32)
    surface = [jnp.zeros((oy, ox), f32), jnp.zeros((oy, ox), f32)]
    for i in range(2 * lev):
        c, l = divmod(i, lev)
        here = forced_ref[i * oy : (i + 1) * oy, :]
        up = jnp.where(is_top, 0.0, pltpu.roll(here, oy - 1, 0))
        down = jnp.where(is_bottom, 0.0, pltpu.roll(here, 1, 0))
        right = jnp.where(is_east, 0.0, pltpu.roll(here, ox - 1, 1))
        left = jnp.where(is_west, 0.0, pltpu.roll(here, 1, 1))
        part = wet * (here + viscous * (up + down + right + left - 4.0 * here))
        part_ref[i * oy : (i + 1) * oy, :] = part
        surface[c] = surface[c] + surf(l) * part
        across = across + thick(l) * (right - left if c == 0 else up - down)
    sums_ref[:oy, :] = surface[0]
    sums_ref[oy : 2 * oy, :] = surface[1]
    sums_ref[2 * oy :, :] = wet * (eta_ref[...] - surface_rate * 0.5 * across)


def k_back(
    n_row, n_col, pad, whole, choose,
    got_row_even, got_row_odd, got_col_even, got_col_odd, sent_col, line_ref, fold_ref, sums_ref, wet_ref, side_ref, lane_ref, send_ref,
    eta_out, north_ref, south_ref, ends_ref, *outs,
):
    *outs, bs = outs
    oy, ox = wet_ref.shape
    planes = north_ref.shape[0]
    row, col = lax.axis_index("row"), lax.axis_index("col")
    even = is_even(row)
    a, b = got_row_even[:planes, :].astype(f32), got_row_odd[:planes, :].astype(f32)
    north_ref[...] = jnp.where(even, a, b)

    @pl.when(row == n_row - 1)
    def _():
        if whole:
            pieces = [(line_ref[t * planes : (t + 1) * planes, :], t) for t in range(n_col)]
        else:
            pair_even = jnp.where(is_even(col), col + 1, col - 1)
            pair_odd = lax.rem(jnp.where(is_even(col), col - 1, col + 1) + n_col, n_col)
            pieces = [
                (sent_col[:planes, :], col),
                (got_col_even[:planes, :], pair_even),
                (got_col_odd[:planes, :], pair_odd),
                (got_row_odd[:planes, :], lax.rem(col + n_col // 2, n_col)),
            ]
        cell = lax.broadcasted_iota(jnp.int32, (ox, ox), 0)
        across = None
        for piece, tile in pieces:
            hot = jnp.where(cell == fold_ref[...] - tile * ox, 1.0, 0.0).astype(bf16)
            part = dot(piece, hot)
            across = part if across is None else across + part
        north_ref[...] = -across

    north = north_ref[...]
    south = jnp.where(row == 0, 0.0, jnp.where(even, b, a))
    even = is_even(col)
    a = got_col_even[pad:, :].astype(f32)[:oy]
    b = got_col_odd[pad:, :].astype(f32)[:oy]
    east, west = jnp.where(even, a, b), jnp.where(even, b, a)
    south_ref[...] = south
    ends_ref[:oy, :] = east
    ends_ref[oy:, :] = west
    wet = wet_ref[...].astype(f32)
    is_top, is_bottom, is_east, is_west = borders(oy, ox)

    def over_rows(x, i):
        return jnp.sum(x * side_ref[i], axis=0, keepdims=True)

    def over_lanes(x, i):
        return jnp.sum(x * lane_ref[i : i + 1, :], axis=1, keepdims=True)

    for c in range(2):
        edge = jnp.where(is_top, over_rows(north, c), 0.0) + jnp.where(is_bottom, over_rows(south, c), 0.0)
        edge = edge + jnp.where(is_east, over_lanes(east, c), 0.0)
        edge = edge + jnp.where(is_west, over_lanes(west, c), 0.0)
        bs[c * oy : (c + 1) * oy, :] = sums_ref[c * oy : (c + 1) * oy, :] + viscous * wet * edge
    flow = jnp.where(is_east, over_lanes(east, 2), 0.0) - jnp.where(is_west, over_lanes(west, 2), 0.0)
    flow = flow + jnp.where(is_top, over_rows(north, 2), 0.0) - jnp.where(is_bottom, over_rows(south, 2), 0.0)
    eta = sums_ref[2 * oy :, :] - surface_rate * 0.5 * wet * flow
    eta_out[...] = eta
    bs[2 * oy : 3 * oy, :] = eta
    bs[3 * oy :, :] = jnp.zeros((5 * oy, ox), f32)
    back = jnp.concatenate([bs[pl.ds(y, 8, stride=oy), :] for y in range(oy)], axis=1)
    choose(back, send_ref, outs)


def k_mix(lev, part_ref, north_ref, south_ref, ends_ref, wet_ref, mix_ref, vel_ref, smooth, wide):
    oy, ox = wet_ref.shape
    planes = 2 * lev
    wet = viscous * wet_ref[...].astype(f32)
    is_top, is_bottom, is_east, is_west = borders(oy, ox)
    east, west = ends_ref[:oy, :], ends_ref[oy:, :]
    for i in range(planes):
        edge = jnp.where(is_top, north_ref[i : i + 1, :], 0.0)
        edge = edge + jnp.where(is_bottom, south_ref[i : i + 1, :], 0.0)
        edge = edge + jnp.where(is_east, pltpu.roll(east, (ox - 1 - i) % ox, 1), 0.0)
        edge = edge + jnp.where(is_west, pltpu.roll(west, (ox - i) % ox, 1), 0.0)
        smooth[i * oy : (i + 1) * oy, :] = part_ref[i * oy : (i + 1) * oy, :] + wet * edge
    step = wide.shape[0] // 3
    blocks = [(c, y) for c in range(2) for y in range(oy)]
    for n, (c, y) in enumerate(blocks):
        column_block = smooth[pl.ds(c * lev * oy + y, lev, stride=oy), :]
        column_block = jnp.concatenate([column_block, jnp.zeros((step - lev, ox), f32)], axis=0)
        high, low = split2(column_block)
        cells = slice(n * ox, (n + 1) * ox)
        wide[:step, cells] = high
        wide[step : 2 * step, cells] = low
        wide[2 * step :, cells] = high
    high, low = split2(mix_ref[...])
    filler = jnp.zeros((lev, step - lev), f32)
    high, low = high.astype(f32), low.astype(f32)
    left = jnp.concatenate([high, filler, high, filler, low, filler], axis=1).astype(bf16)
    mixed = dot(left, wide[...])
    for n, (c, y) in enumerate(blocks):
        vel_ref[pl.ds(c * lev * oy + y, lev, stride=oy), :] = mixed[:, n * ox : (n + 1) * ox]


def pairings(n_row, n_col):
    def place(r, c):
        return r * n_col + c

    row_even = [(place(r, c), place(r ^ 1, c)) for r in range(n_row) for c in range(n_col)]
    row_odd = []
    for r in range(n_row):
        other = r + 1 if r % 2 else r - 1
        for c in range(n_col):
            if 0 <= other < n_row:
                row_odd.append((place(r, c), place(other, c)))
            else:
                row_odd.append((place(r, c), place(r, (c + n_col // 2) % n_col)))
    far_even = [(place(r, c), place(r ^ 2, c)) for r in range(n_row) for c in range(n_col)]
    far_odd = []
    for r in range(n_row):
        other = r - 2 if r % 4 < 2 else r + 2
        for c in range(n_col):
            if 0 <= other < n_row:
                far_odd.append((place(r, c), place(other, c)))
            else:
                far_odd.append((place(r, c), place(r, (c + n_col // 2) % n_col)))
    col_even = [(c, c ^ 1) for c in range(n_col)]
    col_odd = [(c, (c + 1 if c % 2 else c - 1) % n_col) for c in range(n_col)]
    return dict(
        row_even=row_even, row_odd=row_odd, col_even=col_even, col_odd=col_odd, far_even=far_even, far_odd=far_odd
    )


def shards(
    n_row,
    n_col,
    spectra,
    wind,
    wave_current,
    wave_wet,
    interaction,
    input_rate,
    eta_gain,
    stress_map,
    stokes_map,
    ocean_vel,
    ocean_eta,
    ocean_wet,
    coriolis,
    tau_profile,
    stokes_profile,
    thickness,
    mix_inverse,
    fold_index,
    wave_send,
    ocean_recv,
    ocean_send,
    wave_recv,
):
    spec, rows, lanes = spectra.shape
    cells = rows * lanes
    oy, ox = ocean_eta.shape
    lev = ocean_vel.shape[1]
    planes = 2 * lev
    nfreq = input_rate.shape[0]
    slot = wave_send.shape[-1]
    pad = -(-planes // 16) * 16
    pairs = pairings(n_row, n_col)
    both = ("row", "col")
    ocean_w = ocean_recv.reshape(3 * slot, oy * ox)
    wave_w = wave_recv.reshape(3 * slot, cells)
    wsend, osend = wave_send.reshape(3, 1, slot), ocean_send.reshape(3, 1, slot)
    fold = fold_index.reshape(1, ox)
    velocity = ocean_vel.reshape(planes * oy, ox)
    eta = ocean_eta
    whole = n_col != 4

    def trade(label, array):
        axis = "col" if label.startswith("col") else both
        return lax.ppermute(array, axis, pairs[label])

    slots_out = [((8, slot), bf16)] * 3
    soft_out = ((32, cells), f32)
    half = GROUP * (NDIR + 2)
    full = (planes * oy, ox)
    mixer = [pltpu.VMEM(full, f32), pltpu.VMEM((96, 2 * oy * ox), bf16)]

    def edges(step, lists, send_of):
        first = step == 0
        tall = pad + half if first else planes
        forced, row_even, row_odd, col_even, col_odd = call(
            functools.partial(k_force, n_row, lev, pad, first),
            [(full, f32)] + [((tall, ox), bf16)] * 2 + [((pad + 16, ox), bf16)] * 2,
            [VMEM] * (len(lists) + 5),
            [pltpu.VMEM((8 * oy, ox), f32)],
        )(*lists, ocean_w, velocity, ocean_wet, coriolis, coef)
        got_row_odd, got_row_even = trade("row_odd", row_odd), trade("row_even", row_even)
        got_col_odd, got_col_even = trade("col_odd", col_odd), trade("col_even", col_even)
        part, sums = call(
            functools.partial(k_interior, lev), [(full, f32), ((3 * oy, ox), f32)], [VMEM] * 4
        )(forced, eta, ocean_wet, coef)
        if whole:
            top_line = lax.all_gather(col_even[:planes], "col", axis=0, tiled=True)
        else:
            top_line = fold
        choose, slots = send_of
        eta_next, north, south, ends, *sent = call(
            functools.partial(k_back, n_row, n_col, pad, whole, choose),
            [((oy, ox), f32)] + [((planes, ox), f32)] * 2 + [((2 * oy, ox), f32)] + slots,
            [VMEM] * 12,
            [pltpu.VMEM((8 * oy, ox), f32)],
        )(
            got_row_even, got_row_odd, got_col_even, got_col_odd, col_even, top_line, fold, sums, ocean_wet,
            side, lane_rows, osend,
        )
        return (part, north, south, ends), eta_next, sent, (got_row_even, got_row_odd)

    inputs = (
        stress_map, stokes_map, input_rate, eta_gain, wind, wave_current, wave_wet, wsend,
        spectra.reshape(spec * rows, lanes), interaction,
    )
    held = [(pltpu.SMEM if x.ndim == 1 else pltpu.VMEM)(x.shape, x.dtype) for x in inputs]
    to_even, to_odd, own, energy, soft, weights = call(
        functools.partial(k_wave_first, nfreq),
        slots_out + [((spec, cells), bf16), soft_out, ((half + 2 * GROUP, spec), bf16)],
        [HBM] * len(inputs),
        held + [pltpu.VMEM((spec * rows, lanes), f32), pltpu.SemaphoreType.DMA((len(inputs) + 2,))],
    )(*(pltpu.with_memory_space_constraint(x, pltpu.HBM) for x in inputs))
    got_odd, got_even = trade("row_odd", to_odd), trade("row_even", to_even)
    coef, side, lane_rows = call(
        functools.partial(k_prepare, lev), [((8 * 32, 128), f32), ((3, planes, 128), f32), ((8, 128), f32)], [VMEM] * 6
    )(
        tau_profile.reshape(1, lev), stokes_profile, thickness.reshape(1, lev), mix_inverse,
        input_rate.reshape(1, nfreq), eta_gain.reshape(1, nfreq),
    )
    (energy,) = call(
        functools.partial(k_update, nfreq), [((spec, cells), bf16)], [VMEM] * 5, [pltpu.VMEM((spec, cells), f32)]
    )(energy, interaction, soft, wave_wet, coef)
    pack_south, pack_own, pack_north = call(
        k_pack, [((half, 2 * slot), bf16)] * 3, [VMEM] * 6
    )(energy, weights, wave_w, wind, wave_wet, wsend)
    far_slots = [((8, 2 * slot), bf16)] * 2 + [((8, 3 * slot), bf16)] + [((8, slot), bf16)] * 2
    smooth, eta, sent, got_rows = edges(
        0, (got_even, got_odd, own, pack_south, pack_north), (pick_far, far_slots)
    )
    to_even, to_odd, own, far_even, far_odd = sent
    got_odd, got_even = trade("row_odd", to_odd), trade("row_even", to_even)
    got_far_odd, got_far_even = trade("far_odd", far_odd), trade("far_even", far_even)
    (moved,) = call(k_transfer, [((spec, cells), f32)], [VMEM] * 2)(
        energy, interaction
    )
    (velocity,) = call(functools.partial(k_mix, lev), [(full, f32)], [VMEM] * 6, mixer)(*smooth, ocean_wet, mix_inverse)
    fields, mine = call(
        functools.partial(k_wave_next, n_row, pad), [((8, 3 * slot), bf16)] * 2, [VMEM] * 8
    )(got_even, got_odd, got_far_even, got_far_odd, own, *got_rows, pack_own)
    (spectra_new,) = call(
        functools.partial(k_update_last, nfreq),
        [((spec * rows, lanes), bf16)],
        [VMEM] * 7,
        [
            pltpu.VMEM((8, cells), f32),
            pltpu.VMEM(soft_out[0], f32),
            pltpu.VMEM((spec * rows, lanes), f32),
        ],
    )(energy, moved, mine, wave_w, wind, wave_wet, coef)
    smooth, eta, sent, _ = edges(1, (fields,), (pick, slots_out))
    to_even, to_odd, own = sent
    got_odd, got_even = trade("row_odd", to_odd), trade("row_even", to_even)
    spectra_out, eta, velocity = call(
        functools.partial(k_last, lev),
        [((spec * rows, lanes), bf16), ((oy, ox), f32), (full, f32)],
        [VMEM] * 8,
        [pltpu.VMEM(full, f32), *mixer, pltpu.SemaphoreType.DMA((3,))],
        HBM,
    )(spectra_new, eta, *smooth, ocean_wet, mix_inverse)
    (current,) = call(
        functools.partial(k_current_out, n_row), [((3, rows, lanes), f32)], [VMEM] * 4
    )(got_even, got_odd, own, wave_w)
    return (
        spectra_out.reshape(spec, rows, lanes),
        velocity.reshape(2, lev, oy, ox),
        eta,
        current,
    )


def solution(mesh):
    n_row, n_col = mesh.shape["row"], mesh.shape["col"]
    in_specs = (
        P(None, "row", "col"),
        P(None, "row", "col"),
        P(None, "row", "col"),
        P("row", "col"),
        P(),
        P(),
        P(),
        P(),
        P(),
        P(None, None, "row", "col"),
        P("row", "col"),
        P("row", "col"),
        P("row", "col"),
        P(),
        P(),
        P(),
        P(),
        P("col"),
        P("row", "col", None, None),
        P("row", "col", None, None, None),
        P("row", "col", None, None),
        P("row", "col", None, None, None),
    )
    out_specs = (
        P(None, "row", "col"),
        P(None, None, "row", "col"),
        P("row", "col"),
        P(None, "row", "col"),
    )
    body = functools.partial(shards, n_row, n_col)
    return jax.shard_map(body, mesh=mesh, in_specs=in_specs, out_specs=out_specs, check_vma=False)
```

```python
import functools
import math

import jax
import jax.numpy as jnp
from jax import lax
from jax.experimental import pallas as pl
from jax.experimental.pallas import tpu as pltpu
from jax.sharding import PartitionSpec as P


NDIR = 24
NBAND = 3
viscous = 0.2
surface_rate = 0.5

f32, bf16 = jnp.float32, jnp.bfloat16
VMEM = pl.BlockSpec(memory_space=pltpu.VMEM)
SMEM = pl.BlockSpec(memory_space=pltpu.SMEM)
HBM = pl.BlockSpec(memory_space=pltpu.HBM)


def call(kernel, outs, specs, scratch=(), out_spec=VMEM):
    out_shape = tuple(jax.ShapeDtypeStruct(s, d) for s, d in outs)
    return pl.pallas_call(
        kernel,
        out_shape=out_shape,
        in_specs=list(specs),
        out_specs=tuple(out_spec for _ in outs),
        scratch_shapes=list(scratch),
        compiler_params=pltpu.CompilerParams(vmem_limit_bytes=12 << 20),
    )


def dot(a, b):
    return jnp.dot(a, b, preferred_element_type=f32)


def split2(w):
    high = w.astype(bf16)
    low = (w - high.astype(f32)).astype(bf16)
    return high, low


def is_even(index):
    return lax.rem(index, 2) == 0


PACK = 16
GROUP = 8


def field_weights(smap, kmap, rate_ref, gain_ref, nfreq):
    spec = smap.shape[1]
    col = lax.broadcasted_iota(jnp.int32, (1, spec), 1)
    band = jnp.zeros((1, spec), jnp.int32)
    rate = jnp.full((1, spec), rate_ref[0], f32)
    gain = jnp.full((1, spec), gain_ref[0], f32)
    for f in range(1, nfreq):
        past = col >= NDIR * f
        band = band + jnp.where(past, 1, 0)
        rate = jnp.where(past, rate_ref[f], rate)
        gain = jnp.where(past, gain_ref[f], gain)
    keep = lax.broadcasted_iota(jnp.int32, (NDIR, spec), 0) == col - NDIR * band
    maps = [smap[i : i + 1] for i in range(2)] + [kmap[i : i + 1] for i in range(2 * NBAND)]
    rows = jnp.concatenate([jnp.where(keep, m * rate, 0.0) for m in maps], axis=0)
    return rows, jnp.concatenate([jnp.zeros((2, spec), f32), kmap], axis=0), gain


def rest_weights(stokes, gain, inter):
    high, low = split2(stokes)
    moved = dot(jnp.concatenate([high.astype(f32), low.astype(f32)], axis=0).astype(bf16), inter)
    return jnp.concatenate([stokes * gain, stokes + moved[:GROUP] + moved[GROUP:]], axis=0)


def joined(parts):
    direct = GROUP * NDIR
    rest = parts[direct : direct + 2 * GROUP] + parts[direct + 2 * GROUP :]
    return jnp.concatenate([parts[:direct], rest], axis=0)


def soft_growth(dx, dy):
    heading = lax.broadcasted_iota(jnp.int32, (NDIR, dx.shape[1]), 0).astype(f32)
    heading = (heading + 0.5) * (2.0 * math.pi / NDIR)
    relative = dx * jnp.cos(heading) + dy * jnp.sin(heading)
    return jnp.maximum(relative, 0.0) + jnp.log1p(jnp.exp(-jnp.abs(relative)))


def fields_of(soft, level, wet, parts):
    sums = [
        jnp.sum(soft * parts[i * NDIR : (i + 1) * NDIR], axis=0, keepdims=True) for i in range(GROUP)
    ]
    rest = GROUP * NDIR
    total = jnp.concatenate(sums, axis=0) + level * parts[rest : rest + GROUP] + parts[rest + GROUP :]
    row = lax.broadcasted_iota(jnp.int32, total.shape, 0)
    return jnp.where(row < 2, total, wet * total)


def flat(ref, *first):
    rows = ref.shape[-2]
    return jnp.concatenate([ref[(*first, slice(y, y + 1), slice(None))] for y in range(rows)], axis=1)


def update(old_of, moved_of, soft_ref, wet_ref, coef_ref, nfreq, store):
    rows, lanes = wet_ref.shape
    rate, gain = row_of(coef_ref, RATE), row_of(coef_ref, GAIN)
    for y in range(rows):
        cells = slice(y * lanes, (y + 1) * lanes)
        soft, level = soft_ref[:NDIR, cells], soft_ref[NDIR : NDIR + 1, cells]
        wet = wet_ref[y : y + 1, :].astype(f32)
        growth = jnp.concatenate([rate(f) * soft + gain(f) * level for f in range(nfreq)], axis=0)
        old = old_of(cells)
        store(y, cells, wet * (old + growth * old + moved_of(cells)))


def picked(fields, send):
    index = jnp.concatenate([send[j] for j in range(3)], axis=1)
    cell = lax.broadcasted_iota(jnp.int32, (fields.shape[1], index.shape[1]), 0)
    return dot(fields.astype(bf16), jnp.where(cell == index, 1.0, 0.0).astype(bf16))


def pick(fields, send, outs):
    to_even, to_odd, own = outs
    slot = send.shape[2]
    slots = picked(fields, send)
    even = is_even(lax.axis_index("row"))
    south, north = slots[:, :slot], slots[:, 2 * slot :]
    to_even[...] = jnp.where(even, north, south).astype(bf16)
    to_odd[...] = jnp.where(even, south, north).astype(bf16)
    own[...] = slots[:, slot : 2 * slot].astype(bf16)


def in_first_half(row):
    return lax.rem(row, 4) < 2


def pick_far(fields, send, outs):
    to_even, to_odd, own, far_even, far_odd, pack_south, pack_north = outs
    slot = send.shape[2]
    slots = picked(fields, send)
    row = lax.axis_index("row")
    even, first = is_even(row), in_first_half(row)
    south, here, north = slots[:, :slot], slots[:, slot : 2 * slot], slots[:, 2 * slot :]
    rows = slots.shape[0]
    to_even[:rows, :] = jnp.concatenate([jnp.where(even, north, south), here], axis=1).astype(bf16)
    to_odd[:rows, :] = jnp.concatenate([jnp.where(even, south, north), here], axis=1).astype(bf16)
    a, b = pack_south[...].astype(f32), pack_north[...].astype(f32)
    to_even[PACK:, :] = jnp.where(even, b, a).astype(bf16)
    to_odd[PACK:, :] = jnp.where(even, a, b).astype(bf16)
    own[...] = slots.astype(bf16)
    far_even[...] = jnp.where(first, north, south).astype(bf16)
    far_odd[...] = jnp.where(first, south, north).astype(bf16)


def gather_slots(got_even, got_odd, own, rows):
    row = lax.axis_index("row")
    even = is_even(row)
    a, b = got_even[...].astype(f32), got_odd[...].astype(f32)
    north = jnp.where(row == rows - 1, 0.0, jnp.where(even, a, b))
    south = jnp.where(row == 0, 0.0, jnp.where(even, b, a))
    return jnp.concatenate([north, own[...].astype(f32), south], axis=1).astype(bf16)


def k_wave_first(
    nfreq,
    smap_hbm, kmap_hbm, rate_hbm, gain_hbm, wind_hbm, cur_hbm, wet_hbm, send_hbm, spec_hbm, inter_hbm,
    to_even, to_odd, own, old_ref, soft_ref, weight_ref,
    smap_ref, kmap_ref, rate_ref, gain_ref, wind_ref, cur_ref, wet_ref, send_ref, spec_ref, inter_ref,
    wide, sems,
):
    rows, lanes = wet_ref.shape
    spec = inter_ref.shape[0]
    cut = spec // 32 * 16
    small = (
        (smap_hbm, smap_ref), (kmap_hbm, kmap_ref), (rate_hbm, rate_ref), (gain_hbm, gain_ref),
        (wind_hbm, wind_ref), (cur_hbm, cur_ref), (wet_hbm, wet_ref), (send_hbm, send_ref),
    )
    large = []
    for first, size in ((0, cut), (cut, spec - cut)):
        part = pl.ds(first * rows, size * rows)
        large.append((spec_hbm.at[part], spec_ref.at[part]))
    for first, size in ((0, cut), (cut, spec - cut)):
        part = pl.ds(first, size)
        large.append((inter_hbm.at[part], inter_ref.at[part]))
    copies = [pltpu.make_async_copy(a, b, sems.at[i]) for i, (a, b) in enumerate((*small, *large))]
    for copy in copies:
        copy.start()
    for copy in copies[: len(small)]:
        copy.wait()
    level = flat(cur_ref, 2)
    soft = soft_growth(flat(wind_ref, 0) - flat(cur_ref, 0), flat(wind_ref, 1) - flat(cur_ref, 1))
    soft_ref[:NDIR, :] = soft
    soft_ref[NDIR:, :] = jnp.concatenate([level] * (soft_ref.shape[0] - NDIR), axis=0)
    direct = GROUP * NDIR
    weights, stokes, gain = field_weights(smap_ref[...], kmap_ref[...], rate_ref, gain_ref, nfreq)
    weight_ref[:direct, :] = weights.astype(bf16)
    for n, (first, size) in enumerate(((0, cut), (cut, spec - cut))):
        copies[len(small) + n].wait()
        part = slice(first * rows, (first + size) * rows)
        wide[part, :] = spec_ref[part, :].astype(f32)
        for y in range(rows):
            taken = wide[pl.ds(first * rows + y, size, stride=rows), :]
            old_ref[first : first + size, y * lanes : (y + 1) * lanes] = taken.astype(bf16)
    for copy in copies[len(small) + 2 :]:
        copy.wait()
    half = direct + 2 * GROUP
    rest = rest_weights(stokes, gain, inter_ref[...])
    weight_ref[direct:half, :], weight_ref[half:, :] = split2(rest)
    parts = joined(dot(weight_ref[...], old_ref[...]))
    fields = fields_of(soft, level, flat(wet_ref).astype(f32), parts)
    pick(fields, send_ref, (to_even, to_odd, own))


def k_update(nfreq, old_ref, inter_ref, soft_ref, wet_ref, coef_ref, new_ref, moved):
    moved[...] = dot(inter_ref[...], old_ref[...])

    def store(y, cells, value):
        new_ref[:, cells] = value.astype(bf16)

    update(
        lambda cells: old_ref[:, cells].astype(f32), lambda cells: moved[:, cells],
        soft_ref, wet_ref, coef_ref, nfreq, store,
    )


def k_pack(energy_ref, weight_ref, recv_ref, wind_ref, wet_ref, send_ref, south_ref, own_ref, north_ref):
    parts = joined(dot(weight_ref[...], energy_ref[...]))
    slot = send_ref.shape[2]
    rows = parts.shape[0]
    extra = []
    for i in range(2):
        high, low = split2(flat(wind_ref, i))
        extra += [high.astype(f32), low.astype(f32)]
    extra.append(flat(wet_ref).astype(f32))
    extra.append(jnp.zeros((rows - recv_ref.shape[0] - len(extra), parts.shape[1]), f32))
    extra = jnp.concatenate(extra, axis=0).astype(bf16)
    stack = jnp.concatenate([parts.astype(bf16), recv_ref[...], extra], axis=0)
    cells = picked(stack, send_ref)
    for j, ref in enumerate((south_ref, own_ref, north_ref)):
        lanes = slice(j * slot, (j + 1) * slot)
        ref[...] = jnp.concatenate([cells[:rows, lanes], cells[rows:, lanes]], axis=1).astype(bf16)


def k_transfer(old_ref, inter_ref, moved_ref):
    moved_ref[...] = dot(inter_ref[...], old_ref[...])


def k_wave_next(
    n_row,
    got_even, got_odd, far_even, far_odd, own_ref, pack_ref,
    slots_ref, mine_ref,
):
    slot = far_even.shape[1]
    row = lax.axis_index("row")
    even, first = is_even(row), in_first_half(row)
    rows = own_ref.shape[0]
    a, b = got_even[:rows, :].astype(f32), got_odd[:rows, :].astype(f32)
    north = jnp.where(row == n_row - 1, 0.0, jnp.where(even, a, b))
    south = jnp.where(row == 0, 0.0, jnp.where(even, b, a))
    a, b = far_even[...].astype(f32), far_odd[...].astype(f32)
    far_north = jnp.where(row >= n_row - 2, 0.0, jnp.where(first, a, b))
    far_south = jnp.where(row < 2, 0.0, jnp.where(first, b, a))
    own = own_ref[...].astype(f32)
    down, here, up = own[:, :slot], own[:, slot : 2 * slot], own[:, 2 * slot :]
    mine = jnp.concatenate([north[:, :slot], here, south[:, :slot]], axis=1).astype(bf16)
    mine_ref[...] = mine
    slots = [
        jnp.concatenate([far_north, north[:, slot:], up], axis=1).astype(bf16),
        mine,
        jnp.concatenate([down, south[:, slot:], far_south], axis=1).astype(bf16),
    ]
    a, b = got_even[PACK:, :].astype(f32), got_odd[PACK:, :].astype(f32)
    packs = [jnp.where(even, a, b), pack_ref[...].astype(f32), jnp.where(even, b, a)]
    recv = 3 * slot
    current = jnp.concatenate(
        [dot(x, p[:recv, slot:].astype(bf16)) for x, p in zip(slots, packs)], axis=1
    )
    extra = jnp.concatenate([p[recv : recv + 8, slot:] for p in packs], axis=1)
    parts = jnp.concatenate([p[:, :slot] for p in packs], axis=1)
    soft = soft_growth(
        extra[0:1] + extra[1:2] - current[0:1], extra[2:3] + extra[3:4] - current[1:2]
    )
    fields = fields_of(soft, current[2:3], extra[4:5], parts)
    lane = lax.broadcasted_iota(jnp.int32, fields.shape, 1)
    fields = jnp.where((row == n_row - 1) & (lane < slot), 0.0, fields)
    fields = jnp.where((row == 0) & (lane >= 2 * slot), 0.0, fields)
    slots_ref[...] = fields.astype(bf16)


def k_update_last(
    nfreq, old_ref, moved_ref, mine_ref, recv_ref, wind_ref, wet_ref, coef_ref, out_ref, cur, soft_ref, wide
):
    rows, spec = wet_ref.shape[0], old_ref.shape[0]
    cur[...] = dot(mine_ref[...], recv_ref[...])
    soft_ref[:NDIR, :] = soft_growth(
        flat(wind_ref, 0) - cur[0:1, :], flat(wind_ref, 1) - cur[1:2, :]
    )
    soft_ref[NDIR:, :] = jnp.concatenate([cur[2:3, :]] * (soft_ref.shape[0] - NDIR), axis=0)

    def store(y, cells, value):
        wide[pl.ds(y, spec, stride=rows), :] = value

    update(
        lambda cells: old_ref[:, cells].astype(f32), lambda cells: moved_ref[:, cells],
        soft_ref, wet_ref, coef_ref, nfreq, store,
    )
    out_ref[...] = wide[...].astype(bf16)


def k_last(
    lev,
    spectra_ref, eta_ref, part_ref, north_ref, south_ref, ends_ref, sea_ref, mix_ref,
    spectra_out, eta_out, vel_out,
    vel_ref, smooth, pieces, sems,
):
    copies = [
        pltpu.make_async_copy(spectra_ref, spectra_out, sems.at[0]),
        pltpu.make_async_copy(eta_ref, eta_out, sems.at[1]),
        pltpu.make_async_copy(vel_ref, vel_out, sems.at[2]),
    ]
    copies[0].start()
    copies[1].start()
    k_mix(lev, part_ref, north_ref, south_ref, ends_ref, sea_ref, mix_ref, vel_ref, smooth, pieces)
    copies[2].start()
    for copy in copies:
        copy.wait()


def k_current_out(n_row, got_even, got_odd, own, recv_ref, out_ref):
    rows, lanes = out_ref.shape[1:]
    cur = dot(gather_slots(got_even, got_odd, own, n_row), recv_ref[...])
    for i in range(3):
        for y in range(rows):
            out_ref[i, y : y + 1, :] = cur[i : i + 1, y * lanes : (y + 1) * lanes]


TAU, PROF, THICK, SURF, RATE, GAIN = 0, 1, 1 + NBAND, 2 + NBAND, 3 + NBAND, 4 + NBAND


def row_of(coef_ref, which):
    return lambda l: coef_ref[which * 32 + l : which * 32 + l + 1, :]


def column(vector, first, count):
    row = lax.broadcasted_iota(jnp.int32, (count, vector.shape[1]), 0)
    lane = lax.broadcasted_iota(jnp.int32, (count, vector.shape[1]), 1)
    picked = jnp.sum(jnp.where(row - first == lane, vector, 0.0), axis=1, keepdims=True)
    return jnp.broadcast_to(picked, (count, 128))


def spread(vector, first):
    lev = vector.shape[1]
    parts = [vector, jnp.zeros((1, 128 - lev - first), f32)]
    if first:
        parts = [jnp.zeros((1, first), f32)] + parts
    return jnp.concatenate(parts, axis=1)


def k_prepare(lev, tau_ref, prof_ref, thick_ref, mix_ref, rate_ref, gain_ref, coef_ref, side_ref, lane_ref):
    surf = mix_ref[0:1, :]
    vectors = [tau_ref[...]] + [prof_ref[b : b + 1, :] for b in range(NBAND)]
    vectors += [thick_ref[...], surf, rate_ref[...], gain_ref[...]]
    for i, vector in enumerate(vectors):
        coef_ref[i * 32 : (i + 1) * 32, :] = column(vector, 0, 32)
    side_ref[0] = column(surf, 0, 2 * lev)
    side_ref[1] = column(surf, lev, 2 * lev)
    side_ref[2] = column(thick_ref[...], lev, 2 * lev)
    lane_ref[0:1, :] = spread(surf, 0)
    lane_ref[1:2, :] = spread(surf, lev)
    lane_ref[2:3, :] = spread(thick_ref[...], 0)


def k_force(
    n_row, lev, pad, first,
    *refs,
):
    if first:
        got_even, got_odd, own, *refs = refs
        slots = gather_slots(got_even, got_odd, own, n_row)
    else:
        slot_ref, *refs = refs
        slots = slot_ref[...]
    recv_ref, vel_ref, wet_ref, cor_ref, coef_ref, forced_ref, row_even, row_odd, col_even, col_odd, fs = refs
    oy, ox = wet_ref.shape
    planes = 2 * lev
    forcing = dot(slots, recv_ref[...])
    nf = forcing.shape[0]
    for y in range(oy):
        fs[y * nf : (y + 1) * nf, :] = forcing[:, y * ox : (y + 1) * ox]
    field = [fs[pl.ds(i, oy, stride=nf), :] for i in range(nf)]
    wet = wet_ref[...].astype(f32)
    cor = cor_ref[...]
    along = [cor * field[i] for i in range(2, nf)]
    tau = row_of(coef_ref, TAU)
    prof = [row_of(coef_ref, PROF + b) for b in range(NBAND)]
    lane = lax.broadcasted_iota(jnp.int32, (oy, ox), 1)
    east = jnp.zeros((oy, ox), f32)
    west = jnp.zeros((oy, ox), f32)
    for i in range(planes):
        c, l = divmod(i, lev)
        accel = tau(l) * field[c]
        for b in range(NBAND):
            term = prof[b](l) * along[2 * b + 1 - c]
            accel = accel + term if c == 0 else accel - term
        value = wet * (vel_ref[i * oy : (i + 1) * oy, :] + accel)
        forced_ref[i * oy : (i + 1) * oy, :] = value
        here = lane == i
        west = jnp.where(here, pltpu.roll(value, i, 1) if i else value, west)
        east = jnp.where(here, pltpu.roll(value, (i + 1) % ox, 1), east)
    bottom = forced_ref[pl.ds(0, planes, stride=oy), :]
    top = forced_ref[pl.ds(oy - 1, planes, stride=oy), :]
    even = is_even(lax.axis_index("row"))
    row_even[...] = jnp.where(even, top, bottom).astype(bf16)
    row_odd[...] = jnp.where(even, bottom, top).astype(bf16)
    even = is_even(lax.axis_index("col"))
    col_even[:planes, :] = top.astype(bf16)
    col_odd[:planes, :] = top.astype(bf16)
    filler = jnp.zeros((16 - oy, ox), f32)
    col_even[pad:, :] = jnp.concatenate([jnp.where(even, east, west), filler], 0).astype(bf16)
    col_odd[pad:, :] = jnp.concatenate([jnp.where(even, west, east), filler], 0).astype(bf16)


def borders(oy, ox):
    lane = lax.broadcasted_iota(jnp.int32, (oy, ox), 1)
    line = lax.broadcasted_iota(jnp.int32, (oy, ox), 0)
    return line == oy - 1, line == 0, lane == ox - 1, lane == 0


def k_interior(lev, forced_ref, eta_ref, wet_ref, coef_ref, part_ref, sums_ref):
    oy, ox = wet_ref.shape
    wet = wet_ref[...].astype(f32)
    is_top, is_bottom, is_east, is_west = borders(oy, ox)
    thick, surf = row_of(coef_ref, THICK), row_of(coef_ref, SURF)
    across = jnp.zeros((oy, ox), f32)
    surface = [jnp.zeros((oy, ox), f32), jnp.zeros((oy, ox), f32)]
    for i in range(2 * lev):
        c, l = divmod(i, lev)
        here = forced_ref[i * oy : (i + 1) * oy, :]
        up = jnp.where(is_top, 0.0, pltpu.roll(here, oy - 1, 0))
        down = jnp.where(is_bottom, 0.0, pltpu.roll(here, 1, 0))
        right = jnp.where(is_east, 0.0, pltpu.roll(here, ox - 1, 1))
        left = jnp.where(is_west, 0.0, pltpu.roll(here, 1, 1))
        part = wet * (here + viscous * (up + down + right + left - 4.0 * here))
        part_ref[i * oy : (i + 1) * oy, :] = part
        surface[c] = surface[c] + surf(l) * part
        across = across + thick(l) * (right - left if c == 0 else up - down)
    sums_ref[:oy, :] = surface[0]
    sums_ref[oy : 2 * oy, :] = surface[1]
    sums_ref[2 * oy :, :] = wet * (eta_ref[...] - surface_rate * 0.5 * across)


def k_back(
    n_row, n_col, pad, whole, choose, n_extra,
    got_row_even, got_row_odd, got_col_even, got_col_odd, sent_col, line_ref, fold_ref, sums_ref, wet_ref, side_ref, lane_ref, send_ref,
    *refs,
):
    extra = refs[:n_extra]
    eta_out, north_ref, south_ref, ends_ref, *outs, bs = refs[n_extra:]
    oy, ox = wet_ref.shape
    planes = north_ref.shape[0]
    row, col = lax.axis_index("row"), lax.axis_index("col")
    even = is_even(row)
    a, b = got_row_even[:planes, :].astype(f32), got_row_odd[:planes, :].astype(f32)
    north_ref[...] = jnp.where(even, a, b)

    @pl.when(row == n_row - 1)
    def _():
        if whole:
            pieces = [(line_ref[t * planes : (t + 1) * planes, :], t) for t in range(n_col)]
        else:
            pair_even = jnp.where(is_even(col), col + 1, col - 1)
            pair_odd = lax.rem(jnp.where(is_even(col), col - 1, col + 1) + n_col, n_col)
            pieces = [
                (sent_col[:planes, :], col),
                (got_col_even[:planes, :], pair_even),
                (got_col_odd[:planes, :], pair_odd),
                (got_row_odd[:planes, :], lax.rem(col + n_col // 2, n_col)),
            ]
        cell = lax.broadcasted_iota(jnp.int32, (ox, ox), 0)
        across = None
        for piece, tile in pieces:
            hot = jnp.where(cell == fold_ref[...] - tile * ox, 1.0, 0.0).astype(bf16)
            part = dot(piece, hot)
            across = part if across is None else across + part
        north_ref[...] = -across

    north = north_ref[...]
    south = jnp.where(row == 0, 0.0, jnp.where(even, b, a))
    even = is_even(col)
    a = got_col_even[pad:, :].astype(f32)[:oy]
    b = got_col_odd[pad:, :].astype(f32)[:oy]
    east, west = jnp.where(even, a, b), jnp.where(even, b, a)
    south_ref[...] = south
    ends_ref[:oy, :] = east
    ends_ref[oy:, :] = west
    wet = wet_ref[...].astype(f32)
    is_top, is_bottom, is_east, is_west = borders(oy, ox)

    def over_rows(x, i):
        return jnp.sum(x * side_ref[i], axis=0, keepdims=True)

    def over_lanes(x, i):
        return jnp.sum(x * lane_ref[i : i + 1, :], axis=1, keepdims=True)

    for c in range(2):
        edge = jnp.where(is_top, over_rows(north, c), 0.0) + jnp.where(is_bottom, over_rows(south, c), 0.0)
        edge = edge + jnp.where(is_east, over_lanes(east, c), 0.0)
        edge = edge + jnp.where(is_west, over_lanes(west, c), 0.0)
        bs[c * oy : (c + 1) * oy, :] = sums_ref[c * oy : (c + 1) * oy, :] + viscous * wet * edge
    flow = jnp.where(is_east, over_lanes(east, 2), 0.0) - jnp.where(is_west, over_lanes(west, 2), 0.0)
    flow = flow + jnp.where(is_top, over_rows(north, 2), 0.0) - jnp.where(is_bottom, over_rows(south, 2), 0.0)
    eta = sums_ref[2 * oy :, :] - surface_rate * 0.5 * wet * flow
    eta_out[...] = eta
    bs[2 * oy : 3 * oy, :] = eta
    bs[3 * oy :, :] = jnp.zeros((5 * oy, ox), f32)
    back = jnp.concatenate([bs[pl.ds(y, 8, stride=oy), :] for y in range(oy)], axis=1)
    choose(back, send_ref, (*outs, *extra))


def k_mix(lev, part_ref, north_ref, south_ref, ends_ref, wet_ref, mix_ref, vel_ref, smooth, wide):
    oy, ox = wet_ref.shape
    planes = 2 * lev
    wet = viscous * wet_ref[...].astype(f32)
    is_top, is_bottom, is_east, is_west = borders(oy, ox)
    east, west = ends_ref[:oy, :], ends_ref[oy:, :]
    for i in range(planes):
        edge = jnp.where(is_top, north_ref[i : i + 1, :], 0.0)
        edge = edge + jnp.where(is_bottom, south_ref[i : i + 1, :], 0.0)
        edge = edge + jnp.where(is_east, pltpu.roll(east, (ox - 1 - i) % ox, 1), 0.0)
        edge = edge + jnp.where(is_west, pltpu.roll(west, (ox - i) % ox, 1), 0.0)
        smooth[i * oy : (i + 1) * oy, :] = part_ref[i * oy : (i + 1) * oy, :] + wet * edge
    step = wide.shape[0] // 3
    blocks = [(c, y) for c in range(2) for y in range(oy)]
    for n, (c, y) in enumerate(blocks):
        column_block = smooth[pl.ds(c * lev * oy + y, lev, stride=oy), :]
        column_block = jnp.concatenate([column_block, jnp.zeros((step - lev, ox), f32)], axis=0)
        high, low = split2(column_block)
        cells = slice(n * ox, (n + 1) * ox)
        wide[:step, cells] = high
        wide[step : 2 * step, cells] = low
        wide[2 * step :, cells] = high
    high, low = split2(mix_ref[...])
    filler = jnp.zeros((lev, step - lev), f32)
    high, low = high.astype(f32), low.astype(f32)
    left = jnp.concatenate([high, filler, high, filler, low, filler], axis=1).astype(bf16)
    mixed = dot(left, wide[...])
    for n, (c, y) in enumerate(blocks):
        vel_ref[pl.ds(c * lev * oy + y, lev, stride=oy), :] = mixed[:, n * ox : (n + 1) * ox]


def pairings(n_row, n_col):
    def place(r, c):
        return r * n_col + c

    row_even = [(place(r, c), place(r ^ 1, c)) for r in range(n_row) for c in range(n_col)]
    row_odd = []
    for r in range(n_row):
        other = r + 1 if r % 2 else r - 1
        for c in range(n_col):
            if 0 <= other < n_row:
                row_odd.append((place(r, c), place(other, c)))
            else:
                row_odd.append((place(r, c), place(r, (c + n_col // 2) % n_col)))
    far_even = [(place(r, c), place(r ^ 2, c)) for r in range(n_row) for c in range(n_col)]
    far_odd = []
    for r in range(n_row):
        other = r - 2 if r % 4 < 2 else r + 2
        for c in range(n_col):
            if 0 <= other < n_row:
                far_odd.append((place(r, c), place(other, c)))
            else:
                far_odd.append((place(r, c), place(r, (c + n_col // 2) % n_col)))
    col_even = [(c, c ^ 1) for c in range(n_col)]
    col_odd = [(c, (c + 1 if c % 2 else c - 1) % n_col) for c in range(n_col)]
    return dict(
        row_even=row_even, row_odd=row_odd, col_even=col_even, col_odd=col_odd, far_even=far_even, far_odd=far_odd
    )


def shards(
    n_row,
    n_col,
    spectra,
    wind,
    wave_current,
    wave_wet,
    interaction,
    input_rate,
    eta_gain,
    stress_map,
    stokes_map,
    ocean_vel,
    ocean_eta,
    ocean_wet,
    coriolis,
    tau_profile,
    stokes_profile,
    thickness,
    mix_inverse,
    fold_index,
    wave_send,
    ocean_recv,
    ocean_send,
    wave_recv,
):
    spec, rows, lanes = spectra.shape
    cells = rows * lanes
    oy, ox = ocean_eta.shape
    lev = ocean_vel.shape[1]
    planes = 2 * lev
    nfreq = input_rate.shape[0]
    slot = wave_send.shape[-1]
    pad = -(-planes // 16) * 16
    pairs = pairings(n_row, n_col)
    both = ("row", "col")
    ocean_w = ocean_recv.reshape(3 * slot, oy * ox)
    wave_w = wave_recv.reshape(3 * slot, cells)
    wsend, osend = wave_send.reshape(3, 1, slot), ocean_send.reshape(3, 1, slot)
    fold = fold_index.reshape(1, ox)
    velocity = ocean_vel.reshape(planes * oy, ox)
    eta = ocean_eta
    whole = n_col != 4

    def trade(label, array):
        axis = "col" if label.startswith("col") else both
        return lax.ppermute(array, axis, pairs[label])

    slots_out = [((8, slot), bf16)] * 3
    soft_out = ((32, cells), f32)
    half = GROUP * (NDIR + 2)
    full = (planes * oy, ox)
    mixer = [pltpu.VMEM(full, f32), pltpu.VMEM((96, 2 * oy * ox), bf16)]

    def edges(step, lists, send_of, extra=()):
        first = step == 0
        forced, row_even, row_odd, col_even, col_odd = call(
            functools.partial(k_force, n_row, lev, pad, first),
            [(full, f32)] + [((planes, ox), bf16)] * 2 + [((pad + 16, ox), bf16)] * 2,
            [VMEM] * (len(lists) + 5),
            [pltpu.VMEM((8 * oy, ox), f32)],
        )(*lists, ocean_w, velocity, ocean_wet, coriolis, coef)
        got_row_odd, got_row_even = trade("row_odd", row_odd), trade("row_even", row_even)
        got_col_odd, got_col_even = trade("col_odd", col_odd), trade("col_even", col_even)
        part, sums = call(
            functools.partial(k_interior, lev), [(full, f32), ((3 * oy, ox), f32)], [VMEM] * 4
        )(forced, eta, ocean_wet, coef)
        if whole:
            top_line = lax.all_gather(col_even[:planes], "col", axis=0, tiled=True)
        else:
            top_line = fold
        choose, slots = send_of
        eta_next, north, south, ends, *sent = call(
            functools.partial(k_back, n_row, n_col, pad, whole, choose, len(extra)),
            [((oy, ox), f32)] + [((planes, ox), f32)] * 2 + [((2 * oy, ox), f32)] + slots,
            [VMEM] * (12 + len(extra)),
            [pltpu.VMEM((8 * oy, ox), f32)],
        )(
            got_row_even, got_row_odd, got_col_even, got_col_odd, col_even, top_line, fold, sums, ocean_wet,
            side, lane_rows, osend, *extra,
        )
        return (part, north, south, ends), eta_next, sent

    inputs = (
        stress_map, stokes_map, input_rate, eta_gain, wind, wave_current, wave_wet, wsend,
        spectra.reshape(spec * rows, lanes), interaction,
    )
    held = [(pltpu.SMEM if x.ndim == 1 else pltpu.VMEM)(x.shape, x.dtype) for x in inputs]
    to_even, to_odd, own, energy, soft, weights = call(
        functools.partial(k_wave_first, nfreq),
        slots_out + [((spec, cells), bf16), soft_out, ((half + 2 * GROUP, spec), bf16)],
        [HBM] * len(inputs),
        held + [pltpu.VMEM((spec * rows, lanes), f32), pltpu.SemaphoreType.DMA((len(inputs) + 2,))],
    )(*(pltpu.with_memory_space_constraint(x, pltpu.HBM) for x in inputs))
    got_odd, got_even = trade("row_odd", to_odd), trade("row_even", to_even)
    coef, side, lane_rows = call(
        functools.partial(k_prepare, lev), [((8 * 32, 128), f32), ((3, planes, 128), f32), ((8, 128), f32)], [VMEM] * 6
    )(
        tau_profile.reshape(1, lev), stokes_profile, thickness.reshape(1, lev), mix_inverse,
        input_rate.reshape(1, nfreq), eta_gain.reshape(1, nfreq),
    )
    (energy,) = call(
        functools.partial(k_update, nfreq), [((spec, cells), bf16)], [VMEM] * 5, [pltpu.VMEM((spec, cells), f32)]
    )(energy, interaction, soft, wave_wet, coef)
    pack_south, pack_own, pack_north = call(
        k_pack, [((half, 2 * slot), bf16)] * 3, [VMEM] * 6
    )(energy, weights, wave_w, wind, wave_wet, wsend)
    far_slots = [((PACK + half, 2 * slot), bf16)] * 2 + [((8, 3 * slot), bf16)] + [((8, slot), bf16)] * 2
    smooth, eta, sent = edges(
        0, (got_even, got_odd, own), (pick_far, far_slots), (pack_south, pack_north)
    )
    to_even, to_odd, own, far_even, far_odd = sent
    got_odd, got_even = trade("row_odd", to_odd), trade("row_even", to_even)
    got_far_odd, got_far_even = trade("far_odd", far_odd), trade("far_even", far_even)
    (moved,) = call(k_transfer, [((spec, cells), f32)], [VMEM] * 2)(
        energy, interaction
    )
    (velocity,) = call(functools.partial(k_mix, lev), [(full, f32)], [VMEM] * 6, mixer)(*smooth, ocean_wet, mix_inverse)
    fields, mine = call(
        functools.partial(k_wave_next, n_row), [((8, 3 * slot), bf16)] * 2, [VMEM] * 6
    )(got_even, got_odd, got_far_even, got_far_odd, own, pack_own)
    (spectra_new,) = call(
        functools.partial(k_update_last, nfreq),
        [((spec * rows, lanes), bf16)],
        [VMEM] * 7,
        [
            pltpu.VMEM((8, cells), f32),
            pltpu.VMEM(soft_out[0], f32),
            pltpu.VMEM((spec * rows, lanes), f32),
        ],
    )(energy, moved, mine, wave_w, wind, wave_wet, coef)
    smooth, eta, sent = edges(1, (fields,), (pick, slots_out))
    to_even, to_odd, own = sent
    got_odd, got_even = trade("row_odd", to_odd), trade("row_even", to_even)
    spectra_out, eta, velocity = call(
        functools.partial(k_last, lev),
        [((spec * rows, lanes), bf16), ((oy, ox), f32), (full, f32)],
        [VMEM] * 8,
        [pltpu.VMEM(full, f32), *mixer, pltpu.SemaphoreType.DMA((3,))],
        HBM,
    )(spectra_new, eta, *smooth, ocean_wet, mix_inverse)
    (current,) = call(
        functools.partial(k_current_out, n_row), [((3, rows, lanes), f32)], [VMEM] * 4
    )(got_even, got_odd, own, wave_w)
    return (
        spectra_out.reshape(spec, rows, lanes),
        velocity.reshape(2, lev, oy, ox),
        eta,
        current,
    )


def solution(mesh):
    n_row, n_col = mesh.shape["row"], mesh.shape["col"]
    in_specs = (
        P(None, "row", "col"),
        P(None, "row", "col"),
        P(None, "row", "col"),
        P("row", "col"),
        P(),
        P(),
        P(),
        P(),
        P(),
        P(None, None, "row", "col"),
        P("row", "col"),
        P("row", "col"),
        P("row", "col"),
        P(),
        P(),
        P(),
        P(),
        P("col"),
        P("row", "col", None, None),
        P("row", "col", None, None, None),
        P("row", "col", None, None),
        P("row", "col", None, None, None),
    )
    out_specs = (
        P(None, "row", "col"),
        P(None, None, "row", "col"),
        P("row", "col"),
        P(None, "row", "col"),
    )
    body = functools.partial(shards, n_row, n_col)
    return jax.shard_map(body, mesh=mesh, in_specs=in_specs, out_specs=out_specs, check_vma=False)
```

```python
import functools
import math

import jax
import jax.numpy as jnp
from jax import lax
from jax.experimental import pallas as pl
from jax.experimental.pallas import tpu as pltpu
from jax.sharding import PartitionSpec as P


NDIR = 24
NBAND = 3
viscous = 0.2
surface_rate = 0.5

f32, bf16 = jnp.float32, jnp.bfloat16
VMEM = pl.BlockSpec(memory_space=pltpu.VMEM)
SMEM = pl.BlockSpec(memory_space=pltpu.SMEM)
HBM = pl.BlockSpec(memory_space=pltpu.HBM)


def call(kernel, outs, specs, scratch=(), out_spec=VMEM):
    out_shape = tuple(jax.ShapeDtypeStruct(s, d) for s, d in outs)
    return pl.pallas_call(
        kernel,
        out_shape=out_shape,
        in_specs=list(specs),
        out_specs=tuple(out_spec for _ in outs),
        scratch_shapes=list(scratch),
        compiler_params=pltpu.CompilerParams(vmem_limit_bytes=12 << 20),
    )


def dot(a, b):
    return jnp.dot(a, b, preferred_element_type=f32)


def split2(w):
    high = w.astype(bf16)
    low = (w - high.astype(f32)).astype(bf16)
    return high, low


def is_even(index):
    return lax.rem(index, 2) == 0


PACK = 16
GROUP = 8


def field_weights(smap, kmap, rate_ref, gain_ref, nfreq):
    spec = smap.shape[1]
    col = lax.broadcasted_iota(jnp.int32, (1, spec), 1)
    band = jnp.zeros((1, spec), jnp.int32)
    rate = jnp.full((1, spec), rate_ref[0], f32)
    gain = jnp.full((1, spec), gain_ref[0], f32)
    for f in range(1, nfreq):
        past = col >= NDIR * f
        band = band + jnp.where(past, 1, 0)
        rate = jnp.where(past, rate_ref[f], rate)
        gain = jnp.where(past, gain_ref[f], gain)
    keep = lax.broadcasted_iota(jnp.int32, (NDIR, spec), 0) == col - NDIR * band
    maps = [smap[i : i + 1] for i in range(2)] + [kmap[i : i + 1] for i in range(2 * NBAND)]
    rows = jnp.concatenate([jnp.where(keep, m * rate, 0.0) for m in maps], axis=0)
    return rows, jnp.concatenate([jnp.zeros((2, spec), f32), kmap], axis=0), gain


def rest_weights(stokes, gain, inter):
    high, low = split2(stokes)
    moved = dot(jnp.concatenate([high.astype(f32), low.astype(f32)], axis=0).astype(bf16), inter)
    return jnp.concatenate([stokes * gain, stokes + moved[:GROUP] + moved[GROUP:]], axis=0)


def joined(parts):
    direct = GROUP * NDIR
    rest = parts[direct : direct + 2 * GROUP] + parts[direct + 2 * GROUP :]
    return jnp.concatenate([parts[:direct], rest], axis=0)


def soft_growth(dx, dy):
    heading = lax.broadcasted_iota(jnp.int32, (NDIR, dx.shape[1]), 0).astype(f32)
    heading = (heading + 0.5) * (2.0 * math.pi / NDIR)
    relative = dx * jnp.cos(heading) + dy * jnp.sin(heading)
    return jnp.maximum(relative, 0.0) + jnp.log1p(jnp.exp(-jnp.abs(relative)))


def fields_of(soft, level, wet, parts):
    sums = [
        jnp.sum(soft * parts[i * NDIR : (i + 1) * NDIR], axis=0, keepdims=True) for i in range(GROUP)
    ]
    rest = GROUP * NDIR
    total = jnp.concatenate(sums, axis=0) + level * parts[rest : rest + GROUP] + parts[rest + GROUP :]
    row = lax.broadcasted_iota(jnp.int32, total.shape, 0)
    return jnp.where(row < 2, total, wet * total)


def flat(ref, *first):
    rows = ref.shape[-2]
    return jnp.concatenate([ref[(*first, slice(y, y + 1), slice(None))] for y in range(rows)], axis=1)


def update(old_of, moved_of, soft_ref, wet_ref, coef_ref, nfreq, store):
    rows, lanes = wet_ref.shape
    rate, gain = row_of(coef_ref, RATE), row_of(coef_ref, GAIN)
    for y in range(rows):
        cells = slice(y * lanes, (y + 1) * lanes)
        soft, level = soft_ref[:NDIR, cells], soft_ref[NDIR : NDIR + 1, cells]
        wet = wet_ref[y : y + 1, :].astype(f32)
        growth = jnp.concatenate([rate(f) * soft + gain(f) * level for f in range(nfreq)], axis=0)
        old = old_of(cells)
        store(y, cells, wet * (old + growth * old + moved_of(cells)))


def picked(fields, send):
    index = jnp.concatenate([send[j] for j in range(3)], axis=1)
    cell = lax.broadcasted_iota(jnp.int32, (fields.shape[1], index.shape[1]), 0)
    return dot(fields.astype(bf16), jnp.where(cell == index, 1.0, 0.0).astype(bf16))


def pick(fields, send, outs):
    to_even, to_odd, own = outs
    slot = send.shape[2]
    slots = picked(fields, send)
    even = is_even(lax.axis_index("row"))
    south, north = slots[:, :slot], slots[:, 2 * slot :]
    to_even[...] = jnp.where(even, north, south).astype(bf16)
    to_odd[...] = jnp.where(even, south, north).astype(bf16)
    own[...] = slots[:, slot : 2 * slot].astype(bf16)


def in_first_half(row):
    return lax.rem(row, 4) < 2


def pick_far(fields, send, outs):
    to_even, to_odd, own, far_even, far_odd, pack_even, pack_odd = outs
    slot = send.shape[2]
    slots = picked(fields, send)
    row = lax.axis_index("row")
    even, first = is_even(row), in_first_half(row)
    south, here, north = slots[:, :slot], slots[:, slot : 2 * slot], slots[:, 2 * slot :]
    rows = slots.shape[0]
    to_even[:rows, :] = jnp.concatenate([jnp.where(even, north, south), here], axis=1).astype(bf16)
    to_odd[:rows, :] = jnp.concatenate([jnp.where(even, south, north), here], axis=1).astype(bf16)
    to_even[PACK:, :] = pack_even[...]
    to_odd[PACK:, :] = pack_odd[...]
    own[...] = slots.astype(bf16)
    far_even[...] = jnp.where(first, north, south).astype(bf16)
    far_odd[...] = jnp.where(first, south, north).astype(bf16)


def gather_slots(got_even, got_odd, own, rows):
    row = lax.axis_index("row")
    even = is_even(row)
    a, b = got_even[...].astype(f32), got_odd[...].astype(f32)
    north = jnp.where(row == rows - 1, 0.0, jnp.where(even, a, b))
    south = jnp.where(row == 0, 0.0, jnp.where(even, b, a))
    return jnp.concatenate([north, own[...].astype(f32), south], axis=1).astype(bf16)


def k_wave_first(
    nfreq,
    smap_hbm, kmap_hbm, rate_hbm, gain_hbm, wind_hbm, cur_hbm, wet_hbm, send_hbm, spec_hbm, inter_hbm,
    to_even, to_odd, own, old_ref, soft_ref, weight_ref,
    smap_ref, kmap_ref, rate_ref, gain_ref, wind_ref, cur_ref, wet_ref, send_ref, spec_ref, inter_ref,
    wide, sems,
):
    rows, lanes = wet_ref.shape
    spec = inter_ref.shape[0]
    cut = spec // 32 * 16
    small = (
        (smap_hbm, smap_ref), (kmap_hbm, kmap_ref), (rate_hbm, rate_ref), (gain_hbm, gain_ref),
        (wind_hbm, wind_ref), (cur_hbm, cur_ref), (wet_hbm, wet_ref), (send_hbm, send_ref),
    )
    large = []
    for first, size in ((0, cut), (cut, spec - cut)):
        part = pl.ds(first * rows, size * rows)
        large.append((spec_hbm.at[part], spec_ref.at[part]))
    for first, size in ((0, cut), (cut, spec - cut)):
        part = pl.ds(first, size)
        large.append((inter_hbm.at[part], inter_ref.at[part]))
    copies = [pltpu.make_async_copy(a, b, sems.at[i]) for i, (a, b) in enumerate((*small, *large))]
    for copy in copies:
        copy.start()
    for copy in copies[: len(small)]:
        copy.wait()
    level = flat(cur_ref, 2)
    soft = soft_growth(flat(wind_ref, 0) - flat(cur_ref, 0), flat(wind_ref, 1) - flat(cur_ref, 1))
    soft_ref[:NDIR, :] = soft
    soft_ref[NDIR:, :] = jnp.concatenate([level] * (soft_ref.shape[0] - NDIR), axis=0)
    direct = GROUP * NDIR
    weights, stokes, gain = field_weights(smap_ref[...], kmap_ref[...], rate_ref, gain_ref, nfreq)
    weight_ref[:direct, :] = weights.astype(bf16)
    for n, (first, size) in enumerate(((0, cut), (cut, spec - cut))):
        copies[len(small) + n].wait()
        part = slice(first * rows, (first + size) * rows)
        wide[part, :] = spec_ref[part, :].astype(f32)
        for y in range(rows):
            taken = wide[pl.ds(first * rows + y, size, stride=rows), :]
            old_ref[first : first + size, y * lanes : (y + 1) * lanes] = taken.astype(bf16)
    for copy in copies[len(small) + 2 :]:
        copy.wait()
    half = direct + 2 * GROUP
    rest = rest_weights(stokes, gain, inter_ref[...])
    weight_ref[direct:half, :], weight_ref[half:, :] = split2(rest)
    parts = joined(dot(weight_ref[...], old_ref[...]))
    fields = fields_of(soft, level, flat(wet_ref).astype(f32), parts)
    pick(fields, send_ref, (to_even, to_odd, own))


def k_update(nfreq, old_ref, inter_ref, soft_ref, wet_ref, coef_ref, new_ref, moved):
    moved[...] = dot(inter_ref[...], old_ref[...])

    def store(y, cells, value):
        new_ref[:, cells] = value.astype(bf16)

    update(
        lambda cells: old_ref[:, cells].astype(f32), lambda cells: moved[:, cells],
        soft_ref, wet_ref, coef_ref, nfreq, store,
    )


def k_pack(energy_ref, weight_ref, recv_ref, wind_ref, wet_ref, send_ref, even_ref, own_ref, odd_ref):
    parts = joined(dot(weight_ref[...], energy_ref[...]))
    slot = send_ref.shape[2]
    rows = parts.shape[0]
    extra = []
    for i in range(2):
        high, low = split2(flat(wind_ref, i))
        extra += [high.astype(f32), low.astype(f32)]
    extra.append(flat(wet_ref).astype(f32))
    extra.append(jnp.zeros((rows - recv_ref.shape[0] - len(extra), parts.shape[1]), f32))
    extra = jnp.concatenate(extra, axis=0).astype(bf16)
    stack = jnp.concatenate([parts.astype(bf16), recv_ref[...], extra], axis=0)
    cells = picked(stack, send_ref)
    lanes = [slice(j * slot, (j + 1) * slot) for j in range(3)]
    south, own, north = [jnp.concatenate([cells[:rows, x], cells[rows:, x]], axis=1) for x in lanes]
    even = is_even(lax.axis_index("row"))
    even_ref[...] = jnp.where(even, north, south).astype(bf16)
    own_ref[...] = own.astype(bf16)
    odd_ref[...] = jnp.where(even, south, north).astype(bf16)


def k_transfer(old_ref, inter_ref, moved_ref):
    moved_ref[...] = dot(inter_ref[...], old_ref[...])


def k_wave_next(
    n_row,
    got_even, got_odd, far_even, far_odd, own_ref, pack_ref,
    slots_ref, mine_ref,
):
    slot = far_even.shape[1]
    row = lax.axis_index("row")
    even, first = is_even(row), in_first_half(row)
    rows = own_ref.shape[0]
    a, b = got_even[:rows, :].astype(f32), got_odd[:rows, :].astype(f32)
    north = jnp.where(row == n_row - 1, 0.0, jnp.where(even, a, b))
    south = jnp.where(row == 0, 0.0, jnp.where(even, b, a))
    a, b = far_even[...].astype(f32), far_odd[...].astype(f32)
    far_north = jnp.where(row >= n_row - 2, 0.0, jnp.where(first, a, b))
    far_south = jnp.where(row < 2, 0.0, jnp.where(first, b, a))
    own = own_ref[...].astype(f32)
    down, here, up = own[:, :slot], own[:, slot : 2 * slot], own[:, 2 * slot :]
    mine = jnp.concatenate([north[:, :slot], here, south[:, :slot]], axis=1).astype(bf16)
    mine_ref[...] = mine
    slots = [
        jnp.concatenate([far_north, north[:, slot:], up], axis=1).astype(bf16),
        mine,
        jnp.concatenate([down, south[:, slot:], far_south], axis=1).astype(bf16),
    ]
    a, b = got_even[PACK:, :].astype(f32), got_odd[PACK:, :].astype(f32)
    packs = [jnp.where(even, a, b), pack_ref[...].astype(f32), jnp.where(even, b, a)]
    recv = 3 * slot
    current = jnp.concatenate(
        [dot(x, p[:recv, slot:].astype(bf16)) for x, p in zip(slots, packs)], axis=1
    )
    extra = jnp.concatenate([p[recv : recv + 8, slot:] for p in packs], axis=1)
    parts = jnp.concatenate([p[:, :slot] for p in packs], axis=1)
    soft = soft_growth(
        extra[0:1] + extra[1:2] - current[0:1], extra[2:3] + extra[3:4] - current[1:2]
    )
    fields = fields_of(soft, current[2:3], extra[4:5], parts)
    lane = lax.broadcasted_iota(jnp.int32, fields.shape, 1)
    fields = jnp.where((row == n_row - 1) & (lane < slot), 0.0, fields)
    fields = jnp.where((row == 0) & (lane >= 2 * slot), 0.0, fields)
    slots_ref[...] = fields.astype(bf16)


def k_update_last(
    nfreq, old_ref, moved_ref, mine_ref, recv_ref, wind_ref, wet_ref, coef_ref, out_ref, cur, soft_ref, wide
):
    rows, spec = wet_ref.shape[0], old_ref.shape[0]
    cur[...] = dot(mine_ref[...], recv_ref[...])
    soft_ref[:NDIR, :] = soft_growth(
        flat(wind_ref, 0) - cur[0:1, :], flat(wind_ref, 1) - cur[1:2, :]
    )
    soft_ref[NDIR:, :] = jnp.concatenate([cur[2:3, :]] * (soft_ref.shape[0] - NDIR), axis=0)

    def store(y, cells, value):
        wide[pl.ds(y, spec, stride=rows), :] = value

    update(
        lambda cells: old_ref[:, cells].astype(f32), lambda cells: moved_ref[:, cells],
        soft_ref, wet_ref, coef_ref, nfreq, store,
    )
    out_ref[...] = wide[...].astype(bf16)


def k_last(
    lev,
    spectra_ref, eta_ref, part_ref, north_ref, south_ref, ends_ref, sea_ref, mix_ref,
    spectra_out, eta_out, vel_out,
    vel_ref, smooth, pieces, sems,
):
    copies = [
        pltpu.make_async_copy(spectra_ref, spectra_out, sems.at[0]),
        pltpu.make_async_copy(eta_ref, eta_out, sems.at[1]),
        pltpu.make_async_copy(vel_ref, vel_out, sems.at[2]),
    ]
    copies[0].start()
    copies[1].start()
    k_mix(lev, part_ref, north_ref, south_ref, ends_ref, sea_ref, mix_ref, vel_ref, smooth, pieces)
    copies[2].start()
    for copy in copies:
        copy.wait()


def k_current_out(n_row, got_even, got_odd, own, recv_ref, out_ref):
    rows, lanes = out_ref.shape[1:]
    cur = dot(gather_slots(got_even, got_odd, own, n_row), recv_ref[...])
    for i in range(3):
        for y in range(rows):
            out_ref[i, y : y + 1, :] = cur[i : i + 1, y * lanes : (y + 1) * lanes]


TAU, PROF, THICK, SURF, RATE, GAIN = 0, 1, 1 + NBAND, 2 + NBAND, 3 + NBAND, 4 + NBAND


def row_of(coef_ref, which):
    return lambda l: coef_ref[which * 32 + l : which * 32 + l + 1, :]


def column(vector, first, count):
    row = lax.broadcasted_iota(jnp.int32, (count, vector.shape[1]), 0)
    lane = lax.broadcasted_iota(jnp.int32, (count, vector.shape[1]), 1)
    picked = jnp.sum(jnp.where(row - first == lane, vector, 0.0), axis=1, keepdims=True)
    return jnp.broadcast_to(picked, (count, 128))


def spread(vector, first):
    lev = vector.shape[1]
    parts = [vector, jnp.zeros((1, 128 - lev - first), f32)]
    if first:
        parts = [jnp.zeros((1, first), f32)] + parts
    return jnp.concatenate(parts, axis=1)


def k_prepare(lev, tau_ref, prof_ref, thick_ref, mix_ref, rate_ref, gain_ref, coef_ref, side_ref, lane_ref):
    surf = mix_ref[0:1, :]
    vectors = [tau_ref[...]] + [prof_ref[b : b + 1, :] for b in range(NBAND)]
    vectors += [thick_ref[...], surf, rate_ref[...], gain_ref[...]]
    for i, vector in enumerate(vectors):
        coef_ref[i * 32 : (i + 1) * 32, :] = column(vector, 0, 32)
    side_ref[0] = column(surf, 0, 2 * lev)
    side_ref[1] = column(surf, lev, 2 * lev)
    side_ref[2] = column(thick_ref[...], lev, 2 * lev)
    lane_ref[0:1, :] = spread(surf, 0)
    lane_ref[1:2, :] = spread(surf, lev)
    lane_ref[2:3, :] = spread(thick_ref[...], 0)


def k_force(
    n_row, lev, pad, first,
    *refs,
):
    if first:
        got_even, got_odd, own, *refs = refs
        slots = gather_slots(got_even, got_odd, own, n_row)
    else:
        slot_ref, *refs = refs
        slots = slot_ref[...]
    recv_ref, vel_ref, wet_ref, cor_ref, coef_ref, forced_ref, row_even, row_odd, col_even, col_odd, fs = refs
    oy, ox = wet_ref.shape
    planes = 2 * lev
    forcing = dot(slots, recv_ref[...])
    nf = forcing.shape[0]
    for y in range(oy):
        fs[y * nf : (y + 1) * nf, :] = forcing[:, y * ox : (y + 1) * ox]
    field = [fs[pl.ds(i, oy, stride=nf), :] for i in range(nf)]
    wet = wet_ref[...].astype(f32)
    cor = cor_ref[...]
    along = [cor * field[i] for i in range(2, nf)]
    tau = row_of(coef_ref, TAU)
    prof = [row_of(coef_ref, PROF + b) for b in range(NBAND)]
    lane = lax.broadcasted_iota(jnp.int32, (oy, ox), 1)
    east = jnp.zeros((oy, ox), f32)
    west = jnp.zeros((oy, ox), f32)
    for i in range(planes):
        c, l = divmod(i, lev)
        accel = tau(l) * field[c]
        for b in range(NBAND):
            term = prof[b](l) * along[2 * b + 1 - c]
            accel = accel + term if c == 0 else accel - term
        value = wet * (vel_ref[i * oy : (i + 1) * oy, :] + accel)
        forced_ref[i * oy : (i + 1) * oy, :] = value
        here = lane == i
        west = jnp.where(here, pltpu.roll(value, i, 1) if i else value, west)
        east = jnp.where(here, pltpu.roll(value, (i + 1) % ox, 1), east)
    bottom = forced_ref[pl.ds(0, planes, stride=oy), :]
    top = forced_ref[pl.ds(oy - 1, planes, stride=oy), :]
    even = is_even(lax.axis_index("row"))
    row_even[...] = jnp.where(even, top, bottom).astype(bf16)
    row_odd[...] = jnp.where(even, bottom, top).astype(bf16)
    even = is_even(lax.axis_index("col"))
    col_even[:planes, :] = top.astype(bf16)
    col_odd[:planes, :] = top.astype(bf16)
    filler = jnp.zeros((16 - oy, ox), f32)
    col_even[pad:, :] = jnp.concatenate([jnp.where(even, east, west), filler], 0).astype(bf16)
    col_odd[pad:, :] = jnp.concatenate([jnp.where(even, west, east), filler], 0).astype(bf16)


def borders(oy, ox):
    lane = lax.broadcasted_iota(jnp.int32, (oy, ox), 1)
    line = lax.broadcasted_iota(jnp.int32, (oy, ox), 0)
    return line == oy - 1, line == 0, lane == ox - 1, lane == 0


def k_interior(lev, forced_ref, eta_ref, wet_ref, coef_ref, part_ref, sums_ref):
    oy, ox = wet_ref.shape
    wet = wet_ref[...].astype(f32)
    is_top, is_bottom, is_east, is_west = borders(oy, ox)
    thick, surf = row_of(coef_ref, THICK), row_of(coef_ref, SURF)
    across = jnp.zeros((oy, ox), f32)
    surface = [jnp.zeros((oy, ox), f32), jnp.zeros((oy, ox), f32)]
    for i in range(2 * lev):
        c, l = divmod(i, lev)
        here = forced_ref[i * oy : (i + 1) * oy, :]
        up = jnp.where(is_top, 0.0, pltpu.roll(here, oy - 1, 0))
        down = jnp.where(is_bottom, 0.0, pltpu.roll(here, 1, 0))
        right = jnp.where(is_east, 0.0, pltpu.roll(here, ox - 1, 1))
        left = jnp.where(is_west, 0.0, pltpu.roll(here, 1, 1))
        part = wet * (here + viscous * (up + down + right + left - 4.0 * here))
        part_ref[i * oy : (i + 1) * oy, :] = part
        surface[c] = surface[c] + surf(l) * part
        across = across + thick(l) * (right - left if c == 0 else up - down)
    sums_ref[:oy, :] = surface[0]
    sums_ref[oy : 2 * oy, :] = surface[1]
    sums_ref[2 * oy :, :] = wet * (eta_ref[...] - surface_rate * 0.5 * across)


def k_back(
    n_row, n_col, pad, whole, choose, n_extra,
    got_row_even, got_row_odd, got_col_even, got_col_odd, sent_col, line_ref, fold_ref, sums_ref, wet_ref, side_ref, lane_ref, send_ref,
    *refs,
):
    extra = refs[:n_extra]
    eta_out, north_ref, south_ref, ends_ref, *outs, bs = refs[n_extra:]
    oy, ox = wet_ref.shape
    planes = north_ref.shape[0]
    row, col = lax.axis_index("row"), lax.axis_index("col")
    even = is_even(row)
    a, b = got_row_even[:planes, :].astype(f32), got_row_odd[:planes, :].astype(f32)
    north_ref[...] = jnp.where(even, a, b)

    @pl.when(row == n_row - 1)
    def _():
        if whole:
            pieces = [(line_ref[t * planes : (t + 1) * planes, :], t) for t in range(n_col)]
        else:
            pair_even = jnp.where(is_even(col), col + 1, col - 1)
            pair_odd = lax.rem(jnp.where(is_even(col), col - 1, col + 1) + n_col, n_col)
            pieces = [
                (sent_col[:planes, :], col),
                (got_col_even[:planes, :], pair_even),
                (got_col_odd[:planes, :], pair_odd),
                (got_row_odd[:planes, :], lax.rem(col + n_col // 2, n_col)),
            ]
        cell = lax.broadcasted_iota(jnp.int32, (ox, ox), 0)
        across = None
        for piece, tile in pieces:
            hot = jnp.where(cell == fold_ref[...] - tile * ox, 1.0, 0.0).astype(bf16)
            part = dot(piece, hot)
            across = part if across is None else across + part
        north_ref[...] = -across

    north = north_ref[...]
    south = jnp.where(row == 0, 0.0, jnp.where(even, b, a))
    even = is_even(col)
    a = got_col_even[pad:, :].astype(f32)[:oy]
    b = got_col_odd[pad:, :].astype(f32)[:oy]
    east, west = jnp.where(even, a, b), jnp.where(even, b, a)
    south_ref[...] = south
    ends_ref[:oy, :] = east
    ends_ref[oy:, :] = west
    wet = wet_ref[...].astype(f32)
    is_top, is_bottom, is_east, is_west = borders(oy, ox)

    def over_rows(x, i):
        return jnp.sum(x * side_ref[i], axis=0, keepdims=True)

    def over_lanes(x, i):
        return jnp.sum(x * lane_ref[i : i + 1, :], axis=1, keepdims=True)

    for c in range(2):
        edge = jnp.where(is_top, over_rows(north, c), 0.0) + jnp.where(is_bottom, over_rows(south, c), 0.0)
        edge = edge + jnp.where(is_east, over_lanes(east, c), 0.0)
        edge = edge + jnp.where(is_west, over_lanes(west, c), 0.0)
        bs[c * oy : (c + 1) * oy, :] = sums_ref[c * oy : (c + 1) * oy, :] + viscous * wet * edge
    flow = jnp.where(is_east, over_lanes(east, 2), 0.0) - jnp.where(is_west, over_lanes(west, 2), 0.0)
    flow = flow + jnp.where(is_top, over_rows(north, 2), 0.0) - jnp.where(is_bottom, over_rows(south, 2), 0.0)
    eta = sums_ref[2 * oy :, :] - surface_rate * 0.5 * wet * flow
    eta_out[...] = eta
    bs[2 * oy : 3 * oy, :] = eta
    bs[3 * oy :, :] = jnp.zeros((5 * oy, ox), f32)
    back = jnp.concatenate([bs[pl.ds(y, 8, stride=oy), :] for y in range(oy)], axis=1)
    choose(back, send_ref, (*outs, *extra))


def k_mix(lev, part_ref, north_ref, south_ref, ends_ref, wet_ref, mix_ref, vel_ref, smooth, wide):
    oy, ox = wet_ref.shape
    planes = 2 * lev
    wet = viscous * wet_ref[...].astype(f32)
    is_top, is_bottom, is_east, is_west = borders(oy, ox)
    east, west = ends_ref[:oy, :], ends_ref[oy:, :]
    for i in range(planes):
        edge = jnp.where(is_top, north_ref[i : i + 1, :], 0.0)
        edge = edge + jnp.where(is_bottom, south_ref[i : i + 1, :], 0.0)
        edge = edge + jnp.where(is_east, pltpu.roll(east, (ox - 1 - i) % ox, 1), 0.0)
        edge = edge + jnp.where(is_west, pltpu.roll(west, (ox - i) % ox, 1), 0.0)
        smooth[i * oy : (i + 1) * oy, :] = part_ref[i * oy : (i + 1) * oy, :] + wet * edge
    step = wide.shape[0] // 3
    blocks = [(c, y) for c in range(2) for y in range(oy)]
    for n, (c, y) in enumerate(blocks):
        column_block = smooth[pl.ds(c * lev * oy + y, lev, stride=oy), :]
        column_block = jnp.concatenate([column_block, jnp.zeros((step - lev, ox), f32)], axis=0)
        high, low = split2(column_block)
        cells = slice(n * ox, (n + 1) * ox)
        wide[:step, cells] = high
        wide[step : 2 * step, cells] = low
        wide[2 * step :, cells] = high
    high, low = split2(mix_ref[...])
    filler = jnp.zeros((lev, step - lev), f32)
    high, low = high.astype(f32), low.astype(f32)
    left = jnp.concatenate([high, filler, high, filler, low, filler], axis=1).astype(bf16)
    mixed = dot(left, wide[...])
    for n, (c, y) in enumerate(blocks):
        vel_ref[pl.ds(c * lev * oy + y, lev, stride=oy), :] = mixed[:, n * ox : (n + 1) * ox]


def pairings(n_row, n_col):
    def place(r, c):
        return r * n_col + c

    row_even = [(place(r, c), place(r ^ 1, c)) for r in range(n_row) for c in range(n_col)]
    row_odd = []
    for r in range(n_row):
        other = r + 1 if r % 2 else r - 1
        for c in range(n_col):
            if 0 <= other < n_row:
                row_odd.append((place(r, c), place(other, c)))
            else:
                row_odd.append((place(r, c), place(r, (c + n_col // 2) % n_col)))
    far_even = [(place(r, c), place(r ^ 2, c)) for r in range(n_row) for c in range(n_col)]
    far_odd = []
    for r in range(n_row):
        other = r - 2 if r % 4 < 2 else r + 2
        for c in range(n_col):
            if 0 <= other < n_row:
                far_odd.append((place(r, c), place(other, c)))
            else:
                far_odd.append((place(r, c), place(r, (c + n_col // 2) % n_col)))
    col_even = [(c, c ^ 1) for c in range(n_col)]
    col_odd = [(c, (c + 1 if c % 2 else c - 1) % n_col) for c in range(n_col)]
    return dict(
        row_even=row_even, row_odd=row_odd, col_even=col_even, col_odd=col_odd, far_even=far_even, far_odd=far_odd
    )


def shards(
    n_row,
    n_col,
    spectra,
    wind,
    wave_current,
    wave_wet,
    interaction,
    input_rate,
    eta_gain,
    stress_map,
    stokes_map,
    ocean_vel,
    ocean_eta,
    ocean_wet,
    coriolis,
    tau_profile,
    stokes_profile,
    thickness,
    mix_inverse,
    fold_index,
    wave_send,
    ocean_recv,
    ocean_send,
    wave_recv,
):
    spec, rows, lanes = spectra.shape
    cells = rows * lanes
    oy, ox = ocean_eta.shape
    lev = ocean_vel.shape[1]
    planes = 2 * lev
    nfreq = input_rate.shape[0]
    slot = wave_send.shape[-1]
    pad = -(-planes // 16) * 16
    pairs = pairings(n_row, n_col)
    both = ("row", "col")
    ocean_w = ocean_recv.reshape(3 * slot, oy * ox)
    wave_w = wave_recv.reshape(3 * slot, cells)
    wsend, osend = wave_send.reshape(3, 1, slot), ocean_send.reshape(3, 1, slot)
    fold = fold_index.reshape(1, ox)
    velocity = ocean_vel.reshape(planes * oy, ox)
    eta = ocean_eta
    whole = n_col != 4

    def trade(label, array):
        axis = "col" if label.startswith("col") else both
        return lax.ppermute(array, axis, pairs[label])

    slots_out = [((8, slot), bf16)] * 3
    soft_out = ((32, cells), f32)
    half = GROUP * (NDIR + 2)
    full = (planes * oy, ox)
    mixer = [pltpu.VMEM(full, f32), pltpu.VMEM((96, 2 * oy * ox), bf16)]

    def edges(step, lists, send_of, extra=()):
        first = step == 0
        forced, row_even, row_odd, col_even, col_odd = call(
            functools.partial(k_force, n_row, lev, pad, first),
            [(full, f32)] + [((planes, ox), bf16)] * 2 + [((pad + 16, ox), bf16)] * 2,
            [VMEM] * (len(lists) + 5),
            [pltpu.VMEM((8 * oy, ox), f32)],
        )(*lists, ocean_w, velocity, ocean_wet, coriolis, coef)
        got_row_odd, got_row_even = trade("row_odd", row_odd), trade("row_even", row_even)
        got_col_odd, got_col_even = trade("col_odd", col_odd), trade("col_even", col_even)
        part, sums = call(
            functools.partial(k_interior, lev), [(full, f32), ((3 * oy, ox), f32)], [VMEM] * 4
        )(forced, eta, ocean_wet, coef)
        if whole:
            top_line = lax.all_gather(col_even[:planes], "col", axis=0, tiled=True)
        else:
            top_line = fold
        choose, slots = send_of
        eta_next, north, south, ends, *sent = call(
            functools.partial(k_back, n_row, n_col, pad, whole, choose, len(extra)),
            [((oy, ox), f32)] + [((planes, ox), f32)] * 2 + [((2 * oy, ox), f32)] + slots,
            [VMEM] * (12 + len(extra)),
            [pltpu.VMEM((8 * oy, ox), f32)],
        )(
            got_row_even, got_row_odd, got_col_even, got_col_odd, col_even, top_line, fold, sums, ocean_wet,
            side, lane_rows, osend, *extra,
        )
        return (part, north, south, ends), eta_next, sent

    inputs = (
        stress_map, stokes_map, input_rate, eta_gain, wind, wave_current, wave_wet, wsend,
        spectra.reshape(spec * rows, lanes), interaction,
    )
    held = [(pltpu.SMEM if x.ndim == 1 else pltpu.VMEM)(x.shape, x.dtype) for x in inputs]
    to_even, to_odd, own, energy, soft, weights = call(
        functools.partial(k_wave_first, nfreq),
        slots_out + [((spec, cells), bf16), soft_out, ((half + 2 * GROUP, spec), bf16)],
        [HBM] * len(inputs),
        held + [pltpu.VMEM((spec * rows, lanes), f32), pltpu.SemaphoreType.DMA((len(inputs) + 2,))],
    )(*(pltpu.with_memory_space_constraint(x, pltpu.HBM) for x in inputs))
    got_odd, got_even = trade("row_odd", to_odd), trade("row_even", to_even)
    coef, side, lane_rows = call(
        functools.partial(k_prepare, lev), [((8 * 32, 128), f32), ((3, planes, 128), f32), ((8, 128), f32)], [VMEM] * 6
    )(
        tau_profile.reshape(1, lev), stokes_profile, thickness.reshape(1, lev), mix_inverse,
        input_rate.reshape(1, nfreq), eta_gain.reshape(1, nfreq),
    )
    (energy,) = call(
        functools.partial(k_update, nfreq), [((spec, cells), bf16)], [VMEM] * 5, [pltpu.VMEM((spec, cells), f32)]
    )(energy, interaction, soft, wave_wet, coef)
    pack_even, pack_own, pack_odd = call(
        k_pack, [((half, 2 * slot), bf16)] * 3, [VMEM] * 6
    )(energy, weights, wave_w, wind, wave_wet, wsend)
    far_slots = [((PACK + half, 2 * slot), bf16)] * 2 + [((8, 3 * slot), bf16)] + [((8, slot), bf16)] * 2
    smooth, eta, sent = edges(
        0, (got_even, got_odd, own), (pick_far, far_slots), (pack_even, pack_odd)
    )
    to_even, to_odd, own, far_even, far_odd = sent
    got_odd, got_even = trade("row_odd", to_odd), trade("row_even", to_even)
    got_far_odd, got_far_even = trade("far_odd", far_odd), trade("far_even", far_even)
    (moved,) = call(k_transfer, [((spec, cells), f32)], [VMEM] * 2)(
        energy, interaction
    )
    (velocity,) = call(functools.partial(k_mix, lev), [(full, f32)], [VMEM] * 6, mixer)(*smooth, ocean_wet, mix_inverse)
    fields, mine = call(
        functools.partial(k_wave_next, n_row), [((8, 3 * slot), bf16)] * 2, [VMEM] * 6
    )(got_even, got_odd, got_far_even, got_far_odd, own, pack_own)
    (spectra_new,) = call(
        functools.partial(k_update_last, nfreq),
        [((spec * rows, lanes), bf16)],
        [VMEM] * 7,
        [
            pltpu.VMEM((8, cells), f32),
            pltpu.VMEM(soft_out[0], f32),
            pltpu.VMEM((spec * rows, lanes), f32),
        ],
    )(energy, moved, mine, wave_w, wind, wave_wet, coef)
    smooth, eta, sent = edges(1, (fields,), (pick, slots_out))
    to_even, to_odd, own = sent
    got_odd, got_even = trade("row_odd", to_odd), trade("row_even", to_even)
    spectra_out, eta, velocity = call(
        functools.partial(k_last, lev),
        [((spec * rows, lanes), bf16), ((oy, ox), f32), (full, f32)],
        [VMEM] * 8,
        [pltpu.VMEM(full, f32), *mixer, pltpu.SemaphoreType.DMA((3,))],
        HBM,
    )(spectra_new, eta, *smooth, ocean_wet, mix_inverse)
    (current,) = call(
        functools.partial(k_current_out, n_row), [((3, rows, lanes), f32)], [VMEM] * 4
    )(got_even, got_odd, own, wave_w)
    return (
        spectra_out.reshape(spec, rows, lanes),
        velocity.reshape(2, lev, oy, ox),
        eta,
        current,
    )


def solution(mesh):
    n_row, n_col = mesh.shape["row"], mesh.shape["col"]
    in_specs = (
        P(None, "row", "col"),
        P(None, "row", "col"),
        P(None, "row", "col"),
        P("row", "col"),
        P(),
        P(),
        P(),
        P(),
        P(),
        P(None, None, "row", "col"),
        P("row", "col"),
        P("row", "col"),
        P("row", "col"),
        P(),
        P(),
        P(),
        P(),
        P("col"),
        P("row", "col", None, None),
        P("row", "col", None, None, None),
        P("row", "col", None, None),
        P("row", "col", None, None, None),
    )
    out_specs = (
        P(None, "row", "col"),
        P(None, None, "row", "col"),
        P("row", "col"),
        P(None, "row", "col"),
    )
    body = functools.partial(shards, n_row, n_col)
    return jax.shard_map(body, mesh=mesh, in_specs=in_specs, out_specs=out_specs, check_vma=False)
```
